128 devices in a mesh: task: 8 (over x_hi, y), tp: 16 (over z, x_lo, core).
Axes of the slice: x: 4 (x_hi: 2, x_lo: 2; x = x_hi * 2 + x_lo), y: 4, z: 4, core: 2. Of those that a mesh axis runs over, the one named last changes fastest.
Arguments:
- observations: bfloat16 [256, 16, 4096], P('task', None, 'tp'), may hold values from -6 to 6
- gain: float32 [4096], P('tp'), may hold values from 0.5 to 1.5
- w_in: bfloat16 [4096, 4096], P(None, 'tp'), may hold values from -0.09375 to 0.09375
- w_mix: bfloat16 [4096, 4096], P('tp'), may hold values from -0.09375 to 0.09375
- w_out: bfloat16 [4096, 4096], P(None, 'tp'), may hold values from -0.09375 to 0.09375
- w_head: bfloat16 [4096, 75], P('tp'), may hold values from -0.09375 to 0.09375
- head_bias: float32 [75], replicated, may hold values from -4 to 4
- pop_mean: float32 [57], replicated, may hold values from -8 to 8
- pop_scale: float32 [57], replicated, may hold values from 0.5 to 4
- task_indices: int32 [256], P('task'), may hold values from 0 to 56
- actions: int32 [256, 15], P('task'), may hold values from 0 to 17
- rewards: float32 [256, 15], P('task'), may hold values from -18 to 27
- episode_ends: int32 [256, 15], P('task'), may hold values 0 or 1
- behaviour_log_prob: float32 [256, 15], P('task'), may hold values from -4.5 to -1.5
Outputs:
- grad_w_in: float32 [4096, 4096], P(None, 'tp')
- grad_w_mix: float32 [4096, 4096], P('tp')
- grad_w_out: float32 [4096, 4096], P(None, 'tp')
- grad_gain: float32 [4096], P('tp')
- grad_head: float32 [4096, 75], P('tp')
- grad_head_bias: float32 [75], replicated
- new_head: bfloat16 [4096, 75], P('tp')
- new_bias: float32 [75], replicated
- updated_return_mean: float32 [57], replicated
- updated_return_scale: float32 [57], replicated
The draws below stay inside these ranges and needn't reach their ends.
All inputs are finite; a program needn't handle non-finite values. No bound on the sum of `episode_ends` on one device may be relied on, other than what follows from the above.
Results may differ from the reference program's by a relative error of at most 0.03.
Values may be sent and summed in bfloat16 or wider, within the bound.
A program may use at most 128 MiB of HBM per device.

```python
import math
import jax
import jax.numpy as jnp
from jax import lax

D = 4096
ACTIONS = 18
TASKS = 57
HEADS = 75
B_DEV = 32
FRAMES = 16
UNROLL = 15
ENVS = 256
N_TP = 16


def draw_rewards(key, part):
    group_index = (jnp.arange(ENVS, dtype=jnp.int32) // B_DEV).astype(jnp.float32)
    last_group = max(ENVS // B_DEV - 1, 1)
    rising = 1.0 + 2.0 * group_index / last_group
    sample = jnp.clip(jax.random.normal(key, (ENVS, UNROLL), jnp.float32), -4.0, 4.0)
    return sample * rising[:, None]


def set_ends(values, key, least, top_value):
    longest = values.shape.index(max(values.shape))
    spots = []
    for shift in (0, 1):
        where = [jax.random.randint(jax.random.fold_in(key, axis), (), 0, length) for axis, length in enumerate(values.shape)]
        where[longest] = (where[longest] + shift) % values.shape[longest]
        spots.append(tuple(where))
    return values.at[spots[0]].set(least).at[spots[1]].set(top_value)


def shard_levels(own_key, shape, shards, low, top_value):
    def one(axis_at, shards_of):
        heights = jax.random.uniform(jax.random.fold_in(jax.random.fold_in(own_key, 6), axis_at), (shards_of,), jnp.float32, low / len(shards), top_value / len(shards))
        return jnp.repeat(jnp.exp(heights), shape[axis_at] // shards_of).reshape((-1,) + (1,) * (len(shape) - axis_at - 1))

    loudness = one(*shards[0])
    for cut in shards[1:]:
        loudness = loudness * one(*cut)
    return loudness


def bell_draw(rng, extent, width, most, split=(), held_as=jnp.bfloat16):
    entries = width * jax.random.normal(rng, extent, jnp.float32)
    if split:
        entries = entries * shard_levels(rng, extent, split, -0.22, 0.18)
    return jnp.clip(entries, -most, most).astype(held_as)


def setup_inputs(seed: int = 0) -> dict:
    keys = jax.random.split(jax.random.key(seed), 15)
    observations = bell_draw(keys[0], (ENVS, FRAMES, D), 1.0, 6.0, ((0, 8), (2, 16)))
    gain = jnp.clip(1.0 + 0.1 * jax.random.normal(keys[1], (D,), jnp.float32), 0.5, 1.5)
    w_in = bell_draw(keys[2], (D, D), D ** -0.5, 0.09375, ((1, 16),))
    w_mix = bell_draw(keys[3], (D, D), D ** -0.5, 0.09375, ((0, 16),))
    w_out = bell_draw(keys[4], (D, D), D ** -0.5, 0.09375, ((1, 16),))
    w_head = bell_draw(keys[5], (D, HEADS), D ** -0.5, 0.09375, ((0, 16),))
    head_bias = bell_draw(keys[6], (HEADS,), 1.0, 4.0, (), jnp.float32)
    pop_mean = bell_draw(keys[7], (TASKS,), 2.0, 8.0, (), jnp.float32)
    pop_scale = jnp.clip(jnp.exp(jax.random.uniform(keys[8], (TASKS,), jnp.float32, math.log(0.5), math.log(4.0))), 0.5, 4.0)
    task_indices = set_ends(jax.random.randint(keys[9], (ENVS,), 0, TASKS), jax.random.fold_in(keys[9], 1), 0, TASKS - 1).astype(jnp.int32)
    actions = set_ends(jax.random.randint(keys[10], (ENVS, UNROLL), 0, ACTIONS), jax.random.fold_in(keys[10], 1), 0, ACTIONS - 1).astype(jnp.int32)
    rewards = draw_rewards(jax.random.fold_in(keys[14], 71), 0)
    episode_ends = set_ends((jax.random.randint(keys[12], (ENVS, UNROLL), 0, 16) < 1).astype(jnp.int32), jax.random.fold_in(keys[12], 1), 0, 1)
    behaviour_log_prob = jnp.clip(-4.5 + 3.0 * jax.random.uniform(keys[13], (ENVS, UNROLL), jnp.float32) ** shard_levels(keys[13], (ENVS, UNROLL), ((0, 8),), -0.2, 0.2), -4.5, -1.5)
    return dict(observations=observations, gain=gain, w_in=w_in, w_mix=w_mix, w_out=w_out, w_head=w_head, head_bias=head_bias, pop_mean=pop_mean, pop_scale=pop_scale, task_indices=task_indices, actions=actions, rewards=rewards, episode_ends=episode_ends, behaviour_log_prob=behaviour_log_prob)


DISCOUNT = 0.99
BASELINE_COST = 0.5
ENTROPY_COST = 0.01
POPART_PRIOR = 64.0
NORM_EPS = 1e-06

def silu_slope(before):
    sigmoid = jax.nn.sigmoid(before)
    return sigmoid * (1.0 + before * (1.0 - sigmoid))

def discounted_sums(values, factors):

    def advance(running, column):
        latest = column[0] + column[1] * running
        return (latest, latest)
    opening = jnp.zeros((values.shape[0],), jnp.float32)
    ending, stacked = lax.scan(advance, opening, (values.T, factors.T), reverse=True)
    return stacked.T

def task_onehot(task_indices):
    return (task_indices[:, None] == jnp.arange(TASKS, dtype=jnp.int32)[None, :]).astype(jnp.float32)

def popart_partials(task_indices, rewards, discount_factors):
    returns = discounted_sums(rewards, discount_factors)
    task_table = task_onehot(task_indices)
    counts = lax.optimization_barrier(jnp.sum(task_table, axis=0)) * rewards.shape[1]
    totals = jnp.dot(task_table.T, lax.optimization_barrier(jnp.sum(returns, axis=1)), precision=lax.Precision.HIGHEST)
    squares = jnp.dot(task_table.T, lax.optimization_barrier(jnp.sum(returns * returns, axis=1)), precision=lax.Precision.HIGHEST)
    return (counts, totals, squares)

def popart_update(counts, totals, squares, pop_mean, pop_scale):
    mixing = counts / (counts + POPART_PRIOR)
    safe_counts = jnp.maximum(counts, 1.0)
    batch_mean = totals / safe_counts
    batch_square = squares / safe_counts
    updated_return_mean = (1.0 - mixing) * pop_mean + mixing * batch_mean
    mean_gap = batch_mean - pop_mean
    variance = (1.0 - mixing) * pop_scale * pop_scale + mixing * (batch_square - batch_mean * batch_mean) + mixing * (1.0 - mixing) * mean_gap * mean_gap
    return (updated_return_mean, jnp.sqrt(variance))

def rescale_head(w_head, head_bias, pop_mean, pop_scale, updated_return_mean, updated_return_scale):
    scale_ratio = pop_scale / updated_return_scale
    column_scale = jnp.concatenate([jnp.ones((ACTIONS,), jnp.float32), scale_ratio])
    new_head = (w_head.astype(jnp.float32) * column_scale[None, :]).astype(jnp.bfloat16)
    value_bias = (pop_scale * head_bias[ACTIONS:] + pop_mean - updated_return_mean) / updated_return_scale
    new_bias = jnp.concatenate([head_bias[:ACTIONS], value_bias])
    return (new_head, new_bias)

def importance_trace_loss(head_value_estimates, task_indices, actions, rewards, discount_factors, behaviour_log_prob, updated_return_mean, updated_return_scale, loss_weighting):
    task_table = task_onehot(task_indices)
    env_mean = jnp.dot(task_table, updated_return_mean, precision=lax.Precision.HIGHEST)[:, None]
    env_scale = jnp.dot(task_table, updated_return_scale, precision=lax.Precision.HIGHEST)[:, None]
    logits = head_value_estimates[:, :-1, :ACTIONS]
    norm_values = lax.optimization_barrier(jnp.sum(head_value_estimates[:, :, ACTIONS:] * task_table[:, None, :], axis=2))
    values = lax.stop_gradient(norm_values * env_scale + env_mean)
    log_total = jnp.log(lax.optimization_barrier(jnp.sum(jnp.exp(logits), axis=2)))
    chosen = actions[:, :, None] == jnp.arange(ACTIONS, dtype=jnp.int32)[None, None, :]
    log_policy = lax.optimization_barrier(jnp.sum(jnp.where(chosen, logits, 0.0), axis=2)) - log_total
    clipped = jnp.minimum(jnp.exp(lax.stop_gradient(log_policy) - behaviour_log_prob), 1.0)
    deltas = clipped * (rewards + discount_factors * values[:, 1:] - values[:, :-1])
    targets = values[:, :-1] + discounted_sums(deltas, discount_factors * clipped)
    following = jnp.concatenate([targets[:, 1:], values[:, -1:]], axis=1)
    advantage = lax.stop_gradient(clipped * ((rewards + discount_factors * following - env_mean) / env_scale - norm_values[:, :-1]))
    normed_targets = lax.stop_gradient((targets - env_mean) / env_scale)
    policy = jnp.exp(logits - log_total[:, :, None])
    entropy = -lax.optimization_barrier(jnp.sum(policy * (logits - log_total[:, :, None]), axis=2))
    per_frame = -advantage * log_policy + 0.5 * BASELINE_COST * (normed_targets - norm_values[:, :-1]) ** 2 - ENTROPY_COST * entropy
    return loss_weighting * jnp.sum(per_frame)

def reference(observations, gain, w_in, w_mix, w_out, w_head, head_bias, pop_mean, pop_scale, task_indices, actions, rewards, episode_ends, behaviour_log_prob):
    env_count, frames, full_width = observations.shape
    block_width = full_width // N_TP
    row_count = env_count * frames
    tokens = observations.reshape(row_count, full_width)
    pre_in = jnp.dot(tokens, w_in, preferred_element_type=jnp.float32)
    hidden_in = jax.nn.silu(pre_in).astype(jnp.bfloat16)

    def mix_block(running, block_index):
        hidden_block = lax.dynamic_slice_in_dim(hidden_in, block_index * block_width, block_width, 1)
        weight_block = lax.dynamic_slice_in_dim(w_mix, block_index * block_width, block_width, 0)
        block_product = lax.optimization_barrier(jnp.dot(hidden_block, weight_block, preferred_element_type=jnp.float32).astype(jnp.bfloat16))
        return (running + block_product.astype(jnp.float32), None)
    mix_sum, unused = lax.scan(mix_block, jnp.zeros((row_count, full_width), jnp.float32), jnp.arange(N_TP, dtype=jnp.int32))
    residual = tokens.astype(jnp.float32) + mix_sum
    inverse = lax.rsqrt(lax.optimization_barrier(jnp.mean(residual * residual, axis=1, keepdims=True)) + NORM_EPS)
    normed = (residual * inverse * gain[None, :]).astype(jnp.bfloat16)
    pre_out = jnp.dot(normed, w_out, preferred_element_type=jnp.float32)
    hidden_out = jax.nn.silu(pre_out).astype(jnp.bfloat16)
    discount_factors = DISCOUNT * (1.0 - episode_ends.astype(jnp.float32))
    counts, totals, squares = popart_partials(task_indices, rewards, discount_factors)
    updated_return_mean, updated_return_scale = popart_update(counts, totals, squares, pop_mean, pop_scale)
    new_head, new_bias = rescale_head(w_head, head_bias, pop_mean, pop_scale, updated_return_mean, updated_return_scale)
    head_value_estimates = jnp.dot(hidden_out, new_head, preferred_element_type=jnp.float32) + new_bias[None, :]
    head_value_estimates = head_value_estimates.reshape(env_count, frames, -1)
    loss_weighting = float(ENVS) ** (-0.5)

    def whole_loss(network_outputs):
        return importance_trace_loss(network_outputs, task_indices, actions, rewards, discount_factors, behaviour_log_prob, updated_return_mean, updated_return_scale, loss_weighting)
    loss_value, pullback = jax.vjp(whole_loss, head_value_estimates)
    d_heads, = pullback(jnp.ones((), jnp.float32))
    d_rounded = d_heads.reshape(row_count, -1).astype(jnp.bfloat16)
    grad_head = jnp.dot(hidden_out.T, d_rounded, preferred_element_type=jnp.float32)
    grad_bias = lax.optimization_barrier(jnp.sum(d_rounded.astype(jnp.float32), axis=0))
    d_hidden_out = jnp.dot(d_rounded, new_head.T, preferred_element_type=jnp.float32)
    d_pre_out = (d_hidden_out * silu_slope(pre_out)).astype(jnp.bfloat16)
    grad_out = jnp.dot(normed.T, d_pre_out, preferred_element_type=jnp.float32)

    def back_block(running, block_index):
        grad_block = lax.dynamic_slice_in_dim(d_pre_out, block_index * block_width, block_width, 1)
        weight_block = lax.dynamic_slice_in_dim(w_out, block_index * block_width, block_width, 1)
        block_product = lax.optimization_barrier(jnp.dot(grad_block, weight_block.T, preferred_element_type=jnp.float32).astype(jnp.bfloat16))
        return (running + block_product.astype(jnp.float32), None)
    d_normed, unused = lax.scan(back_block, jnp.zeros((row_count, full_width), jnp.float32), jnp.arange(N_TP, dtype=jnp.int32))
    scaled = d_normed * gain[None, :]
    inner_sum = lax.optimization_barrier(jnp.sum(scaled * residual, axis=1, keepdims=True))
    d_residual = (inverse * scaled - residual * inverse ** 3 * inner_sum / full_width).astype(jnp.bfloat16)
    grad_gain = lax.optimization_barrier(jnp.sum(d_normed * residual * inverse, axis=0))
    grad_mix = jnp.dot(hidden_in.T, d_residual, preferred_element_type=jnp.float32)
    d_hidden_in = jnp.dot(d_residual, w_mix.T, preferred_element_type=jnp.float32)
    d_pre_in = (d_hidden_in * silu_slope(pre_in)).astype(jnp.bfloat16)
    grad_in = jnp.dot(tokens.T, d_pre_in, preferred_element_type=jnp.float32)
    return (grad_in, grad_mix, grad_out, grad_gain, grad_head, grad_bias, new_head, new_bias, updated_return_mean, updated_return_scale)
```

```python
import jax
import jax.numpy as jnp
from jax import lax
from jax.experimental import pallas as pl
from jax.experimental.pallas import tpu as pltpu
from jax.sharding import PartitionSpec as P

ACTIONS = 18
TASKS = 57


DISCOUNT = 0.99
BASELINE_COST = 0.5
ENTROPY_COST = 0.01
POPART_PRIOR = 64.0
NORM_EPS = 1e-06


MESH = pl.DeviceIdType.MESH
F32 = jnp.float32
BF16 = jnp.bfloat16
HALVES = (0, 1)


def plus(a, b, n):
    return lax.rem(a + b, n)


class Place:
    def __init__(self):
        self.me = lax.axis_index("tp")
        self.z = self.me // 4
        self.x = lax.rem(self.me // 2, 2)
        self.c = lax.rem(self.me, 2)
        self.across = self.at(0, 1)
        self.up = self.at(1, 0)
        self.down = self.at(3, 0)
        self.partner = self.at(0, 0, 1)

    def at(self, dz, dx, dc=0):
        return (plus(self.z, dz, 4) * 2 + plus(self.x, dx, 2)) * 2 + plus(self.c, dc, 2)

    def greet(self):
        barrier = pltpu.get_barrier_semaphore()
        peers = (self.across, self.up, self.down, self.partner)
        for peer in peers:
            pl.semaphore_signal(barrier, inc=1, device_id={"tp": peer}, device_id_type=MESH)
        pl.semaphore_wait(barrier, len(peers))


def greet_all(task):
    barrier = pltpu.get_barrier_semaphore()
    me = lax.axis_index("tp")
    for hop in range(1, 16):
        pl.semaphore_signal(
            barrier, inc=1, device_id={"tp": plus(me, hop, 16)}, device_id_type=MESH
        )
    for peer in (task.up, task.down, task.across):
        pl.semaphore_signal(barrier, inc=1, device_id={"task": peer}, device_id_type=MESH)
    pl.semaphore_wait(barrier, 18)


class Wires:
    def __init__(self, send_sems, recv_sems):
        self.send_sems = send_sems
        self.recv_sems = recv_sems
        self.sent = []
        self.slots = 0

    def claim(self, count):
        first = self.slots
        self.slots += count
        return first

    def send(self, src, dst, slot, peer, axis="tp"):
        copy = pltpu.make_async_remote_copy(
            src_ref=src,
            dst_ref=dst,
            send_sem=self.send_sems.at[len(self.sent)],
            recv_sem=self.recv_sems.at[slot],
            device_id={axis: peer},
            device_id_type=MESH,
        )
        copy.start()
        self.sent.append(copy)

    def arrived(self, dst, slot, axis="tp"):
        pltpu.make_async_remote_copy(
            src_ref=dst,
            dst_ref=dst,
            send_sem=self.send_sems.at[0],
            recv_sem=self.recv_sems.at[slot],
            device_id={axis: lax.axis_index(axis)},
            device_id_type=MESH,
        ).wait_recv()

    def drain(self):
        for copy in self.sent:
            copy.wait_send()


class Gather:
    ACROSS, FROM_DOWN, FROM_UP, DOWN_ACROSS, UP_ACROSS, FAR, FAR_ACROSS, OWN = range(8)

    def __init__(self, place, wires, view):
        self.place = place
        self.wires = wires
        self.view = view
        self.first = wires.claim(30)
        p = place
        self.block = {
            self.ACROSS: p.at(0, 1),
            self.FROM_DOWN: p.at(3, 0),
            self.FROM_UP: p.at(1, 0),
            self.DOWN_ACROSS: p.at(3, 1),
            self.UP_ACROSS: p.at(1, 1),
            self.FAR: p.at(2, 0),
            self.FAR_ACROSS: p.at(2, 1),
            self.OWN: p.me,
        }
        self.twin = {k: plus(b, 0, 16) + 1 - 2 * p.c for k, b in self.block.items()}

    def slot(self, kind, half):
        return self.first + kind * 2 + half

    def twin_slot(self, kind, half):
        return self.first + 14 + kind * 2 + half

    def pass_on(self, kind, half, peer, kind_there):
        v = self.view(self.block[kind], half)
        self.wires.send(v, v, self.slot(kind_there, half), peer)

    def to_twin(self, kind, half):
        v = self.view(self.block[kind], half)
        self.wires.send(v, v, self.twin_slot(kind, half), self.place.partner)

    def wait(self, kind, half):
        self.wires.arrived(self.view(self.block[kind], half), self.slot(kind, half))

    def wait_twin(self, *kinds):
        for kind in kinds:
            for half in HALVES:
                self.wires.arrived(
                    self.view(self.twin[kind], half), self.twin_slot(kind, half)
                )

    def open(self):
        p = self.place
        for half in HALVES:
            self.pass_on(self.OWN, half, p.up, self.FROM_DOWN)
            self.pass_on(self.OWN, half, p.down, self.FROM_UP)
            self.pass_on(self.OWN, half, p.across, self.ACROSS)
            self.to_twin(self.OWN, half)

    def middle(self):
        p = self.place
        self.wait(self.FROM_DOWN, 0)
        self.pass_on(self.FROM_DOWN, 0, p.up, self.FAR)
        self.to_twin(self.FROM_DOWN, 0)
        self.wait(self.FROM_UP, 0)
        self.to_twin(self.FROM_UP, 0)
        self.wait(self.ACROSS, 0)
        self.pass_on(self.ACROSS, 0, p.down, self.UP_ACROSS)
        self.wait(self.FROM_UP, 1)
        self.pass_on(self.FROM_UP, 1, p.down, self.FAR)
        self.pass_on(self.ACROSS, 0, p.up, self.DOWN_ACROSS)
        self.to_twin(self.ACROSS, 0)
        self.to_twin(self.FROM_UP, 1)
        self.wait(self.FROM_DOWN, 1)
        self.to_twin(self.FROM_DOWN, 1)
        self.wait(self.ACROSS, 1)
        self.pass_on(self.ACROSS, 1, p.up, self.DOWN_ACROSS)
        self.pass_on(self.ACROSS, 1, p.down, self.UP_ACROSS)
        self.to_twin(self.ACROSS, 1)
        for half in HALVES:
            self.wait(self.FAR, half)
            self.pass_on(self.FAR, half, p.across, self.FAR_ACROSS)
            self.to_twin(self.FAR, half)

    def late(self):
        for half in HALVES:
            for kind in (self.DOWN_ACROSS, self.UP_ACROSS):
                self.wait(kind, half)
                self.to_twin(kind, half)

    def last(self):
        for half in HALVES:
            self.wait(self.FAR_ACROSS, half)
            self.to_twin(self.FAR_ACROSS, half)


def half_cols(half):
    return pl.ds(half * 2048, 2048)


class Scatter:
    G, D, E, F, A, B, C = range(7)
    ORDER = ((2, 1), (1, 1), (3, 1), (1, 0), (3, 0), (2, 0), (0, 1), (0, 0))

    def __init__(self, place, wires, partial, twin_part, landing):
        self.place = place
        self.wires = wires
        self.partial = partial
        self.twin_part = twin_part
        self.landing = landing
        self.first = wires.claim(30)

    def rows(self, where, dc=0):
        return pl.ds(pl.multiple_of(self.place.at(*where, dc) * 32, 32), 32)

    def mine(self, where, half):
        return self.partial.at[self.rows(where), half_cols(half)]

    def twins(self, where, half):
        return self.twin_part.at[self.ORDER.index(where), :, half_cols(half)]

    def land(self, kind, half):
        return self.landing.at[kind, :, half_cols(half)]

    def total(self, where, half, kinds=(), waited=()):
        slot = self.first + 14 + self.ORDER.index(where) * 2 + half
        if (where, half) not in self.seen:
            self.wires.arrived(self.twins(where, half), slot)
            self.seen.add((where, half))
        for kind in kinds:
            self.wires.arrived(self.land(kind, half), self.first + kind * 2 + half)
        value = self.mine(where, half)[...].astype(F32) + self.twins(where, half)[...].astype(F32)
        for kind in kinds:
            value = value + self.land(kind, half)[...].astype(F32)
        return value

    def forward(self, where, half, kinds, peer, kind_there):
        self.mine(where, half)[...] = self.total(where, half, kinds).astype(BF16)
        self.wires.send(
            self.mine(where, half),
            self.land(kind_there, half),
            self.first + kind_there * 2 + half,
            peer,
        )

    def open(self, produce):
        self.seen = set()
        p = self.place
        for half in HALVES:
            produce(half)
            for where in self.ORDER:
                self.wires.send(
                    self.partial.at[self.rows(where, 1), half_cols(half)],
                    self.twins(where, half),
                    self.first + 14 + self.ORDER.index(where) * 2 + half,
                    p.partner,
                )
            self.forward((2, 1), half, (), p.across, self.G)
            self.forward((1, 1), half, (), p.up, self.D)
            self.forward((3, 1), half, (), p.down, self.E)
        self.forward((1, 0), 1, (), p.up, self.B)
        self.forward((3, 0), 0, (), p.down, self.C)

    def finish_far(self):
        p = self.place
        self.forward((2, 0), 0, (self.G,), p.up, self.F)
        self.forward((2, 0), 1, (self.G,), p.down, self.F)

    def finish_across(self):
        for half in HALVES:
            self.forward((0, 1), half, (self.D, self.E), self.place.across, self.A)

    def finish_near(self):
        p = self.place
        self.forward((1, 0), 0, (self.F,), p.up, self.B)
        self.forward((3, 0), 1, (self.F,), p.down, self.C)

    def finish(self, store):
        for half in HALVES:
            store(half, self.total((0, 0), half, (self.A, self.B, self.C)))


def sigmoid(v):
    return 1.0 / (1.0 + jnp.exp(-v))


def dot(a, b, contract=((1,), (0,))):
    return lax.dot_general(a, b, (contract, ((), ())), preferred_element_type=F32)


def load(src, dst, sems, at):
    copy = pltpu.make_async_copy(src, dst, sems.at[at])
    copy.start()
    return copy


def wide_product(left, right, partial, half, transposed):
    def tile(n, carry):
        at = pl.multiple_of(half * 2048 + n * 256, 256)
        if transposed:
            value = dot(left[...], right[pl.ds(at, 256), :], ((1,), (1,)))
        else:
            value = dot(left[...], right[:, pl.ds(at, 256)])
        partial[:, pl.ds(at, 256)] = value.astype(BF16)
        return carry

    lax.fori_loop(0, 8, tile, 0)


def row_view(ref):
    return lambda block, half: ref.at[
        pl.ds(pl.multiple_of(block * 32, 32), 32), half_cols(half)
    ]


def forward_kernel(
    own_tokens, gain, w_in, w_mix,
    tokens_out, pre_in, hidden_in, residual, gain_all, normed_out,
    tokens, w_in_v, w_mix_v, partial, twin_part, landing, normed,
    send_sems, recv_sems, local_sems,
):
    place = Place()
    wires = Wires(send_sems, recv_sems)
    me = place.me
    own_cols = pl.ds(pl.multiple_of(me * 256, 256), 256)
    first = load(own_tokens, tokens.at[pl.ds(0, 512), own_cols], local_sems, 0)
    g = gain[...]
    hi = g.astype(BF16).astype(F32)
    mid = (g - hi).astype(BF16).astype(F32)
    low = g - hi - mid
    row = lax.broadcasted_iota(jnp.int32, (16, 256), 0)
    rows = jnp.where(row == 0, hi, jnp.where(row == 1, mid, jnp.where(row == 2, low, 0.0)))
    tokens[pl.ds(512, 16), own_cols] = rows.astype(BF16)
    place.greet()
    first.wait()

    def token_view(block, half):
        rows = pl.ds(0, 256) if half == 0 else pl.ds(256, 272)
        return tokens.at[rows, pl.ds(pl.multiple_of(block * 256, 256), 256)]

    gather = Gather(place, wires, token_view)
    gather.open()
    get_in = load(w_in, w_in_v, local_sems, 1)
    get_mix = load(w_mix, w_mix_v, local_sems, 2)
    gather.middle()

    def slab(dz, opening=False):
        at = pl.multiple_of(plus(place.z, dz, 4) * 1024, 1024)

        def tile(m, carry):
            r = pl.ds(pl.multiple_of(m * 128, 128), 128)
            value = dot(tokens[r, pl.ds(at, 1024)], w_in_v[pl.ds(at, 1024), :])
            pre_in[r, :] = value if opening else pre_in[r, :] + value
            return carry

        lax.fori_loop(0, 4, tile, 0)

    get_in.wait()
    gather.wait_twin(gather.OWN, gather.ACROSS)
    slab(0, True)
    gather.late()
    gather.wait_twin(gather.FROM_UP, gather.UP_ACROSS)
    slab(1)
    gather.last()
    gather.wait_twin(gather.FROM_DOWN, gather.DOWN_ACROSS)
    slab(3)
    gather.wait_twin(gather.FAR, gather.FAR_ACROSS)
    slab(2)
    keep = load(tokens.at[pl.ds(0, 512), :], tokens_out, local_sems, 3)

    def activate(m, carry):
        r = pl.ds(pl.multiple_of(m * 128, 128), 128)
        v = pre_in[r, :]
        hidden_in[r, :] = (v * sigmoid(v)).astype(BF16)
        return carry

    lax.fori_loop(0, 4, activate, 0)
    g3 = tokens[pl.ds(512, 16), :].astype(F32)
    gain_all[...] = g3[0:1, :] + g3[1:2, :] + g3[2:3, :]
    get_mix.wait()
    scatter = Scatter(place, wires, partial, twin_part, landing)
    scatter.open(lambda half: wide_product(hidden_in, w_mix_v, partial, half, False))
    own_rows = pl.ds(pl.multiple_of(me * 32, 32), 32)

    def store(half, value):
        residual[:, half_cols(half)] = (
            value + tokens[own_rows, half_cols(half)].astype(F32)
        )

    scatter.finish_far()
    scatter.finish_across()
    scatter.finish_near()
    scatter.finish(store)
    for m in range(2):
        v = residual[pl.ds(m * 16, 16), :]
        inverse = lax.rsqrt(jnp.mean(v * v, axis=1, keepdims=True) + NORM_EPS)
        normed[pl.ds(pl.multiple_of(me * 32 + m * 16, 16), 16), :] = (
            v * inverse * gain_all[...]
        ).astype(BF16)
    spread = Gather(place, wires, row_view(normed))
    spread.open()
    spread.middle()
    spread.late()
    spread.last()
    spread.wait_twin(*range(8))
    out = load(normed, normed_out, local_sems, 4)
    keep.wait()
    out.wait()
    wires.drain()


class TaskPlace:
    def __init__(self):
        task = lax.axis_index("task")
        self.xh = task // 4
        self.y = lax.rem(task, 4)
        self.up = self.xh * 4 + plus(self.y, 1, 4)
        self.down = self.xh * 4 + plus(self.y, 3, 4)
        self.across = (1 - self.xh) * 4 + self.y


class TaskSum:
    F, B, C = range(3)
    OWN, FROM_DOWN, FROM_UP, DOWN_ACROSS, UP_ACROSS, FAR, FAR_ACROSS = range(7)

    def __init__(self, place, wires, view, whole, land, land_x, result):
        self.place = place
        self.wires = wires
        self.view = view
        self.whole = whole
        self.land = land
        self.land_x = land_x
        self.result = result
        self.first = wires.claim(14)

    def slab(self, ref, dy, part):
        return self.view(ref, plus(self.place.y, dy, 4) * 2 + part)

    def post(self, src, dst, slot, peer):
        self.wires.send(src, dst, self.first + slot, peer, "task")

    def wait(self, dst, slot):
        self.wires.arrived(dst, self.first + slot, "task")

    def far(self):
        p = self.place
        self.post(self.slab(self.whole, 2, 0), self.land.at[self.F, 0], 0, p.up)
        self.post(self.slab(self.whole, 2, 1), self.land.at[self.F, 1], 1, p.down)

    def near(self):
        p = self.place
        self.post(self.slab(self.whole, 1, 1), self.land.at[self.B, 1], 3, p.up)
        self.post(self.slab(self.whole, 3, 0), self.land.at[self.C, 0], 4, p.down)

    def relay(self):
        p = self.place
        for dy, part, kind, slot, peer in ((1, 0, self.B, 2, p.up), (3, 1, self.C, 5, p.down)):
            self.wait(self.land.at[self.F, part], part)
            own = self.slab(self.whole, dy, part)
            total = own[...].astype(F32) + self.land[self.F, part].astype(F32)
            own[...] = total.astype(BF16)
            self.post(own, self.land.at[kind, part], slot, peer)

    def local(self, part):
        return (
            self.slab(self.whole, 0, part)[...].astype(F32)
            + self.land[self.B, part].astype(F32)
            + self.land[self.C, part].astype(F32)
        )

    def fold(self):
        for kind, part, slot in ((self.B, 1, 3), (self.C, 0, 4), (self.B, 0, 2), (self.C, 1, 5)):
            self.wait(self.land.at[kind, part], slot)
        other = 1 - self.place.xh
        away = self.slab(self.whole, 0, other)
        away[...] = self.local(other).astype(BF16)
        self.post(away, self.land_x, 6, self.place.across)

    def pass_on(self, kind, peer, kind_there):
        v = self.held(kind)
        self.post(v, v, 6 + kind_there, peer)

    def held(self, kind):
        dy, across = {
            self.OWN: (0, 0),
            self.FROM_DOWN: (3, 0),
            self.FROM_UP: (1, 0),
            self.DOWN_ACROSS: (3, 1),
            self.UP_ACROSS: (1, 1),
            self.FAR: (2, 0),
            self.FAR_ACROSS: (2, 1),
        }[kind]
        xh = self.place.xh
        return self.slab(self.result, dy, 1 - xh if across else xh)

    def across_held(self):
        return self.slab(self.result, 0, 1 - self.place.xh)

    def finish(self):
        p = self.place
        self.wait(self.land_x, 6)
        own = self.held(self.OWN)
        own[...] = (self.local(p.xh) + self.land_x[...].astype(F32)).astype(BF16)
        self.post(own, own, 13, p.across)
        self.pass_on(self.OWN, p.up, self.FROM_DOWN)
        self.pass_on(self.OWN, p.down, self.FROM_UP)

    def get(self, kind):
        self.wait(self.held(kind), 6 + kind)

    def spread(self):
        p = self.place
        self.get(self.FROM_DOWN)
        self.pass_on(self.FROM_DOWN, p.up, self.FAR)
        self.get(self.FROM_UP)
        v = self.across_held()
        self.wait(v, 13)
        self.post(v, v, 6 + self.DOWN_ACROSS, p.up)
        self.post(v, v, 6 + self.UP_ACROSS, p.down)

    def spread_far(self):
        self.get(self.UP_ACROSS)
        self.pass_on(self.UP_ACROSS, self.place.down, self.FAR_ACROSS)
        self.get(self.DOWN_ACROSS)

    def end(self):
        self.get(self.FAR)
        self.get(self.FAR_ACROSS)


def slope(v):
    s = sigmoid(v)
    return s * (1.0 + v * (1.0 - s))


def slab_rows(height):
    return lambda ref, n: ref.at[pl.ds(pl.multiple_of(n * height, 16), height), :]


def slab_cols(ref, n):
    return ref.at[:, pl.ds(pl.multiple_of(n * 512, 512), 512)]


def backward_kernel(
    d_heads, new_head, hidden_out, pre_out, w_out, w_mix, residual, gain_all, hidden_in, pre_in,
    tokens_in, normed_in,
    sum_out, sum_mix, sum_in,
    w_out_v, w_mix_v, tokens, normed, d_pre_out, d_pre_in, hidden_t, d_normed,
    partial, twin_part, landing, arrived, gain_parts, gain_land,
    whole_out, whole_mix, whole_in, land_out, land_mix, land_in, x_out, x_mix, x_in,
    send_sems, recv_sems, local_sems,
):
    place = Place()
    task = TaskPlace()
    wires = Wires(send_sems, recv_sems)
    me = place.me
    get_out = load(w_out, w_out_v, local_sems, 0)
    get_normed = load(normed_in, normed, local_sems, 1)
    get_mix = load(w_mix, w_mix_v, local_sems, 2)
    get_tokens = load(tokens_in, tokens, local_sems, 3)
    greet_all(task)

    d_hidden = dot(d_heads[...], new_head[...], ((1,), (1,)))
    d_pre_out[...] = (d_hidden * slope(pre_out[...])).astype(BF16)
    get_out.wait()
    scatter = Scatter(place, wires, partial, twin_part, landing)
    scatter.open(lambda half: wide_product(d_pre_out, w_out_v, partial, half, True))
    for_out = TaskSum(task, wires, slab_rows(512), whole_out, land_out, x_out, sum_out)
    for_mix = TaskSum(task, wires, slab_cols, whole_mix, land_mix, x_mix, sum_mix)
    for_in = TaskSum(task, wires, slab_rows(528), whole_in, land_in, x_in, sum_in)

    def tall_product(left, right, whole, height, dy):
        k = plus(task.y, dy, 4)

        def tile(n, carry):
            feature = pl.multiple_of(k * 1024 + n * 256, 256)
            at = pl.multiple_of((k * 2 + n // 2) * height + lax.rem(n, 2) * 256, 16)
            value = dot(left[:, pl.ds(feature, 256)], right[...], ((0,), (0,)))
            whole[pl.ds(at, 256), :] = value.astype(BF16)
            return carry

        lax.fori_loop(0, 4, tile, 0)

    def mix_product(dy):
        k = plus(task.y, dy, 4)

        def tile(n, carry):
            at = pl.multiple_of(k * 1024 + n * 256, 256)
            whole_mix[:, pl.ds(at, 256)] = dot(hidden_t[...], arrived[:, pl.ds(at, 256)]).astype(BF16)
            return carry

        lax.fori_loop(0, 4, tile, 0)

    def out_product(dy):
        tall_product(normed, d_pre_out, whole_out, 512, dy)

    def in_product(dy):
        tall_product(tokens, d_pre_in, whole_in, 528, dy)

    get_normed.wait()
    out_product(2)
    for_out.far()
    scatter.finish_far()
    out_product(1)
    out_product(3)
    for_out.near()
    scatter.finish_across()
    out_product(0)
    scatter.finish_near()
    hidden_t[...] = hidden_in[...].T
    for_out.relay()

    def store(half, value):
        d_normed[:, half_cols(half)] = value

    scatter.finish(store)
    gain_rows = jnp.zeros((8, 4096), F32)
    for m in range(2):
        r = pl.ds(m * 16, 16)
        v = residual[r, :]
        inverse = lax.rsqrt(jnp.mean(v * v, axis=1, keepdims=True) + NORM_EPS)
        d = d_normed[r, :]
        scaled = d * gain_all[...]
        inner = jnp.sum(scaled * v, axis=1, keepdims=True)
        step = inverse * scaled - v * (inverse * inverse * inverse * inner * (1.0 / 4096))
        arrived[pl.ds(pl.multiple_of(me * 32 + m * 16, 16), 16), :] = step.astype(BF16)
        d_normed[r, :] = d * v * inverse
    gather = Gather(place, wires, row_view(arrived))
    gather.open()
    for m in range(4):
        gain_rows = gain_rows + d_normed[pl.ds(m * 8, 8), :]
    for n in range(16):
        gain_parts[n] = gain_rows[:, n * 256 : n * 256 + 256]
    for_out.fold()
    gain_slot = wires.claim(15)
    for hop in range(1, 16):
        peer = plus(me, hop, 16)
        wires.send(gain_parts.at[peer], gain_land.at[hop - 1], gain_slot + hop - 1, peer)
    gather.middle()
    get_mix.wait()

    def hidden_slab(dz):
        rows = pl.ds(pl.multiple_of(plus(place.z, dz, 4) * 128, 128), 128)
        d = dot(arrived[rows, :], w_mix_v[...], ((1,), (1,)))
        d_pre_in[rows, :] = (d * slope(pre_in[rows, :])).astype(BF16)

    gather.wait_twin(gather.OWN, gather.ACROSS)
    hidden_slab(0)
    gather.late()
    for_out.finish()
    gather.wait_twin(gather.FROM_UP, gather.UP_ACROSS)
    hidden_slab(1)
    gather.last()
    gather.wait_twin(gather.FROM_DOWN, gather.DOWN_ACROSS)
    hidden_slab(3)
    gather.wait_twin(gather.FAR, gather.FAR_ACROSS)
    mix_product(2)
    for_mix.far()
    hidden_slab(2)
    mix_product(1)
    mix_product(3)
    for_mix.near()
    for_out.spread()
    mix_product(0)
    get_tokens.wait()
    in_product(2)
    small = dot(d_heads[...], hidden_out[...], ((0,), (0,)))
    bias = jnp.sum(d_heads[...].astype(F32), axis=0, keepdims=True)
    gain_total = jnp.sum(gain_parts[me], axis=0, keepdims=True)
    for hop in range(1, 16):
        wires.arrived(gain_land.at[hop - 1], gain_slot + hop - 1)
        gain_total = gain_total + jnp.sum(gain_land[hop - 1], axis=0, keepdims=True)
    row = lax.broadcasted_iota(jnp.int32, (128, 256), 0)
    bias = jnp.concatenate([bias, jnp.zeros((1, 128), F32)], axis=1)
    small = jnp.where(row == 80, bias, jnp.where(row == 88, gain_total, small)).astype(BF16)
    for n in range(8):
        whole_in[pl.ds(n * 528 + 512, 16), :] = small[n * 16 : n * 16 + 16, :]
    for_in.far()
    in_product(1)
    in_product(3)
    for_in.near()
    for_mix.relay()
    in_product(0)
    for_out.spread_far()
    for_in.relay()
    for_mix.fold()
    for_out.end()
    for_in.fold()
    for_mix.finish()
    for_mix.spread()
    for_in.finish()
    for_mix.spread_far()
    for_in.spread()
    for_mix.end()
    for_in.spread_far()
    for_in.end()
    wires.drain()


def hbm():
    return pl.BlockSpec(memory_space=pltpu.HBM)


def vmem():
    return pl.BlockSpec(memory_space=pltpu.VMEM)


def exchange_scratch():
    return [
        pltpu.VMEM((512, 4096), BF16),
        pltpu.VMEM((8, 32, 4096), BF16),
        pltpu.VMEM((7, 32, 4096), BF16),
        pltpu.VMEM((512, 4096), BF16),
    ]


def parameters(collective_id):
    return pltpu.CompilerParams(
        collective_id=collective_id, has_side_effects=True, vmem_limit_bytes=62 * 2**20
    )


def forward_call(own_tokens, gain, w_in, w_mix):
    return pl.pallas_call(
        forward_kernel,
        out_shape=[
            jax.ShapeDtypeStruct((512, 4096), BF16),
            jax.ShapeDtypeStruct((512, 256), F32),
            jax.ShapeDtypeStruct((512, 256), BF16),
            jax.ShapeDtypeStruct((32, 4096), F32),
            jax.ShapeDtypeStruct((1, 4096), F32),
            jax.ShapeDtypeStruct((512, 4096), BF16),
        ],
        in_specs=[hbm(), vmem(), hbm(), hbm()],
        out_specs=[hbm(), vmem(), vmem(), vmem(), vmem(), hbm()],
        scratch_shapes=[
            pltpu.VMEM((528, 4096), BF16),
            pltpu.VMEM((4096, 256), BF16),
            pltpu.VMEM((256, 4096), BF16),
            *exchange_scratch(),
            pltpu.SemaphoreType.DMA((96,)),
            pltpu.SemaphoreType.DMA((96,)),
            pltpu.SemaphoreType.DMA((5,)),
        ],
        compiler_params=parameters(0),
        name="forward",
    )(own_tokens, gain, w_in, w_mix)


def backward_call(
    d_heads, new_head, hidden_out, pre_out, w_out, w_mix, residual, gain_all, hidden_in, pre_in,
    tokens, normed,
):
    v, h = vmem(), hbm()
    return pl.pallas_call(
        backward_kernel,
        out_shape=[
            jax.ShapeDtypeStruct((4096, 256), BF16),
            jax.ShapeDtypeStruct((256, 4096), BF16),
            jax.ShapeDtypeStruct((4224, 256), BF16),
        ],
        in_specs=[v, v, v, v, h, h, v, v, v, v, h, h],
        out_specs=[v, v, v],
        scratch_shapes=[
            pltpu.VMEM((4096, 256), BF16),
            pltpu.VMEM((256, 4096), BF16),
            pltpu.VMEM((512, 4096), BF16),
            pltpu.VMEM((512, 4096), BF16),
            pltpu.VMEM((512, 256), BF16),
            pltpu.VMEM((512, 256), BF16),
            pltpu.VMEM((256, 512), BF16),
            pltpu.VMEM((32, 4096), F32),
            *exchange_scratch(),
            pltpu.VMEM((16, 8, 256), F32),
            pltpu.VMEM((15, 8, 256), F32),
            pltpu.VMEM((4096, 256), BF16),
            pltpu.VMEM((256, 4096), BF16),
            pltpu.VMEM((4224, 256), BF16),
            pltpu.VMEM((3, 2, 512, 256), BF16),
            pltpu.VMEM((3, 2, 256, 512), BF16),
            pltpu.VMEM((3, 2, 528, 256), BF16),
            pltpu.VMEM((512, 256), BF16),
            pltpu.VMEM((256, 512), BF16),
            pltpu.VMEM((528, 256), BF16),
            pltpu.SemaphoreType.DMA((128,)),
            pltpu.SemaphoreType.DMA((128,)),
            pltpu.SemaphoreType.DMA((4,)),
        ],
        compiler_params=parameters(1),
        name="backward",
    )(
        d_heads, new_head, hidden_out, pre_out, w_out, w_mix, residual, gain_all, hidden_in,
        pre_in, tokens, normed,
    )


def sent_to_all(value, axis):
    copies = jnp.broadcast_to(value, (lax.axis_size(axis), *value.shape))
    return lax.all_to_all(copies, axis, split_axis=0, concat_axis=0, tiled=True)


def of_everyone(value, axis):
    everything = sent_to_all(value, axis)
    return jnp.sum(everything, axis=0)


def packed_total(arrays, axis):
    line, at, gathered = (jnp.concatenate([a.reshape(-1) for a in arrays]), 0, [])
    subtotal = of_everyone(line, axis)
    for a in arrays:
        gathered.append(subtotal[at : at + a.size].reshape(a.shape))
        at += a.size
    return tuple(gathered)


def cut_along(value, dim, devices):
    before, after = (value.shape[:dim], value.shape[dim + 1 :])
    return jnp.moveaxis(value.reshape(*before, devices, -1, *after), dim, 0)


def sum_at_owner(value, axis, dim):
    parts = cut_along(value, dim, lax.axis_size(axis))
    arrived = lax.all_to_all(parts, axis, split_axis=0, concat_axis=0, tiled=True)
    return arrived.astype(jnp.float32).sum(axis=0)


def joined_along(parts, dim):
    dims = list(parts.shape[1:])
    dims[dim] *= parts.shape[0]
    return jnp.moveaxis(parts, 0, dim).reshape(dims)


def gathered_copies(value, axis, dim):
    parts = sent_to_all(value, axis)
    return joined_along(parts, dim)


def discounted_sums(values, factors):

    def advance(running, column):
        latest = column[0] + column[1] * running
        return (latest, latest)

    opening = jnp.zeros((values.shape[0],), jnp.float32)
    ending, stacked = lax.scan(advance, opening, (values.T, factors.T), reverse=True)
    return stacked.T


def task_onehot(task_indices):
    return (task_indices[:, None] == jnp.arange(TASKS, dtype=jnp.int32)[None, :]).astype(
        jnp.float32
    )


def popart_partials(task_indices, rewards, discount_factors):
    returns = discounted_sums(rewards, discount_factors)
    task_table = task_onehot(task_indices)
    counts = jnp.sum(task_table, axis=0) * rewards.shape[1]
    totals = jnp.dot(task_table.T, jnp.sum(returns, axis=1))
    squares = jnp.dot(task_table.T, jnp.sum(returns * returns, axis=1))
    return (counts, totals, squares)


def popart_update(counts, totals, squares, pop_mean, pop_scale):
    mixing = counts / (counts + POPART_PRIOR)
    safe_counts = jnp.maximum(counts, 1.0)
    batch_mean = totals / safe_counts
    batch_square = squares / safe_counts
    updated_return_mean = (1.0 - mixing) * pop_mean + mixing * batch_mean
    mean_gap = batch_mean - pop_mean
    variance = (
        (1.0 - mixing) * pop_scale * pop_scale
        + mixing * (batch_square - batch_mean * batch_mean)
        + mixing * (1.0 - mixing) * mean_gap * mean_gap
    )
    return (updated_return_mean, jnp.sqrt(variance))


def rescale_head(w_head, head_bias, pop_mean, pop_scale, updated_return_mean, updated_return_scale):
    scale_ratio = pop_scale / updated_return_scale
    column_scale = jnp.concatenate([jnp.ones((ACTIONS,), jnp.float32), scale_ratio])
    new_head = (w_head.astype(jnp.float32) * column_scale[None, :]).astype(jnp.bfloat16)
    value_bias = (
        pop_scale * head_bias[ACTIONS:] + pop_mean - updated_return_mean
    ) / updated_return_scale
    new_bias = jnp.concatenate([head_bias[:ACTIONS], value_bias])
    return (new_head, new_bias)


def importance_trace_loss(
    head_value_estimates,
    task_indices,
    actions,
    rewards,
    discount_factors,
    behaviour_log_prob,
    updated_return_mean,
    updated_return_scale,
    loss_weighting,
):
    task_table = task_onehot(task_indices)
    env_mean = jnp.dot(task_table, updated_return_mean)[:, None]
    env_scale = jnp.dot(task_table, updated_return_scale)[:, None]
    logits = head_value_estimates[:, :-1, :ACTIONS]
    norm_values = jnp.sum(head_value_estimates[:, :, ACTIONS:] * task_table[:, None, :], axis=2)
    values = lax.stop_gradient(norm_values * env_scale + env_mean)
    log_total = jnp.log(jnp.sum(jnp.exp(logits), axis=2))
    chosen = actions[:, :, None] == jnp.arange(ACTIONS, dtype=jnp.int32)[None, None, :]
    log_policy = jnp.sum(jnp.where(chosen, logits, 0.0), axis=2) - log_total
    clipped = jnp.minimum(jnp.exp(lax.stop_gradient(log_policy) - behaviour_log_prob), 1.0)
    deltas = clipped * (rewards + discount_factors * values[:, 1:] - values[:, :-1])
    targets = values[:, :-1] + discounted_sums(deltas, discount_factors * clipped)
    following = jnp.concatenate([targets[:, 1:], values[:, -1:]], axis=1)
    advantage = lax.stop_gradient(
        clipped
        * ((rewards + discount_factors * following - env_mean) / env_scale - norm_values[:, :-1])
    )
    normed_targets = lax.stop_gradient((targets - env_mean) / env_scale)
    policy = jnp.exp(logits - log_total[:, :, None])
    entropy = -jnp.sum(policy * (logits - log_total[:, :, None]), axis=2)
    per_frame = (
        -advantage * log_policy
        + 0.5 * BASELINE_COST * (normed_targets - norm_values[:, :-1]) ** 2
        - ENTROPY_COST * entropy
    )
    return loss_weighting * jnp.sum(per_frame)


def on_device(
    observations,
    gain,
    w_in,
    w_mix,
    w_out,
    w_head,
    head_bias,
    pop_mean,
    pop_scale,
    task_indices,
    actions,
    rewards,
    episode_ends,
    behaviour_log_prob,
):
    env_count, frames, part_width = observations.shape
    groups = lax.axis_size("tp")
    full_width = part_width * groups
    row_count = env_count * frames
    own_tokens = observations.reshape(row_count, part_width)
    discount_factors = DISCOUNT * (1.0 - episode_ends.astype(jnp.float32))
    counts, totals, squares = popart_partials(task_indices, rewards, discount_factors)
    counts, totals, squares = packed_total((counts, totals, squares), "task")
    updated_return_mean, updated_return_scale = popart_update(
        counts, totals, squares, pop_mean, pop_scale
    )
    new_head, new_bias = rescale_head(
        w_head, head_bias, pop_mean, pop_scale, updated_return_mean, updated_return_scale
    )
    loss_weighting = float(env_count * lax.axis_size("task")) ** (-0.5)
    tokens, pre_in, hidden_in, residual, gain_all, normed_all = forward_call(
        own_tokens, gain.reshape(1, part_width), w_in, w_mix
    )
    pre_out = jnp.dot(normed_all, w_out, preferred_element_type=jnp.float32)
    hidden_out = jax.nn.silu(pre_out).astype(jnp.bfloat16)
    head_terms = jnp.dot(hidden_out, new_head, preferred_element_type=jnp.float32)
    env_share = env_count // groups
    env_offset = lax.axis_index("tp") * env_share

    def select_envs(source):
        return lax.dynamic_slice_in_dim(source, env_offset, env_share, 0)

    head_value_estimates = (
        sum_at_owner(head_terms.astype(jnp.bfloat16), "tp", 0) + new_bias[None, :]
    )
    head_value_estimates = head_value_estimates.reshape(env_share, frames, -1)

    def share_loss(network_outputs):
        return importance_trace_loss(
            network_outputs,
            select_envs(task_indices),
            select_envs(actions),
            select_envs(rewards),
            select_envs(discount_factors),
            select_envs(behaviour_log_prob),
            updated_return_mean,
            updated_return_scale,
            loss_weighting,
        )

    loss_value, pullback = jax.vjp(share_loss, head_value_estimates)
    (d_heads,) = pullback(jnp.ones((), jnp.float32))
    d_local = d_heads.reshape(env_share * frames, -1).astype(jnp.bfloat16)
    d_rounded = gathered_copies(d_local, "tp", 0)
    pad = ((0, 0), (0, 128 - d_rounded.shape[1]))
    sum_out, sum_mix, sum_in = backward_call(
        jnp.pad(d_rounded, pad),
        jnp.pad(new_head, pad),
        hidden_out,
        pre_out,
        w_out,
        w_mix,
        residual,
        gain_all,
        hidden_in,
        pre_in,
        tokens,
        normed_all,
    )
    sum_in = sum_in.reshape(8, 528, part_width)
    grad_in = sum_in[:, :512].astype(jnp.float32).reshape(full_width, part_width)
    small = sum_in[:, 512:].astype(jnp.float32).reshape(128, part_width)
    grad_head = small[: ACTIONS + TASKS].T
    grad_bias = small[80, : ACTIONS + TASKS]
    grad_gain = small[88]
    grad_out, grad_mix = sum_out.astype(jnp.float32), sum_mix.astype(jnp.float32)
    return (
        grad_in,
        grad_mix,
        grad_out,
        grad_gain,
        grad_head,
        grad_bias,
        new_head,
        new_bias,
        updated_return_mean,
        updated_return_scale,
    )


def solution(mesh):
    in_specs = (
        P("task", None, "tp"),
        P("tp"),
        P(None, "tp"),
        P("tp", None),
        P(None, "tp"),
        P("tp", None),
        P(),
        P(),
        P(),
        P("task"),
        P("task", None),
        P("task", None),
        P("task", None),
        P("task", None),
    )
    out_specs = (
        P(None, "tp"),
        P("tp", None),
        P(None, "tp"),
        P("tp"),
        P("tp", None),
        P(),
        P("tp", None),
        P(),
        P(),
        P(),
    )
    return jax.shard_map(
        on_device, mesh=mesh, in_specs=in_specs, out_specs=out_specs, check_vma=False
    )
```

```python
import jax
import jax.numpy as jnp
from jax import lax
from jax.experimental import pallas as pl
from jax.experimental.pallas import tpu as pltpu
from jax.sharding import PartitionSpec as P

ACTIONS = 18
TASKS = 57
DISCOUNT = 0.99
BASELINE_COST = 0.5
ENTROPY_COST = 0.01
POPART_PRIOR = 64.0
NORM_EPS = 1e-06
LOSS_WEIGHT = 256**-0.5
SENDS = 248
RECEIVES = 248


MESH = pl.DeviceIdType.MESH
F32 = jnp.float32
BF16 = jnp.bfloat16
HALVES = (0, 1)


def plus(a, b, n):
    return lax.rem(a + b, n)


class Place:
    def __init__(self):
        self.me = lax.axis_index("tp")
        self.z = self.me // 4
        self.x = lax.rem(self.me // 2, 2)
        self.c = lax.rem(self.me, 2)
        self.across = self.at(0, 1)
        self.up = self.at(1, 0)
        self.down = self.at(3, 0)
        self.partner = self.at(0, 0, 1)

    def at(self, dz, dx, dc=0):
        return (plus(self.z, dz, 4) * 2 + plus(self.x, dx, 2)) * 2 + plus(self.c, dc, 2)


class Wires:
    def __init__(self, send_sems, recv_sems):
        self.send_sems = send_sems
        self.recv_sems = recv_sems
        self.sent = []
        self.drained = 0
        self.slots = 0

    def claim(self, count):
        first = self.slots
        self.slots += count
        return first

    def send(self, src, dst, slot, peer, axis="tp"):
        copy = pltpu.make_async_remote_copy(
            src_ref=src,
            dst_ref=dst,
            send_sem=self.send_sems.at[len(self.sent)],
            recv_sem=self.recv_sems.at[slot],
            device_id={axis: peer},
            device_id_type=MESH,
        )
        copy.start()
        self.sent.append(copy)

    def arrived(self, dst, slot, axis="tp"):
        pltpu.make_async_remote_copy(
            src_ref=dst,
            dst_ref=dst,
            send_sem=self.send_sems.at[0],
            recv_sem=self.recv_sems.at[slot],
            device_id={axis: lax.axis_index(axis)},
            device_id_type=MESH,
        ).wait_recv()

    def drain_all_but(self, last):
        for copy in self.sent[: len(self.sent) - last]:
            copy.wait_send()
        self.drained = len(self.sent) - last

    def drain(self):
        for copy in self.sent[self.drained :]:
            copy.wait_send()


class Gather:
    ACROSS, FROM_DOWN, FROM_UP, DOWN_ACROSS, UP_ACROSS, FAR, FAR_ACROSS, OWN = range(8)

    def __init__(self, place, wires, view):
        self.place = place
        self.wires = wires
        self.view = view
        self.first = wires.claim(30)
        p = place
        self.block = {
            self.ACROSS: p.at(0, 1),
            self.FROM_DOWN: p.at(3, 0),
            self.FROM_UP: p.at(1, 0),
            self.DOWN_ACROSS: p.at(3, 1),
            self.UP_ACROSS: p.at(1, 1),
            self.FAR: p.at(2, 0),
            self.FAR_ACROSS: p.at(2, 1),
            self.OWN: p.me,
        }
        self.twin = {k: plus(b, 0, 16) + 1 - 2 * p.c for k, b in self.block.items()}

    def slot(self, kind, half):
        return self.first + kind * 2 + half

    def twin_slot(self, kind, half):
        return self.first + 14 + kind * 2 + half

    def pass_on(self, kind, half, peer, kind_there):
        v = self.view(self.block[kind], half)
        self.wires.send(v, v, self.slot(kind_there, half), peer)

    def to_twin(self, kind, half):
        v = self.view(self.block[kind], half)
        self.wires.send(v, v, self.twin_slot(kind, half), self.place.partner)

    def wait(self, kind, half):
        self.wires.arrived(self.view(self.block[kind], half), self.slot(kind, half))

    def wait_twin(self, *kinds):
        for kind in kinds:
            for half in HALVES:
                self.wires.arrived(
                    self.view(self.twin[kind], half), self.twin_slot(kind, half)
                )

    def open(self):
        p = self.place
        for half in HALVES:
            self.pass_on(self.OWN, half, p.up, self.FROM_DOWN)
            self.pass_on(self.OWN, half, p.down, self.FROM_UP)
            self.pass_on(self.OWN, half, p.across, self.ACROSS)
            self.to_twin(self.OWN, half)

    def middle(self):
        p = self.place
        self.wait(self.FROM_DOWN, 0)
        self.pass_on(self.FROM_DOWN, 0, p.up, self.FAR)
        self.to_twin(self.FROM_DOWN, 0)
        self.wait(self.FROM_UP, 0)
        self.to_twin(self.FROM_UP, 0)
        self.wait(self.ACROSS, 0)
        self.pass_on(self.ACROSS, 0, p.down, self.UP_ACROSS)
        self.wait(self.FROM_UP, 1)
        self.pass_on(self.FROM_UP, 1, p.down, self.FAR)
        self.pass_on(self.ACROSS, 0, p.up, self.DOWN_ACROSS)
        self.to_twin(self.ACROSS, 0)
        self.to_twin(self.FROM_UP, 1)
        self.wait(self.FROM_DOWN, 1)
        self.to_twin(self.FROM_DOWN, 1)
        self.wait(self.ACROSS, 1)
        self.pass_on(self.ACROSS, 1, p.up, self.DOWN_ACROSS)
        self.pass_on(self.ACROSS, 1, p.down, self.UP_ACROSS)
        self.to_twin(self.ACROSS, 1)
        for half in HALVES:
            self.wait(self.FAR, half)
            self.pass_on(self.FAR, half, p.across, self.FAR_ACROSS)
            self.to_twin(self.FAR, half)

    def late(self):
        for half in HALVES:
            for kind in (self.DOWN_ACROSS, self.UP_ACROSS):
                self.wait(kind, half)
                self.to_twin(kind, half)

    def last(self):
        for half in HALVES:
            self.wait(self.FAR_ACROSS, half)
            self.to_twin(self.FAR_ACROSS, half)


def half_cols(half):
    return pl.ds(half * 2048, 2048)


class Scatter:
    G, D, E, F, A, B, C = range(7)
    ORDER = ((2, 1), (1, 1), (3, 1), (1, 0), (3, 0), (2, 0), (0, 1), (0, 0))

    def __init__(self, place, wires, partial, twin_part, landing):
        self.place = place
        self.wires = wires
        self.partial = partial
        self.twin_part = twin_part
        self.landing = landing
        self.first = wires.claim(30)

    def rows(self, where, dc=0):
        return pl.ds(pl.multiple_of(self.place.at(*where, dc) * 32, 32), 32)

    def mine(self, where, half):
        return self.partial.at[self.rows(where), half_cols(half)]

    def twins(self, where, half):
        return self.twin_part.at[self.ORDER.index(where), :, half_cols(half)]

    def land(self, kind, half):
        return self.landing.at[kind, :, half_cols(half)]

    def total(self, where, half, kinds=(), waited=()):
        slot = self.first + 14 + self.ORDER.index(where) * 2 + half
        if (where, half) not in self.seen:
            self.wires.arrived(self.twins(where, half), slot)
            self.seen.add((where, half))
        for kind in kinds:
            self.wires.arrived(self.land(kind, half), self.first + kind * 2 + half)
        value = self.mine(where, half)[...].astype(F32) + self.twins(where, half)[...].astype(F32)
        for kind in kinds:
            value = value + self.land(kind, half)[...].astype(F32)
        return value

    def forward(self, where, half, kinds, peer, kind_there):
        self.mine(where, half)[...] = self.total(where, half, kinds).astype(BF16)
        self.wires.send(
            self.mine(where, half),
            self.land(kind_there, half),
            self.first + kind_there * 2 + half,
            peer,
        )

    def open(self, produce):
        self.seen = set()
        p = self.place
        for half in HALVES:
            produce(half)
            for where in self.ORDER:
                self.wires.send(
                    self.partial.at[self.rows(where, 1), half_cols(half)],
                    self.twins(where, half),
                    self.first + 14 + self.ORDER.index(where) * 2 + half,
                    p.partner,
                )
            self.forward((2, 1), half, (), p.across, self.G)
            self.forward((1, 1), half, (), p.up, self.D)
            self.forward((3, 1), half, (), p.down, self.E)
        self.forward((1, 0), 1, (), p.up, self.B)
        self.forward((3, 0), 0, (), p.down, self.C)

    def finish_far(self):
        p = self.place
        self.forward((2, 0), 0, (self.G,), p.up, self.F)
        self.forward((2, 0), 1, (self.G,), p.down, self.F)

    def finish_across(self):
        for half in HALVES:
            self.forward((0, 1), half, (self.D, self.E), self.place.across, self.A)

    def finish_near(self):
        p = self.place
        self.forward((1, 0), 0, (self.F,), p.up, self.B)
        self.forward((3, 0), 1, (self.F,), p.down, self.C)

    def finish(self, store):
        for half in HALVES:
            store(half, self.total((0, 0), half, (self.A, self.B, self.C)))


def sigmoid(v):
    return 1.0 / (1.0 + jnp.exp(-v))


def dot(a, b, contract=((1,), (0,))):
    return lax.dot_general(a, b, (contract, ((), ())), preferred_element_type=F32)


def load(src, dst, sems, at):
    copy = pltpu.make_async_copy(src, dst, sems.at[at])
    copy.start()
    return copy


def wide_product(left, right, partial, half, transposed):
    def tile(n, carry):
        at = pl.multiple_of(half * 2048 + n * 256, 256)
        if transposed:
            value = dot(left[...], right[pl.ds(at, 256), :], ((1,), (1,)))
        else:
            value = dot(left[...], right[:, pl.ds(at, 256)])
        partial[:, pl.ds(at, 256)] = value.astype(BF16)
        return carry

    lax.fori_loop(0, 8, tile, 0)


def row_view(ref):
    return lambda block, half: ref.at[
        pl.ds(pl.multiple_of(block * 32, 32), 32), half_cols(half)
    ]


class TaskPlace:
    def __init__(self):
        task = lax.axis_index("task")
        self.xh = task // 4
        self.y = lax.rem(task, 4)
        self.up = self.xh * 4 + plus(self.y, 1, 4)
        self.down = self.xh * 4 + plus(self.y, 3, 4)
        self.across = (1 - self.xh) * 4 + self.y


class TaskSum:
    F, B, C = range(3)
    OWN, FROM_DOWN, FROM_UP, DOWN_ACROSS, UP_ACROSS, FAR, FAR_ACROSS = range(7)

    def __init__(self, place, wires, view, whole, land, land_x, result):
        self.place = place
        self.wires = wires
        self.view = view
        self.whole = whole
        self.land = land
        self.land_x = land_x
        self.result = result
        self.first = wires.claim(14)

    def slab(self, ref, dy, part):
        return self.view(ref, plus(self.place.y, dy, 4) * 2 + part)

    def post(self, src, dst, slot, peer):
        self.wires.send(src, dst, self.first + slot, peer, "task")

    def wait(self, dst, slot):
        self.wires.arrived(dst, self.first + slot, "task")

    def far(self):
        p = self.place
        self.post(self.slab(self.whole, 2, 0), self.land.at[self.F, 0], 0, p.up)
        self.post(self.slab(self.whole, 2, 1), self.land.at[self.F, 1], 1, p.down)

    def near(self):
        p = self.place
        self.post(self.slab(self.whole, 1, 1), self.land.at[self.B, 1], 3, p.up)
        self.post(self.slab(self.whole, 3, 0), self.land.at[self.C, 0], 4, p.down)

    def relay(self):
        p = self.place
        for dy, part, kind, slot, peer in ((1, 0, self.B, 2, p.up), (3, 1, self.C, 5, p.down)):
            self.wait(self.land.at[self.F, part], part)
            own = self.slab(self.whole, dy, part)
            total = own[...].astype(F32) + self.land[self.F, part].astype(F32)
            own[...] = total.astype(BF16)
            self.post(own, self.land.at[kind, part], slot, peer)

    def local(self, part):
        return (
            self.slab(self.whole, 0, part)[...].astype(F32)
            + self.land[self.B, part].astype(F32)
            + self.land[self.C, part].astype(F32)
        )

    def fold(self):
        for kind, part, slot in ((self.B, 1, 3), (self.C, 0, 4), (self.B, 0, 2), (self.C, 1, 5)):
            self.wait(self.land.at[kind, part], slot)
        other = 1 - self.place.xh
        away = self.slab(self.whole, 0, other)
        away[...] = self.local(other).astype(BF16)
        self.post(away, self.land_x, 6, self.place.across)

    def pass_on(self, kind, peer, kind_there):
        v = self.held(kind)
        self.post(v, v, 6 + kind_there, peer)

    def held(self, kind):
        dy, across = {
            self.OWN: (0, 0),
            self.FROM_DOWN: (3, 0),
            self.FROM_UP: (1, 0),
            self.DOWN_ACROSS: (3, 1),
            self.UP_ACROSS: (1, 1),
            self.FAR: (2, 0),
            self.FAR_ACROSS: (2, 1),
        }[kind]
        xh = self.place.xh
        return self.slab(self.result, dy, 1 - xh if across else xh)

    def across_held(self):
        return self.slab(self.result, 0, 1 - self.place.xh)

    def finish(self):
        p = self.place
        self.wait(self.land_x, 6)
        own = self.held(self.OWN)
        own[...] = (self.local(p.xh) + self.land_x[...].astype(F32)).astype(BF16)
        self.post(own, own, 13, p.across)
        self.pass_on(self.OWN, p.up, self.FROM_DOWN)
        self.pass_on(self.OWN, p.down, self.FROM_UP)

    def get(self, kind):
        self.wait(self.held(kind), 6 + kind)

    def spread(self):
        p = self.place
        self.get(self.FROM_DOWN)
        self.pass_on(self.FROM_DOWN, p.up, self.FAR)
        self.get(self.FROM_UP)
        v = self.across_held()
        self.wait(v, 13)
        self.post(v, v, 6 + self.DOWN_ACROSS, p.up)
        self.post(v, v, 6 + self.UP_ACROSS, p.down)

    def spread_far(self):
        self.get(self.UP_ACROSS)
        self.pass_on(self.UP_ACROSS, self.place.down, self.FAR_ACROSS)
        self.get(self.DOWN_ACROSS)

    def end(self):
        self.get(self.FAR)
        self.get(self.FAR_ACROSS)


def slope(v):
    s = sigmoid(v)
    return s * (1.0 + v * (1.0 - s))


def slab_rows(height):
    return lambda ref, n: ref.at[pl.ds(pl.multiple_of(n * height, 16), height), :]


def slab_cols(ref, n):
    return ref.at[:, pl.ds(pl.multiple_of(n * 512, 512), 512)]


def popart_update(counts, totals, squares, pop_mean, pop_scale):
    mixing = counts / (counts + POPART_PRIOR)
    safe_counts = jnp.maximum(counts, 1.0)
    batch_mean = totals / safe_counts
    batch_square = squares / safe_counts
    updated_return_mean = (1.0 - mixing) * pop_mean + mixing * batch_mean
    mean_gap = batch_mean - pop_mean
    variance = (
        (1.0 - mixing) * pop_scale * pop_scale
        + mixing * (batch_square - batch_mean * batch_mean)
        + mixing * (1.0 - mixing) * mean_gap * mean_gap
    )
    return (updated_return_mean, jnp.sqrt(variance))


class AllPairs:
    def __init__(self, wires, axis, size, land):
        self.wires = wires
        self.axis = axis
        self.size = size
        self.here = lax.axis_index(axis)
        self.land = land
        self.first = wires.claim(size - 1)

    def post(self, peer_at, src):
        peer = plus(self.here, peer_at, self.size)
        self.wires.send(
            src(peer), self.land.at[peer_at - 1], self.first + peer_at - 1, peer, self.axis
        )

    def wait(self, peer_at):
        self.wires.arrived(self.land.at[peer_at - 1], self.first + peer_at - 1, self.axis)


def greet_everyone():
    barrier = pltpu.get_barrier_semaphore()
    for axis, size in (("tp", 16), ("task", 8)):
        here = lax.axis_index(axis)
        for hop in range(1, size):
            pl.semaphore_signal(
                barrier, inc=1, device_id={axis: plus(here, hop, size)}, device_id_type=MESH
            )
    pl.semaphore_wait(barrier, 22)


def lanes(shape):
    return lax.broadcasted_iota(jnp.int32, shape, 1)


def sublanes(shape):
    return lax.broadcasted_iota(jnp.int32, shape, 0)


def popart_rows(tasks, rewards, ends):
    factors = DISCOUNT * (1.0 - ends[...].astype(F32))
    gains = rewards[...]
    running = jnp.zeros((1, 32), F32)
    total = jnp.zeros((1, 32), F32)
    square = jnp.zeros((1, 32), F32)
    for t in range(14, -1, -1):
        running = gains[t : t + 1, :] + factors[t : t + 1, :] * running
        total = total + running
        square = square + running * running
    member = sublanes((128, 32)) == tasks[...] + ACTIONS
    diagonal = sublanes((128, 128)) == lanes((128, 128))
    rows = []
    for value in (jnp.full((1, 32), 15.0, F32), total, square):
        column = jnp.sum(jnp.where(member, value, 0.0), axis=1, keepdims=True)
        rows.append(jnp.sum(jnp.where(diagonal, column, 0.0), axis=0, keepdims=True))
    return jnp.concatenate([*rows, jnp.zeros((5, 128), F32)], axis=0)


def as_column(row):
    diagonal = sublanes((128, 128)) == lanes((128, 128))
    return jnp.sum(jnp.where(diagonal, row, 0.0), axis=1, keepdims=True)


def step_columns(ref, first_env):
    value = ref[...].astype(F32)
    value = jnp.concatenate([value, jnp.zeros((1, 32), F32)], axis=0)
    lane = lanes((16, 32))
    return jnp.concatenate(
        [
            jnp.sum(jnp.where(lane == first_env + e, value, 0.0), axis=1, keepdims=True)
            for e in (0, 1)
        ],
        axis=0,
    )


def loss_gradient(outputs, own, columns, mean, scale):
    action, reward, factor, behaviour = columns
    shape = (32, 128)
    lane = lanes(shape)
    frame = lax.rem(sublanes(shape), 16)
    live = frame < 15

    def later(value, by):
        return jnp.where(frame + by < 16, pltpu.roll(value, 32 - by, 0), 0.0)

    def over_lanes(mask, value):
        return jnp.broadcast_to(
            jnp.sum(jnp.where(mask, value, 0.0), axis=1, keepdims=True), shape
        )

    is_logit = lane < ACTIONS
    chosen = lane == action.astype(jnp.int32)
    log_total = jnp.log(over_lanes(is_logit, jnp.exp(jnp.where(is_logit, outputs, 0.0))))
    log_prob = jnp.where(is_logit, outputs - log_total, 0.0)
    log_policy = over_lanes(chosen, log_prob)
    env_mean = over_lanes(own, mean)
    env_scale = over_lanes(own, scale)
    norm_values = over_lanes(own, outputs)
    values = norm_values * env_scale + env_mean
    clipped = jnp.minimum(jnp.exp(log_policy - behaviour), 1.0)
    total = jnp.where(live, clipped * (reward + factor * later(values, 1) - values), 0.0)
    decay = jnp.where(live, factor * clipped, 0.0)
    for by in (1, 2, 4, 8):
        total = total + decay * later(total, by)
        decay = decay * later(decay, by)
    targets = values + total
    following = later(targets, 1)
    advantage = clipped * ((reward + factor * following - env_mean) / env_scale - norm_values)
    normed_targets = (targets - env_mean) / env_scale
    policy = jnp.where(is_logit, jnp.exp(log_prob), 0.0)
    entropy = -over_lanes(is_logit, policy * log_prob)
    d_logits = -advantage * (jnp.where(chosen, 1.0, 0.0) - policy) + ENTROPY_COST * policy * (
        log_prob + entropy
    )
    d_value = -BASELINE_COST * (normed_targets - norm_values)
    d = jnp.where(is_logit, d_logits, jnp.where(own, d_value, 0.0))
    return jnp.where(live, d * LOSS_WEIGHT, 0.0)


def step_kernel(
    own_tokens, gain, w_in, w_mix, w_out, head, vectors, tasks, actions, rewards, ends, behaviour,
    sum_out_hbm, sum_mix_hbm, sum_in_hbm, new_head, stats,
    tokens, w_in_v, w_mix_v, w_out_v, pre_in, hidden_in, residual, gain_all, normed,
    pre_out, hidden_out, head_part, head_land, d_heads, stat_own, stat_land,
    d_pre_out, d_pre_in, hidden_t, d_normed,
    partial, twin_part, landing, twin_part_b, landing_b, arrived, gain_parts, gain_land,
    whole_out, whole_mix, whole_in, land_out, land_mix, land_in, x_out, x_mix, x_in,
    sum_out, sum_mix, sum_in,
    send_sems, recv_sems, local_sems,
):
    place = Place()
    task = TaskPlace()
    wires = Wires(send_sems, recv_sems)
    me = place.me
    own_cols = pl.ds(pl.multiple_of(me * 256, 256), 256)
    first = load(own_tokens, tokens.at[pl.ds(0, 512), own_cols], local_sems, 0)
    g = gain[...]
    hi = g.astype(BF16).astype(F32)
    mid = (g - hi).astype(BF16).astype(F32)
    low = g - hi - mid
    row = sublanes((16, 256))
    rows = jnp.where(row == 0, hi, jnp.where(row == 1, mid, jnp.where(row == 2, low, 0.0)))
    tokens[pl.ds(512, 16), own_cols] = rows.astype(BF16)
    greet_everyone()
    first.wait()

    def token_view(block, half):
        rows = pl.ds(0, 256) if half == 0 else pl.ds(256, 272)
        return tokens.at[rows, pl.ds(pl.multiple_of(block * 256, 256), 256)]

    gather = Gather(place, wires, token_view)
    gather.open()
    get_in = load(w_in, w_in_v, local_sems, 1)
    get_mix = load(w_mix, w_mix_v, local_sems, 2)
    get_out = load(w_out, w_out_v, local_sems, 3)

    stat_own[...] = popart_rows(tasks, rewards, ends)
    statistics = AllPairs(wires, "task", 8, stat_land)
    for hop in range(1, 8):
        statistics.post(hop, lambda peer: stat_own)
    gather.middle()

    def slab(dz, opening=False):
        at = pl.multiple_of(plus(place.z, dz, 4) * 1024, 1024)

        def tile(m, carry):
            r = pl.ds(pl.multiple_of(m * 128, 128), 128)
            value = dot(tokens[r, pl.ds(at, 1024)], w_in_v[pl.ds(at, 1024), :])
            pre_in[r, :] = value if opening else pre_in[r, :] + value
            return carry

        lax.fori_loop(0, 4, tile, 0)

    get_in.wait()
    gather.wait_twin(gather.OWN, gather.ACROSS)
    slab(0, True)
    gather.late()
    gather.wait_twin(gather.FROM_UP, gather.UP_ACROSS)
    slab(1)
    gather.last()
    gather.wait_twin(gather.FROM_DOWN, gather.DOWN_ACROSS)
    slab(3)
    gather.wait_twin(gather.FAR, gather.FAR_ACROSS)
    slab(2)

    def activate(m, carry):
        r = pl.ds(pl.multiple_of(m * 128, 128), 128)
        v = pre_in[r, :]
        hidden_in[r, :] = (v * sigmoid(v)).astype(BF16)
        return carry

    lax.fori_loop(0, 4, activate, 0)
    get_mix.wait()
    scatter = Scatter(place, wires, partial, twin_part, landing)
    scatter.open(lambda half: wide_product(hidden_in, w_mix_v, partial, half, False))

    g3 = tokens[pl.ds(512, 16), :].astype(F32)
    gain_all[...] = g3[0:1, :] + g3[1:2, :] + g3[2:3, :]
    summed = stat_own[...]
    for hop in range(1, 8):
        statistics.wait(hop)
        summed = summed + stat_land[hop - 1]
    counts, totals, squares = summed[0:1, :], summed[1:2, :], summed[2:3, :]
    bias, pop_mean, pop_scale = vectors[0:1, :], vectors[1:2, :], vectors[2:3, :]
    mean, scale = popart_update(counts, totals, squares, pop_mean, pop_scale)
    is_value = lanes((1, 128)) >= ACTIONS
    ratio = jnp.where(is_value, pop_scale / scale, 1.0)
    new_bias = jnp.where(is_value, (pop_scale * bias + pop_mean - mean) / scale, bias)
    new_head[pl.ds(0, 75), :] = (head[...].astype(F32) * as_column(ratio)[0:75, :]).astype(BF16)
    new_head[pl.ds(75, 53), :] = jnp.zeros((53, 256), BF16)
    stats[...] = jnp.concatenate([mean, scale, new_bias, jnp.zeros((5, 128), F32)], axis=0)

    scatter.finish_far()
    scatter.finish_across()
    scatter.finish_near()
    first_env = me * 2
    columns = [
        step_columns(ref, first_env) for ref in (actions, rewards, ends, behaviour)
    ]
    columns[2] = DISCOUNT * (1.0 - columns[2])
    env = [
        jnp.sum(jnp.where(lanes((1, 32)) == first_env + e, tasks[...].astype(F32), 0.0), axis=1, keepdims=True)
        for e in (0, 1)
    ]
    game = jnp.where(sublanes((32, 128)) < 16, env[0], env[1])
    own_value = lanes((32, 128)) == game.astype(jnp.int32) + ACTIONS
    own_rows = pl.ds(pl.multiple_of(me * 32, 32), 32)

    def store(half, value):
        residual[:, half_cols(half)] = (
            value + tokens[own_rows, half_cols(half)].astype(F32)
        )

    scatter.finish(store)
    for m in range(2):
        v = residual[pl.ds(m * 16, 16), :]
        inverse = lax.rsqrt(jnp.mean(v * v, axis=1, keepdims=True) + NORM_EPS)
        normed[pl.ds(pl.multiple_of(me * 32 + m * 16, 16), 16), :] = (
            v * inverse * gain_all[...]
        ).astype(BF16)
    spread = Gather(place, wires, row_view(normed))
    spread.open()
    heads = AllPairs(wires, "tp", 16, head_land)

    def out_slab(dz):
        start = plus(place.z, dz, 4) * 128
        rows = pl.ds(pl.multiple_of(start, 128), 128)
        v = dot(normed[rows, :], w_out_v[...])
        pre_out[rows, :] = v
        hidden_out[rows, :] = (v * sigmoid(v)).astype(BF16)
        head_part[rows, :] = dot(hidden_out[rows, :], new_head[...], ((1,), (1,))).astype(BF16)

    spread.middle()
    get_out.wait()
    spread.wait_twin(spread.OWN, spread.ACROSS)
    out_slab(0)
    spread.late()
    spread.wait_twin(spread.FROM_UP, spread.UP_ACROSS)
    out_slab(1)
    spread.last()
    spread.wait_twin(spread.FROM_DOWN, spread.DOWN_ACROSS)
    out_slab(3)
    spread.wait_twin(spread.FAR, spread.FAR_ACROSS)
    out_slab(2)

    def frames_of(ref):
        return lambda device: ref.at[pl.ds(pl.multiple_of(device * 32, 32), 32), :]

    for hop in range(1, 16):
        heads.post(hop, frames_of(head_part))
    outputs = head_part[own_rows, :].astype(F32)
    for hop in range(1, 16):
        heads.wait(hop)
        outputs = outputs + head_land[hop - 1].astype(F32)
    d_own = loss_gradient(outputs + new_bias, own_value, columns, mean, scale)
    d_heads[own_rows, :] = d_own.astype(BF16)
    d_slot = wires.claim(15)
    d_view = frames_of(d_heads)
    for hop in range(1, 16):
        wires.send(d_view(me), d_view(me), d_slot + hop - 1, plus(me, hop, 16))
    wires.drain_all_but(15)
    for hop in range(1, 16):
        wires.arrived(d_view(plus(me, 16 - hop, 16)), d_slot + hop - 1)

    def pre_gradient(m, carry):
        r = pl.ds(pl.multiple_of(m * 128, 128), 128)
        d_hidden = dot(d_heads[r, :], new_head[...])
        d_pre_out[r, :] = (d_hidden * slope(pre_out[r, :])).astype(BF16)
        return carry

    lax.fori_loop(0, 4, pre_gradient, 0)
    scatter = Scatter(place, wires, partial, twin_part_b, landing_b)
    scatter.open(lambda half: wide_product(d_pre_out, w_out_v, partial, half, True))
    for_out = TaskSum(task, wires, slab_rows(512), whole_out, land_out, x_out, sum_out)
    for_mix = TaskSum(task, wires, slab_cols, whole_mix, land_mix, x_mix, sum_mix)
    for_in = TaskSum(task, wires, slab_rows(528), whole_in, land_in, x_in, sum_in)

    def tall_product(left, right, whole, height, dy):
        k = plus(task.y, dy, 4)

        def tile(n, carry):
            feature = pl.multiple_of(k * 1024 + n * 256, 256)
            at = pl.multiple_of((k * 2 + n // 2) * height + lax.rem(n, 2) * 256, 16)
            value = dot(left[pl.ds(0, 512), pl.ds(feature, 256)], right[...], ((0,), (0,)))
            whole[pl.ds(at, 256), :] = value.astype(BF16)
            return carry

        lax.fori_loop(0, 4, tile, 0)

    def mix_product(dy):
        k = plus(task.y, dy, 4)

        def tile(n, carry):
            at = pl.multiple_of(k * 1024 + n * 256, 256)
            whole_mix[:, pl.ds(at, 256)] = dot(hidden_t[...], arrived[:, pl.ds(at, 256)]).astype(BF16)
            return carry

        lax.fori_loop(0, 4, tile, 0)

    def out_product(dy):
        tall_product(normed, d_pre_out, whole_out, 512, dy)

    def in_product(dy):
        tall_product(tokens, d_pre_in, whole_in, 528, dy)

    out_product(2)
    for_out.far()
    scatter.finish_far()
    out_product(1)
    out_product(3)
    for_out.near()
    scatter.finish_across()
    out_product(0)
    scatter.finish_near()
    hidden_t[...] = hidden_in[...].T
    for_out.relay()

    def store(half, value):
        d_normed[:, half_cols(half)] = value

    scatter.finish(store)
    gain_rows = jnp.zeros((8, 4096), F32)
    for m in range(2):
        r = pl.ds(m * 16, 16)
        v = residual[r, :]
        inverse = lax.rsqrt(jnp.mean(v * v, axis=1, keepdims=True) + NORM_EPS)
        d = d_normed[r, :]
        scaled = d * gain_all[...]
        inner = jnp.sum(scaled * v, axis=1, keepdims=True)
        step = inverse * scaled - v * (inverse * inverse * inverse * inner * (1.0 / 4096))
        arrived[pl.ds(pl.multiple_of(me * 32 + m * 16, 16), 16), :] = step.astype(BF16)
        d_normed[r, :] = d * v * inverse
    gather = Gather(place, wires, row_view(arrived))
    gather.open()
    for m in range(4):
        gain_rows = gain_rows + d_normed[pl.ds(m * 8, 8), :]
    for n in range(16):
        gain_parts[n] = gain_rows[:, n * 256 : n * 256 + 256]
    for_out.fold()
    gains = AllPairs(wires, "tp", 16, gain_land)
    for hop in range(1, 16):
        gains.post(hop, lambda peer: gain_parts.at[peer])
    gather.middle()

    def hidden_slab(dz):
        rows = pl.ds(pl.multiple_of(plus(place.z, dz, 4) * 128, 128), 128)
        d = dot(arrived[rows, :], w_mix_v[...], ((1,), (1,)))
        d_pre_in[rows, :] = (d * slope(pre_in[rows, :])).astype(BF16)

    gather.wait_twin(gather.OWN, gather.ACROSS)
    hidden_slab(0)
    gather.late()
    for_out.finish()
    gather.wait_twin(gather.FROM_UP, gather.UP_ACROSS)
    hidden_slab(1)
    gather.last()
    gather.wait_twin(gather.FROM_DOWN, gather.DOWN_ACROSS)
    hidden_slab(3)
    gather.wait_twin(gather.FAR, gather.FAR_ACROSS)
    mix_product(2)
    for_mix.far()
    hidden_slab(2)
    mix_product(1)
    mix_product(3)
    for_mix.near()
    for_out.spread()
    mix_product(0)
    in_product(2)
    small = dot(d_heads[...], hidden_out[...], ((0,), (0,)))
    bias = jnp.sum(d_heads[...].astype(F32), axis=0, keepdims=True)
    gain_total = jnp.sum(gain_parts[me], axis=0, keepdims=True)
    for hop in range(1, 16):
        gains.wait(hop)
        gain_total = gain_total + jnp.sum(gain_land[hop - 1], axis=0, keepdims=True)
    row = lax.broadcasted_iota(jnp.int32, (128, 256), 0)
    bias = jnp.concatenate([bias, jnp.zeros((1, 128), F32)], axis=1)
    small = jnp.where(row == 80, bias, jnp.where(row == 88, gain_total, small)).astype(BF16)
    for n in range(8):
        whole_in[pl.ds(n * 528 + 512, 16), :] = small[n * 16 : n * 16 + 16, :]
    for_in.far()
    in_product(1)
    in_product(3)
    for_in.near()
    for_mix.relay()
    in_product(0)
    for_out.spread_far()
    for_in.relay()
    for_mix.fold()
    for_out.end()
    keep_out = load(sum_out, sum_out_hbm, local_sems, 4)
    for_in.fold()
    for_mix.finish()
    for_mix.spread()
    for_in.finish()
    for_mix.spread_far()
    for_in.spread()
    for_mix.end()
    keep_mix = load(sum_mix, sum_mix_hbm, local_sems, 5)
    for_in.spread_far()
    for_in.end()
    keep_in = load(sum_in, sum_in_hbm, local_sems, 6)
    wires.drain()
    for keep in (keep_out, keep_mix, keep_in):
        keep.wait()


def finish_kernel(
    sum_out, sum_mix, sum_in, new_head, stats,
    grad_in, grad_mix, grad_out, gain, head, bias, head_now, bias_now, mean, scale,
    out_b, mix_b, in_b, small_b, out_f, mix_f, in_f, sems,
):
    gets = []
    for n in range(8):
        r = pl.ds(n * 512, 512)
        gets.append(load(sum_in.at[pl.ds(n * 528, 512), :], in_b.at[r, :], sems, n))
    for n in range(8):
        gets.append(
            load(sum_in.at[pl.ds(n * 528 + 512, 16), :], small_b.at[pl.ds(n * 16, 16), :], sems, 8 + n)
        )
    for n in range(4):
        r = pl.ds(n * 64, 64)
        gets.append(load(sum_mix.at[r, :], mix_b.at[r, :], sems, 16 + n))
    for n in range(8):
        r = pl.ds(n * 512, 512)
        gets.append(load(sum_out.at[r, :], out_b.at[r, :], sems, 20 + n))
    puts = []
    for n in range(8):
        r = pl.ds(n * 512, 512)
        gets[n].wait()
        in_f[r, :] = in_b[r, :].astype(F32)
        puts.append(load(in_f.at[r, :], grad_in.at[r, :], sems, 28 + n))
    for n in range(4):
        r = pl.ds(n * 64, 64)
        gets[16 + n].wait()
        mix_f[r, :] = mix_b[r, :].astype(F32)
        puts.append(load(mix_f.at[r, :], grad_mix.at[r, :], sems, 36 + n))
    for n in range(8):
        r = pl.ds(n * 512, 512)
        gets[20 + n].wait()
        out_f[r, :] = out_b[r, :].astype(F32)
        puts.append(load(out_f.at[r, :], grad_out.at[r, :], sems, 40 + n))
    for n in range(8):
        gets[8 + n].wait()
    small = small_b[...].astype(F32)
    head[...] = small[0:75, :]
    bias[...] = small[80:81, 0:75]
    gain[...] = small[88:89, :]
    head_now[...] = new_head[0:75, :]
    values = pltpu.roll(stats[...], 128 - ACTIONS, 1)
    mean[...] = values[0:1, 0:TASKS]
    scale[...] = values[1:2, 0:TASKS]
    bias_now[...] = stats[2:3, 0:75]
    for put in puts:
        put.wait()


def hbm():
    return pl.BlockSpec(memory_space=pltpu.HBM)


def vmem():
    return pl.BlockSpec(memory_space=pltpu.VMEM)


def step_call(*arguments):
    v, h = vmem(), hbm()
    scratch = [
        ((528, 4096), BF16), ((4096, 256), BF16), ((256, 4096), BF16), ((4096, 256), BF16),
        ((512, 256), F32), ((512, 256), BF16), ((32, 4096), F32), ((1, 4096), F32),
        ((512, 4096), BF16),
        ((512, 256), F32), ((512, 256), BF16), ((512, 128), BF16), ((15, 32, 128), BF16),
        ((512, 128), BF16), ((8, 128), F32), ((7, 8, 128), F32),
        ((512, 256), BF16), ((512, 256), BF16), ((256, 512), BF16), ((32, 4096), F32),
        ((512, 4096), BF16), ((8, 32, 4096), BF16), ((7, 32, 4096), BF16),
        ((8, 32, 4096), BF16), ((7, 32, 4096), BF16), ((512, 4096), BF16),
        ((16, 8, 256), F32), ((15, 8, 256), F32),
        ((4096, 256), BF16), ((256, 4096), BF16), ((4224, 256), BF16),
        ((3, 2, 512, 256), BF16), ((3, 2, 256, 512), BF16), ((3, 2, 528, 256), BF16),
        ((512, 256), BF16), ((256, 512), BF16), ((528, 256), BF16),
        ((4096, 256), BF16), ((256, 4096), BF16), ((4224, 256), BF16),
    ]
    return pl.pallas_call(
        step_kernel,
        out_shape=[
            jax.ShapeDtypeStruct((4096, 256), BF16),
            jax.ShapeDtypeStruct((256, 4096), BF16),
            jax.ShapeDtypeStruct((4224, 256), BF16),
            jax.ShapeDtypeStruct((128, 256), BF16),
            jax.ShapeDtypeStruct((8, 128), F32),
        ],
        in_specs=[h, v, h, h, h, v, v, v, v, v, v, v],
        out_specs=[h, h, h, v, v],
        scratch_shapes=[pltpu.VMEM(*s) for s in scratch]
        + [pltpu.SemaphoreType.DMA((SENDS,)), pltpu.SemaphoreType.DMA((RECEIVES,)), pltpu.SemaphoreType.DMA((7,))],
        compiler_params=pltpu.CompilerParams(
            collective_id=0, has_side_effects=True, vmem_limit_bytes=63 * 2**20
        ),
        name="step",
    )(*arguments)


def finish_call(*arguments):
    v, h = vmem(), hbm()
    return pl.pallas_call(
        finish_kernel,
        out_shape=[
            jax.ShapeDtypeStruct((4096, 256), F32),
            jax.ShapeDtypeStruct((256, 4096), F32),
            jax.ShapeDtypeStruct((4096, 256), F32),
            jax.ShapeDtypeStruct((1, 256), F32),
            jax.ShapeDtypeStruct((75, 256), F32),
            jax.ShapeDtypeStruct((1, 75), F32),
            jax.ShapeDtypeStruct((75, 256), BF16),
            jax.ShapeDtypeStruct((1, 75), F32),
            jax.ShapeDtypeStruct((1, TASKS), F32),
            jax.ShapeDtypeStruct((1, TASKS), F32),
        ],
        in_specs=[h, h, h, v, v],
        out_specs=[h, h, h, v, v, v, v, v, v, v],
        scratch_shapes=[
            pltpu.VMEM((4096, 256), BF16),
            pltpu.VMEM((256, 4096), BF16),
            pltpu.VMEM((4096, 256), BF16),
            pltpu.VMEM((128, 256), BF16),
            pltpu.VMEM((4096, 256), F32),
            pltpu.VMEM((256, 4096), F32),
            pltpu.VMEM((4096, 256), F32),
            pltpu.SemaphoreType.DMA((48,)),
        ],
        compiler_params=pltpu.CompilerParams(vmem_limit_bytes=48 * 2**20),
        name="finish",
    )(*arguments)


def on_device(
    observations, gain, w_in, w_mix, w_out, w_head, head_bias, pop_mean, pop_scale,
    task_indices, actions, rewards, episode_ends, behaviour_log_prob,
):
    pad = (ACTIONS, 128 - ACTIONS - TASKS)
    vectors = jnp.stack(
        [
            jnp.pad(head_bias, (0, 128 - ACTIONS - TASKS)),
            jnp.pad(pop_mean, pad),
            jnp.pad(pop_scale, pad, constant_values=1.0),
        ]
    )
    sums = step_call(
        observations.reshape(512, 256),
        gain.reshape(1, 256),
        w_in,
        w_mix,
        w_out,
        w_head.T,
        vectors,
        task_indices.reshape(1, 32),
        actions.T,
        rewards.T,
        episode_ends.T,
        behaviour_log_prob.T,
    )
    (
        grad_in, grad_mix, grad_out, grad_gain, grad_head, grad_bias,
        new_head, new_bias, mean, scale,
    ) = finish_call(*sums)
    return (
        grad_in,
        grad_mix,
        grad_out,
        grad_gain.reshape(256),
        grad_head.T,
        grad_bias.reshape(75),
        new_head.T,
        new_bias.reshape(75),
        mean.reshape(TASKS),
        scale.reshape(TASKS),
    )


def solution(mesh):
    in_specs = (
        P("task", None, "tp"),
        P("tp"),
        P(None, "tp"),
        P("tp", None),
        P(None, "tp"),
        P("tp", None),
        P(),
        P(),
        P(),
        P("task"),
        P("task", None),
        P("task", None),
        P("task", None),
        P("task", None),
    )
    out_specs = (
        P(None, "tp"),
        P("tp", None),
        P(None, "tp"),
        P("tp"),
        P("tp", None),
        P(),
        P("tp", None),
        P(),
        P(),
        P(),
    )
    return jax.shard_map(
        on_device, mesh=mesh, in_specs=in_specs, out_specs=out_specs, check_vma=False
    )
```

```python
import jax
import jax.numpy as jnp
from jax import lax
from jax.experimental import pallas as pl
from jax.experimental.pallas import tpu as pltpu
from jax.sharding import PartitionSpec as P

ACTIONS = 18
TASKS = 57
DISCOUNT = 0.99
BASELINE_COST = 0.5
ENTROPY_COST = 0.01
POPART_PRIOR = 64.0
NORM_EPS = 1e-06
LOSS_WEIGHT = 256**-0.5
SENDS = 148
RECEIVES = 208


MESH = pl.DeviceIdType.MESH
F32 = jnp.float32
BF16 = jnp.bfloat16
HALVES = (0, 1)


def plus(a, b, n):
    return lax.rem(a + b, n)


class Place:
    def __init__(self):
        self.me = lax.axis_index("tp")
        self.z = self.me // 4
        self.x = lax.rem(self.me // 2, 2)
        self.c = lax.rem(self.me, 2)
        self.across = self.at(0, 1)
        self.up = self.at(1, 0)
        self.down = self.at(3, 0)
        self.partner = self.at(0, 0, 1)

    def at(self, dz, dx, dc=0):
        return (plus(self.z, dz, 4) * 2 + plus(self.x, dx, 2)) * 2 + plus(self.c, dc, 2)


class Wires:
    def __init__(self, send_sems, recv_sems):
        self.send_sems = send_sems
        self.recv_sems = recv_sems
        self.sent = []
        self.slots = 0

    def claim(self, count):
        first = self.slots
        self.slots += count
        return first

    def send(self, src, dst, slot, peer, axis="tp"):
        copy = pltpu.make_async_remote_copy(
            src_ref=src,
            dst_ref=dst,
            send_sem=self.send_sems.at[len(self.sent)],
            recv_sem=self.recv_sems.at[slot],
            device_id={axis: peer},
            device_id_type=MESH,
        )
        copy.start()
        self.sent.append(copy)

    def arrived(self, dst, slot, axis="tp"):
        pltpu.make_async_remote_copy(
            src_ref=dst,
            dst_ref=dst,
            send_sem=self.send_sems.at[0],
            recv_sem=self.recv_sems.at[slot],
            device_id={axis: lax.axis_index(axis)},
            device_id_type=MESH,
        ).wait_recv()

    def drain(self):
        for copy in self.sent:
            copy.wait_send()
        self.sent = []


class Gather:
    ACROSS, FROM_DOWN, FROM_UP, DOWN_ACROSS, UP_ACROSS, FAR, FAR_ACROSS, OWN = range(8)

    def __init__(self, place, wires, view, first):
        self.place = place
        self.wires = wires
        self.view = view
        self.first = first
        p = place
        self.block = {
            self.ACROSS: p.at(0, 1),
            self.FROM_DOWN: p.at(3, 0),
            self.FROM_UP: p.at(1, 0),
            self.DOWN_ACROSS: p.at(3, 1),
            self.UP_ACROSS: p.at(1, 1),
            self.FAR: p.at(2, 0),
            self.FAR_ACROSS: p.at(2, 1),
            self.OWN: p.me,
        }
        self.twin = {k: plus(b, 0, 16) + 1 - 2 * p.c for k, b in self.block.items()}

    def slot(self, kind, half):
        return self.first + kind * 2 + half

    def twin_slot(self, kind, half):
        return self.first + 14 + kind * 2 + half

    def pass_on(self, kind, half, peer, kind_there):
        v = self.view(self.block[kind], half)
        self.wires.send(v, v, self.slot(kind_there, half), peer)

    def to_twin(self, kind, half):
        v = self.view(self.block[kind], half)
        self.wires.send(v, v, self.twin_slot(kind, half), self.place.partner)

    def wait(self, kind, half):
        self.wires.arrived(self.view(self.block[kind], half), self.slot(kind, half))

    def wait_twin(self, *kinds):
        for kind in kinds:
            for half in HALVES:
                self.wires.arrived(
                    self.view(self.twin[kind], half), self.twin_slot(kind, half)
                )

    def open(self):
        p = self.place
        for half in HALVES:
            self.pass_on(self.OWN, half, p.up, self.FROM_DOWN)
            self.pass_on(self.OWN, half, p.down, self.FROM_UP)
            self.pass_on(self.OWN, half, p.across, self.ACROSS)
            self.to_twin(self.OWN, half)

    def middle(self):
        self.middle_near()
        self.middle_across()
        self.middle_far()

    def middle_near(self):
        p = self.place
        self.wait(self.FROM_DOWN, 0)
        self.pass_on(self.FROM_DOWN, 0, p.up, self.FAR)
        self.to_twin(self.FROM_DOWN, 0)
        self.wait(self.FROM_UP, 0)
        self.to_twin(self.FROM_UP, 0)
        self.wait(self.ACROSS, 0)
        self.pass_on(self.ACROSS, 0, p.down, self.UP_ACROSS)
        self.wait(self.FROM_UP, 1)
        self.pass_on(self.FROM_UP, 1, p.down, self.FAR)
        self.pass_on(self.ACROSS, 0, p.up, self.DOWN_ACROSS)
        self.to_twin(self.ACROSS, 0)
        self.to_twin(self.FROM_UP, 1)

    def middle_across(self):
        p = self.place
        self.wait(self.FROM_DOWN, 1)
        self.to_twin(self.FROM_DOWN, 1)
        self.wait(self.ACROSS, 1)
        self.pass_on(self.ACROSS, 1, p.up, self.DOWN_ACROSS)
        self.pass_on(self.ACROSS, 1, p.down, self.UP_ACROSS)
        self.to_twin(self.ACROSS, 1)

    def middle_far(self):
        for half in HALVES:
            self.wait(self.FAR, half)
            self.pass_on(self.FAR, half, self.place.across, self.FAR_ACROSS)
            self.to_twin(self.FAR, half)

    def late(self):
        for half in HALVES:
            for kind in (self.DOWN_ACROSS, self.UP_ACROSS):
                self.wait(kind, half)
                self.to_twin(kind, half)

    def last(self):
        for half in HALVES:
            self.wait(self.FAR_ACROSS, half)
            self.to_twin(self.FAR_ACROSS, half)


def half_cols(half):
    return pl.ds(half * 2048, 2048)


class Scatter:
    G, D, E, F, A, B, C = range(7)
    ORDER = ((2, 1), (1, 1), (3, 1), (1, 0), (3, 0), (2, 0), (0, 1), (0, 0))

    def __init__(self, place, wires, partial, twin_part, landing, first):
        self.place = place
        self.wires = wires
        self.partial = partial
        self.twin_part = twin_part
        self.landing = landing
        self.first = first

    def rows(self, where, dc=0):
        return pl.ds(pl.multiple_of(self.place.at(*where, dc) * 32, 32), 32)

    def mine(self, where, half):
        return self.partial.at[self.rows(where), half_cols(half)]

    def twins(self, where, half):
        return self.twin_part.at[self.ORDER.index(where), :, half_cols(half)]

    def land(self, kind, half):
        return self.landing.at[kind, :, half_cols(half)]

    def total(self, where, half, kinds=(), waited=()):
        slot = self.first + 14 + self.ORDER.index(where) * 2 + half
        if (where, half) not in self.seen:
            self.wires.arrived(self.twins(where, half), slot)
            self.seen.add((where, half))
        for kind in kinds:
            self.wires.arrived(self.land(kind, half), self.first + kind * 2 + half)
        value = self.mine(where, half)[...].astype(F32) + self.twins(where, half)[...].astype(F32)
        for kind in kinds:
            value = value + self.land(kind, half)[...].astype(F32)
        return value

    def forward(self, where, half, kinds, peer, kind_there):
        self.mine(where, half)[...] = self.total(where, half, kinds).astype(BF16)
        self.wires.send(
            self.mine(where, half),
            self.land(kind_there, half),
            self.first + kind_there * 2 + half,
            peer,
        )

    def open(self, produce):
        self.seen = set()
        p = self.place
        for half in HALVES:
            produce(half)
            for where in self.ORDER:
                self.wires.send(
                    self.partial.at[self.rows(where, 1), half_cols(half)],
                    self.twins(where, half),
                    self.first + 14 + self.ORDER.index(where) * 2 + half,
                    p.partner,
                )
            self.forward((2, 1), half, (), p.across, self.G)
            self.forward((1, 1), half, (), p.up, self.D)
            self.forward((3, 1), half, (), p.down, self.E)
        self.forward((1, 0), 1, (), p.up, self.B)
        self.forward((3, 0), 0, (), p.down, self.C)

    def finish_far(self):
        p = self.place
        self.forward((2, 0), 0, (self.G,), p.up, self.F)
        self.forward((2, 0), 1, (self.G,), p.down, self.F)

    def finish_across(self):
        for half in HALVES:
            self.forward((0, 1), half, (self.D, self.E), self.place.across, self.A)

    def finish_near(self):
        p = self.place
        self.forward((1, 0), 0, (self.F,), p.up, self.B)
        self.forward((3, 0), 1, (self.F,), p.down, self.C)

    def finish(self, store):
        for half in HALVES:
            store(half, self.total((0, 0), half, (self.A, self.B, self.C)))


def sigmoid(v):
    return 1.0 / (1.0 + jnp.exp(-v))


def dot(a, b, contract=((1,), (0,))):
    return lax.dot_general(a, b, (contract, ((), ())), preferred_element_type=F32)


def load(src, dst, sems, at):
    copy = pltpu.make_async_copy(src, dst, sems.at[at])
    copy.start()
    return copy


def wide_product(left, right, partial, half, transposed):
    def tile(n, carry):
        at = pl.multiple_of(half * 2048 + n * 256, 256)
        if transposed:
            value = dot(left[...], right[pl.ds(at, 256), :], ((1,), (1,)))
        else:
            value = dot(left[...], right[:, pl.ds(at, 256)])
        partial[:, pl.ds(at, 256)] = value.astype(BF16)
        return carry

    lax.fori_loop(0, 8, tile, 0)


def row_view(ref):
    return lambda block, half: ref.at[
        pl.ds(pl.multiple_of(block * 32, 32), 32), half_cols(half)
    ]


class TaskPlace:
    def __init__(self):
        task = lax.axis_index("task")
        self.xh = task // 4
        self.y = lax.rem(task, 4)
        self.up = self.xh * 4 + plus(self.y, 1, 4)
        self.down = self.xh * 4 + plus(self.y, 3, 4)
        self.across = (1 - self.xh) * 4 + self.y


class TaskSum:
    F, B, C = range(3)
    OWN, FROM_DOWN, FROM_UP, DOWN_ACROSS, UP_ACROSS, FAR, FAR_ACROSS = range(7)

    def __init__(self, place, wires, view, whole, land, land_x, result):
        self.place = place
        self.wires = wires
        self.view = view
        self.whole = whole
        self.land = land
        self.land_x = land_x
        self.result = result
        self.first = wires.claim(14)

    def slab(self, ref, dy, part):
        return self.view(ref, plus(self.place.y, dy, 4) * 2 + part)

    def post(self, src, dst, slot, peer):
        self.wires.send(src, dst, self.first + slot, peer, "task")

    def wait(self, dst, slot):
        self.wires.arrived(dst, self.first + slot, "task")

    def far(self):
        p = self.place
        self.post(self.slab(self.whole, 2, 0), self.land.at[self.F, 0], 0, p.up)
        self.post(self.slab(self.whole, 2, 1), self.land.at[self.F, 1], 1, p.down)

    def near(self):
        p = self.place
        self.post(self.slab(self.whole, 1, 1), self.land.at[self.B, 1], 3, p.up)
        self.post(self.slab(self.whole, 3, 0), self.land.at[self.C, 0], 4, p.down)

    def relay(self):
        p = self.place
        for dy, part, kind, slot, peer in ((1, 0, self.B, 2, p.up), (3, 1, self.C, 5, p.down)):
            self.wait(self.land.at[self.F, part], part)
            own = self.slab(self.whole, dy, part)
            total = own[...].astype(F32) + self.land[self.F, part].astype(F32)
            own[...] = total.astype(BF16)
            self.post(own, self.land.at[kind, part], slot, peer)

    def local(self, part):
        if self.land is None:
            return self.view(self.whole, part)[...].astype(F32)
        return (
            self.slab(self.whole, 0, part)[...].astype(F32)
            + self.land[self.B, part].astype(F32)
            + self.land[self.C, part].astype(F32)
        )

    def fold(self):
        if self.land is None:
            away = self.view(self.whole, 1 - self.place.xh)
            self.post(away, self.land_x, 6, self.place.across)
            return
        for kind, part, slot in ((self.B, 1, 3), (self.C, 0, 4), (self.B, 0, 2), (self.C, 1, 5)):
            self.wait(self.land.at[kind, part], slot)
        other = 1 - self.place.xh
        away = self.slab(self.whole, 0, other)
        away[...] = self.local(other).astype(BF16)
        self.post(away, self.land_x, 6, self.place.across)

    def pass_on(self, kind, peer, kind_there):
        v = self.held(kind)
        self.post(v, v, 6 + kind_there, peer)

    def held(self, kind):
        dy, across = {
            self.OWN: (0, 0),
            self.FROM_DOWN: (3, 0),
            self.FROM_UP: (1, 0),
            self.DOWN_ACROSS: (3, 1),
            self.UP_ACROSS: (1, 1),
            self.FAR: (2, 0),
            self.FAR_ACROSS: (2, 1),
        }[kind]
        xh = self.place.xh
        return self.slab(self.result, dy, 1 - xh if across else xh)

    def across_held(self):
        return self.slab(self.result, 0, 1 - self.place.xh)

    def finish(self):
        p = self.place
        self.wait(self.land_x, 6)
        own = self.held(self.OWN)
        own[...] = (self.local(p.xh) + self.land_x[...].astype(F32)).astype(BF16)
        self.post(own, own, 13, p.across)
        self.pass_on(self.OWN, p.up, self.FROM_DOWN)
        self.pass_on(self.OWN, p.down, self.FROM_UP)

    def get(self, kind):
        self.wait(self.held(kind), 6 + kind)

    def spread(self):
        p = self.place
        self.get(self.FROM_DOWN)
        self.pass_on(self.FROM_DOWN, p.up, self.FAR)
        self.get(self.FROM_UP)
        v = self.across_held()
        self.wait(v, 13)
        self.post(v, v, 6 + self.DOWN_ACROSS, p.up)
        self.post(v, v, 6 + self.UP_ACROSS, p.down)

    def spread_far(self):
        self.get(self.UP_ACROSS)
        self.pass_on(self.UP_ACROSS, self.place.down, self.FAR_ACROSS)
        self.get(self.DOWN_ACROSS)

    def end(self):
        self.get(self.FAR)
        self.get(self.FAR_ACROSS)


class RingGather:
    FROM_DOWN, FROM_UP, FAR = range(3)

    def __init__(self, place, wires, view):
        self.place = place
        self.wires = wires
        self.view = view
        self.first = wires.claim(6)

    def block(self, kind, half):
        dy = {self.FROM_DOWN: 3, self.FROM_UP: 1, self.FAR: 2}[kind]
        return self.view(plus(self.place.y, dy, 4), half)

    def post(self, v, kind, half, peer):
        self.wires.send(v, v, self.first + kind * 2 + half, peer, "task")

    def wait(self, kind, half):
        self.wires.arrived(self.block(kind, half), self.first + kind * 2 + half, "task")

    def open(self):
        p = self.place
        for up_half, down_half in ((0, 1), (1, 0)):
            self.post(self.view(p.y, up_half), self.FROM_DOWN, up_half, p.up)
            self.post(self.view(p.y, down_half), self.FROM_UP, down_half, p.down)

    def relay(self):
        self.wait(self.FROM_DOWN, 0)
        self.post(self.block(self.FROM_DOWN, 0), self.FAR, 0, self.place.up)
        self.wait(self.FROM_UP, 1)
        self.post(self.block(self.FROM_UP, 1), self.FAR, 1, self.place.down)

    def end(self):
        self.wait(self.FROM_DOWN, 1)
        self.wait(self.FROM_UP, 0)
        self.wait(self.FAR, 0)
        self.wait(self.FAR, 1)


class RingExchange:
    def __init__(self, place, wires, source, land):
        self.place = place
        self.wires = wires
        self.source = source
        self.land = land
        self.first = wires.claim(3)

    def open(self):
        p = self.place
        for dy in (2, 1, 3):
            y = plus(p.y, dy, 4)
            self.wires.send(
                self.source(y), self.land(4 - dy), self.first + 3 - dy, p.xh * 4 + y, "task"
            )

    def wait(self, dy):
        self.wires.arrived(self.land(dy), self.first + dy - 1, "task")


def slope(v):
    s = sigmoid(v)
    return s * (1.0 + v * (1.0 - s))


def slab_rows(height):
    return lambda ref, n: ref.at[pl.ds(pl.multiple_of(n * height, 16), height), :]


def slab_cols(ref, n):
    return ref.at[:, pl.ds(pl.multiple_of(n * 512, 512), 512)]


def popart_update(counts, totals, squares, pop_mean, pop_scale):
    mixing = counts / (counts + POPART_PRIOR)
    safe_counts = jnp.maximum(counts, 1.0)
    batch_mean = totals / safe_counts
    batch_square = squares / safe_counts
    updated_return_mean = (1.0 - mixing) * pop_mean + mixing * batch_mean
    mean_gap = batch_mean - pop_mean
    variance = (
        (1.0 - mixing) * pop_scale * pop_scale
        + mixing * (batch_square - batch_mean * batch_mean)
        + mixing * (1.0 - mixing) * mean_gap * mean_gap
    )
    return (updated_return_mean, jnp.sqrt(variance))


class AllPairs:
    def __init__(self, wires, axis, size, land):
        self.wires = wires
        self.axis = axis
        self.size = size
        self.here = lax.axis_index(axis)
        self.land = land
        self.first = wires.claim(size - 1)

    def post(self, peer_at, src):
        peer = plus(self.here, peer_at, self.size)
        self.wires.send(
            src(peer), self.land.at[peer_at - 1], self.first + peer_at - 1, peer, self.axis
        )

    def wait(self, peer_at):
        self.wires.arrived(self.land.at[peer_at - 1], self.first + peer_at - 1, self.axis)


def greet_everyone():
    barrier = pltpu.get_barrier_semaphore()
    for axis, size in (("tp", 16), ("task", 8)):
        here = lax.axis_index(axis)
        for hop in range(1, size):
            pl.semaphore_signal(
                barrier, inc=1, device_id={axis: plus(here, hop, size)}, device_id_type=MESH
            )
    pl.semaphore_wait(barrier, 22)


def lanes(shape):
    return lax.broadcasted_iota(jnp.int32, shape, 1)


def sublanes(shape):
    return lax.broadcasted_iota(jnp.int32, shape, 0)


def popart_rows(tasks, rewards, ends):
    factors = DISCOUNT * (1.0 - ends[...].astype(F32))
    gains = rewards[...]
    running = jnp.zeros((1, 32), F32)
    total = jnp.zeros((1, 32), F32)
    square = jnp.zeros((1, 32), F32)
    for t in range(14, -1, -1):
        running = gains[t : t + 1, :] + factors[t : t + 1, :] * running
        total = total + running
        square = square + running * running
    member = sublanes((128, 32)) == tasks[...] + ACTIONS
    diagonal = sublanes((128, 128)) == lanes((128, 128))
    rows = []
    for value in (jnp.full((1, 32), 15.0, F32), total, square):
        column = jnp.sum(jnp.where(member, value, 0.0), axis=1, keepdims=True)
        rows.append(jnp.sum(jnp.where(diagonal, column, 0.0), axis=0, keepdims=True))
    return jnp.concatenate([*rows, jnp.zeros((5, 128), F32)], axis=0)


def as_column(row):
    diagonal = sublanes((128, 128)) == lanes((128, 128))
    return jnp.sum(jnp.where(diagonal, row, 0.0), axis=1, keepdims=True)


def step_columns(ref, first_env):
    value = ref[...].astype(F32)
    value = jnp.concatenate([value, jnp.zeros((1, 32), F32)], axis=0)
    lane = lanes((16, 32))
    return jnp.concatenate(
        [
            jnp.sum(jnp.where(lane == first_env + e, value, 0.0), axis=1, keepdims=True)
            for e in (0, 1)
        ],
        axis=0,
    )


def loss_gradient(outputs, own, columns, mean, scale):
    action, reward, factor, behaviour = columns
    shape = (32, 128)
    lane = lanes(shape)
    frame = lax.rem(sublanes(shape), 16)
    live = frame < 15

    def later(value, by):
        return jnp.where(frame + by < 16, pltpu.roll(value, 32 - by, 0), 0.0)

    def over_lanes(mask, value):
        return jnp.broadcast_to(
            jnp.sum(jnp.where(mask, value, 0.0), axis=1, keepdims=True), shape
        )

    is_logit = lane < ACTIONS
    chosen = lane == action.astype(jnp.int32)
    log_total = jnp.log(over_lanes(is_logit, jnp.exp(jnp.where(is_logit, outputs, 0.0))))
    log_prob = jnp.where(is_logit, outputs - log_total, 0.0)
    log_policy = over_lanes(chosen, log_prob)
    env_mean = over_lanes(own, mean)
    env_scale = over_lanes(own, scale)
    norm_values = over_lanes(own, outputs)
    values = norm_values * env_scale + env_mean
    clipped = jnp.minimum(jnp.exp(log_policy - behaviour), 1.0)
    total = jnp.where(live, clipped * (reward + factor * later(values, 1) - values), 0.0)
    decay = jnp.where(live, factor * clipped, 0.0)
    for by in (1, 2, 4, 8):
        total = total + decay * later(total, by)
        decay = decay * later(decay, by)
    targets = values + total
    following = later(targets, 1)
    advantage = clipped * ((reward + factor * following - env_mean) / env_scale - norm_values)
    normed_targets = (targets - env_mean) / env_scale
    policy = jnp.where(is_logit, jnp.exp(log_prob), 0.0)
    entropy = -over_lanes(is_logit, policy * log_prob)
    d_logits = -advantage * (jnp.where(chosen, 1.0, 0.0) - policy) + ENTROPY_COST * policy * (
        log_prob + entropy
    )
    d_value = -BASELINE_COST * (normed_targets - norm_values)
    d = jnp.where(is_logit, d_logits, jnp.where(own, d_value, 0.0))
    return jnp.where(live, d * LOSS_WEIGHT, 0.0)


def step_kernel(
    own_tokens, gain, w_in, w_mix, w_out, head, vectors, tasks, actions, rewards, ends, behaviour,
    sum_out_hbm, sum_mix_hbm, sum_in_hbm, new_head, stats,
    tokens, w_in_v, w_mix_v, w_out_v, pre_in, hidden_in, residual, gain_all, normed,
    pre_out, hidden_out, head_part, head_land, d_heads, stat_own, stat_land,
    d_pre_out, d_pre_in, hidden_t, d_normed,
    hidden_ring, far_tokens, residual_ring, small_own, small_land,
    partial, twin_part, landing, twin_part_b, landing_b, arrived, gain_parts, gain_land,
    whole_out, whole_mix, whole_in, land_out, x_out, x_mix, x_in,
    sum_out, sum_mix, sum_in,
    send_sems, recv_sems, local_sems,
):
    place = Place()
    task = TaskPlace()
    wires = Wires(send_sems, recv_sems)
    gather_a, gather_b, scatter_slots = wires.claim(30), wires.claim(30), wires.claim(30)
    me = place.me
    own_cols = pl.ds(pl.multiple_of(me * 256, 256), 256)
    first = load(own_tokens, tokens.at[pl.ds(0, 512), own_cols], local_sems, 0)
    g = gain[...]
    hi = g.astype(BF16).astype(F32)
    mid = (g - hi).astype(BF16).astype(F32)
    low = g - hi - mid
    row = sublanes((16, 256))
    rows = jnp.where(row == 0, hi, jnp.where(row == 1, mid, jnp.where(row == 2, low, 0.0)))
    tokens[pl.ds(512, 16), own_cols] = rows.astype(BF16)
    greet_everyone()
    first.wait()

    def token_view(block, half):
        rows = pl.ds(0, 256) if half == 0 else pl.ds(256, 272)
        return tokens.at[rows, pl.ds(pl.multiple_of(block * 256, 256), 256)]

    gather = Gather(place, wires, token_view, gather_a)
    gather.open()
    get_in = load(w_in, w_in_v, local_sems, 1)
    get_mix = load(w_mix, w_mix_v, local_sems, 2)
    get_out = load(w_out, w_out_v, local_sems, 3)

    stat_own[...] = popart_rows(tasks, rewards, ends)
    statistics = AllPairs(wires, "task", 8, stat_land)
    for hop in range(1, 8):
        statistics.post(hop, lambda peer: stat_own)
    gather.middle()

    def slab(dz, opening=False):
        at = pl.multiple_of(plus(place.z, dz, 4) * 1024, 1024)

        def tile(m, carry):
            r = pl.ds(pl.multiple_of(m * 128, 128), 128)
            value = dot(tokens[r, pl.ds(at, 1024)], w_in_v[pl.ds(at, 1024), :])
            pre_in[r, :] = value if opening else pre_in[r, :] + value
            return carry

        lax.fori_loop(0, 4, tile, 0)

    get_in.wait()
    gather.wait_twin(gather.OWN, gather.ACROSS)
    slab(0, True)
    gather.late()
    gather.wait_twin(gather.FROM_UP, gather.UP_ACROSS)
    slab(1)
    gather.last()
    gather.wait_twin(gather.FROM_DOWN, gather.DOWN_ACROSS)
    slab(3)
    gather.wait_twin(gather.FAR, gather.FAR_ACROSS)
    slab(2)

    def activate(m, carry):
        r = pl.ds(pl.multiple_of(m * 128, 128), 128)
        v = pre_in[r, :]
        hidden = (v * sigmoid(v)).astype(BF16)
        hidden_in[r, :] = hidden
        hidden_ring[pl.ds(m * 4, 4), task.y] = hidden.reshape(4, 32, 256)
        return carry

    lax.fori_loop(0, 4, activate, 0)
    get_mix.wait()
    scatter = Scatter(place, wires, partial, twin_part, landing, scatter_slots)
    scatter.open(lambda half: wide_product(hidden_in, w_mix_v, partial, half, False))

    for_hidden = RingGather(
        task, wires, lambda y, half: hidden_ring.at[pl.ds(half * 8, 8), y]
    )
    for_hidden.open()
    core_rows = pl.ds(pl.multiple_of(place.c * 256, 256), 256)
    twin_rows = pl.ds(pl.multiple_of(256 - place.c * 256, 256), 256)
    for_tokens = RingExchange(
        task,
        wires,
        lambda y: tokens.at[core_rows, pl.ds(pl.multiple_of(y * 1024, 1024), 1024)],
        lambda dy: far_tokens.at[dy - 1, core_rows, :],
    )
    for_tokens.open()
    token_slot = wires.claim(3)
    g3 = tokens[pl.ds(512, 16), :].astype(F32)
    gain_all[...] = g3[0:1, :] + g3[1:2, :] + g3[2:3, :]
    summed = stat_own[...]
    for hop in range(1, 8):
        statistics.wait(hop)
        summed = summed + stat_land[hop - 1]
    counts, totals, squares = summed[0:1, :], summed[1:2, :], summed[2:3, :]
    bias, pop_mean, pop_scale = vectors[0:1, :], vectors[1:2, :], vectors[2:3, :]
    mean, scale = popart_update(counts, totals, squares, pop_mean, pop_scale)
    is_value = lanes((1, 128)) >= ACTIONS
    ratio = jnp.where(is_value, pop_scale / scale, 1.0)
    new_bias = jnp.where(is_value, (pop_scale * bias + pop_mean - mean) / scale, bias)
    new_head[pl.ds(0, 75), :] = (head[...].astype(F32) * as_column(ratio)[0:75, :]).astype(BF16)
    new_head[pl.ds(75, 53), :] = jnp.zeros((53, 256), BF16)
    stats[...] = jnp.concatenate([mean, scale, new_bias, jnp.zeros((5, 128), F32)], axis=0)

    scatter.finish_far()
    scatter.finish_across()
    scatter.finish_near()
    first_env = me * 2
    columns = [
        step_columns(ref, first_env) for ref in (actions, rewards, ends, behaviour)
    ]
    columns[2] = DISCOUNT * (1.0 - columns[2])
    env = [
        jnp.sum(jnp.where(lanes((1, 32)) == first_env + e, tasks[...].astype(F32), 0.0), axis=1, keepdims=True)
        for e in (0, 1)
    ]
    game = jnp.where(sublanes((32, 128)) < 16, env[0], env[1])
    own_value = lanes((32, 128)) == game.astype(jnp.int32) + ACTIONS
    own_rows = pl.ds(pl.multiple_of(me * 32, 32), 32)

    def store(half, value):
        residual[:, half_cols(half)] = (
            value + tokens[own_rows, half_cols(half)].astype(F32)
        )

    scatter.finish(store)
    for m in range(2):
        v = residual[pl.ds(m * 16, 16), :]
        inverse = lax.rsqrt(jnp.mean(v * v, axis=1, keepdims=True) + NORM_EPS)
        normed[pl.ds(pl.multiple_of(me * 32 + m * 16, 16), 16), :] = (
            v * inverse * gain_all[...]
        ).astype(BF16)
    spread = Gather(place, wires, row_view(normed), gather_b)
    spread.open()
    for_hidden.relay()
    heads = AllPairs(wires, "tp", 16, head_land)

    def out_slab(dz):
        start = plus(place.z, dz, 4) * 128
        rows = pl.ds(pl.multiple_of(start, 128), 128)
        v = dot(normed[rows, :], w_out_v[...])
        pre_out[rows, :] = v
        hidden_out[rows, :] = (v * sigmoid(v)).astype(BF16)
        head_part[rows, :] = dot(hidden_out[rows, :], new_head[...], ((1,), (1,))).astype(BF16)

    spread.middle()
    get_out.wait()
    spread.wait_twin(spread.OWN, spread.ACROSS)
    out_slab(0)
    spread.late()
    spread.wait_twin(spread.FROM_UP, spread.UP_ACROSS)
    out_slab(1)
    spread.last()
    spread.wait_twin(spread.FROM_DOWN, spread.DOWN_ACROSS)
    out_slab(3)
    spread.wait_twin(spread.FAR, spread.FAR_ACROSS)
    out_slab(2)

    def frames_of(ref):
        return lambda device: ref.at[pl.ds(pl.multiple_of(device * 32, 32), 32), :]

    for hop in range(1, 16):
        heads.post(hop, frames_of(head_part))
    for dy in (1, 2, 3):
        for_tokens.wait(dy)
        share = far_tokens.at[dy - 1, core_rows, :]
        wires.send(share, share, token_slot + dy - 1, place.partner)
    for_hidden.end()
    for b in range(4):
        hidden_t[:, b * 512 : b * 512 + 512] = (
            hidden_ring[b * 4 : b * 4 + 4].reshape(512, 256).T
        )
    outputs = head_part[own_rows, :].astype(F32)
    for hop in range(1, 16):
        heads.wait(hop)
        outputs = outputs + head_land[hop - 1].astype(F32)
    d_own = loss_gradient(outputs + new_bias, own_value, columns, mean, scale)
    d_heads[own_rows, :] = d_own.astype(BF16)
    d_slot = wires.claim(15)
    d_view = frames_of(d_heads)
    for hop in range(1, 16):
        wires.send(d_view(me), d_view(me), d_slot + hop - 1, plus(me, hop, 16))
    for hop in range(1, 16):
        wires.arrived(d_view(plus(me, 16 - hop, 16)), d_slot + hop - 1)
    wires.drain()

    def pre_gradient(m, carry):
        r = pl.ds(pl.multiple_of(m * 128, 128), 128)
        d_hidden = dot(d_heads[r, :], new_head[...])
        d_pre_out[r, :] = (d_hidden * slope(pre_out[r, :])).astype(BF16)
        return carry

    lax.fori_loop(0, 4, pre_gradient, 0)
    scatter = Scatter(place, wires, partial, twin_part_b, landing_b, scatter_slots)
    scatter.open(lambda half: wide_product(d_pre_out, w_out_v, partial, half, True))
    for_out = TaskSum(task, wires, slab_rows(512), whole_out, land_out, x_out, sum_out)
    for_mix = TaskSum(task, wires, slab_cols, whole_mix, None, x_mix, sum_mix)
    for_in = TaskSum(task, wires, slab_rows(528), whole_in, None, x_in, sum_in)

    def tall_product(left, right, whole, height, dy):
        k = plus(task.y, dy, 4)

        def tile(n, carry):
            feature = pl.multiple_of(k * 1024 + n * 256, 256)
            at = pl.multiple_of((k * 2 + n // 2) * height + lax.rem(n, 2) * 256, 16)
            value = dot(left[pl.ds(0, 512), pl.ds(feature, 256)], right[...], ((0,), (0,)))
            whole[pl.ds(at, 256), :] = value.astype(BF16)
            return carry

        lax.fori_loop(0, 4, tile, 0)

    def mix_product(part):
        def tile(n, carry):
            at = pl.multiple_of(part * 512 + n * 256, 256)
            whole_mix[:, pl.ds(at, 256)] = dot(
                hidden_t[...], residual_ring[:, pl.ds(at, 256)]
            ).astype(BF16)
            return carry

        lax.fori_loop(0, 2, tile, 0)

    def in_product(part):
        def tile(n, carry):
            at = pl.multiple_of(part * 512 + n * 256, 256)
            here = pl.ds(pl.multiple_of(task.y * 1024 + at, 256), 256)
            value = dot(tokens[pl.ds(0, 512), here], d_pre_in[task.y], ((0,), (0,)))
            for dy in (1, 2, 3):
                value = value + dot(
                    far_tokens[dy - 1, :, pl.ds(at, 256)],
                    d_pre_in[plus(task.y, dy, 4)],
                    ((0,), (0,)),
                )
            whole_in[pl.ds(pl.multiple_of(part * 528 + n * 256, 16), 256), :] = value.astype(BF16)
            return carry

        lax.fori_loop(0, 2, tile, 0)

    def out_product(dy):
        tall_product(normed, d_pre_out, whole_out, 512, dy)

    out_product(2)
    for_out.far()
    scatter.finish_far()
    out_product(1)
    out_product(3)
    for_out.near()
    scatter.finish_across()
    out_product(0)
    for_out.relay()
    scatter.finish_near()

    def store(half, value):
        d_normed[:, half_cols(half)] = value

    scatter.finish(store)
    gain_rows = jnp.zeros((8, 4096), F32)
    for m in range(2):
        r = pl.ds(m * 16, 16)
        v = residual[r, :]
        inverse = lax.rsqrt(jnp.mean(v * v, axis=1, keepdims=True) + NORM_EPS)
        d = d_normed[r, :]
        scaled = d * gain_all[...]
        inner = jnp.sum(scaled * v, axis=1, keepdims=True)
        step = inverse * scaled - v * (inverse * inverse * inverse * inner * (1.0 / 4096))
        arrived[pl.ds(pl.multiple_of(me * 32 + m * 16, 16), 16), :] = step.astype(BF16)
        d_normed[r, :] = d * v * inverse
    gather = Gather(place, wires, row_view(arrived), gather_a)
    gather.open()
    ring_rows = lambda y: pl.ds(pl.multiple_of(me * 128 + y * 32, 32), 32)
    quarter = lambda y: pl.ds(pl.multiple_of(y * 1024, 1024), 1024)
    own32 = pl.ds(pl.multiple_of(me * 32, 32), 32)
    residual_ring[ring_rows(task.y), :] = arrived[own32, quarter(task.y)]
    for_residual = RingExchange(
        task,
        wires,
        lambda y: arrived.at[own32, quarter(y)],
        lambda dy: residual_ring.at[ring_rows(plus(task.y, dy, 4)), :],
    )
    for dy in (2, 1, 3):
        y = plus(task.y, dy, 4)
        wires.send(
            arrived.at[own32, quarter(y)],
            residual_ring.at[ring_rows(task.y), :],
            for_residual.first + 3 - dy,
            task.xh * 4 + y,
            "task",
        )
    for m in range(4):
        gain_rows = gain_rows + d_normed[pl.ds(m * 8, 8), :]
    for n in range(16):
        gain_parts[n] = gain_rows[:, n * 256 : n * 256 + 256]
    gains = AllPairs(wires, "tp", 16, gain_land)
    for hop in range(1, 16):
        gains.post(hop, lambda peer: gain_parts.at[peer])

    def hidden_slab(dz):
        rows = pl.ds(pl.multiple_of(plus(place.z, dz, 4) * 128, 128), 128)
        d = dot(arrived[rows, :], w_mix_v[...], ((1,), (1,)))
        d_pre_in[task.y, rows, :] = (d * slope(pre_in[rows, :])).astype(BF16)

    gather.middle_near()
    for_out.fold()
    gather.middle_across()
    gather.middle_far()
    gather.wait_twin(gather.OWN, gather.ACROSS)
    hidden_slab(0)
    gather.late()
    for dy in (1, 3, 2):
        for_residual.wait(dy)
    ring = Gather(
        place,
        wires,
        lambda block, half: residual_ring.at[
            pl.ds(pl.multiple_of(block * 128, 128), 128), pl.ds(half * 512, 512)
        ],
        gather_b,
    )
    ring.open()
    for_out.finish()
    gather.wait_twin(gather.FROM_UP, gather.UP_ACROSS)
    hidden_slab(1)
    gather.last()
    gather.wait_twin(gather.FROM_DOWN, gather.DOWN_ACROSS)
    hidden_slab(3)
    gather.wait_twin(gather.FAR, gather.FAR_ACROSS)
    hidden_slab(2)
    for_slope = RingGather(
        task,
        wires,
        lambda y, half: d_pre_in.at[y, pl.ds(half * 256, 256), :],
    )
    for_slope.open()
    small = dot(d_heads[...], hidden_out[...], ((0,), (0,)))
    bias = jnp.sum(d_heads[...].astype(F32), axis=0, keepdims=True)
    gain_total = jnp.sum(gain_parts[me], axis=0, keepdims=True)
    for hop in range(1, 16):
        gains.wait(hop)
        gain_total = gain_total + jnp.sum(gain_land[hop - 1], axis=0, keepdims=True)
    row = sublanes((128, 256))
    bias = jnp.concatenate([bias, jnp.zeros((1, 128), F32)], axis=1)
    small_own[...] = jnp.where(
        row == 80, bias, jnp.where(row == 88, gain_total, small)
    ).astype(BF16)
    small_rows = lambda y: small_own.at[pl.ds(pl.multiple_of(y * 32, 32), 32), :]
    for_small = RingExchange(task, wires, small_rows, lambda dy: small_land.at[dy - 1])
    for_small.open()
    ring.middle_near()
    for_out.spread()
    ring.middle_across()
    for_slope.relay()
    ring.middle_far()
    ring.late()
    for dy in (1, 2, 3):
        wires.arrived(far_tokens.at[dy - 1, twin_rows, :], token_slot + dy - 1)
    extra = small_rows(task.y)[...].astype(F32)
    for dy in (1, 3, 2):
        for_small.wait(dy)
        extra = extra + small_land[dy - 1].astype(F32)
    for part in (0, 1):
        whole_in[pl.ds(part * 528 + 512, 16), :] = extra[part * 16 : part * 16 + 16, :].astype(BF16)
    for_slope.end()
    in_product(1 - task.xh)
    for_in.fold()
    ring.last()
    in_product(task.xh)
    ring.wait_twin(*range(8))
    mix_product(1 - task.xh)
    for_mix.fold()
    mix_product(task.xh)
    for_out.spread_far()
    for_in.finish()
    for_in.spread()
    for_mix.finish()
    for_in.spread_far()
    for_out.end()
    keep_out = load(sum_out, sum_out_hbm, local_sems, 4)
    for_mix.spread()
    for_in.end()
    keep_in = load(sum_in, sum_in_hbm, local_sems, 6)
    for_mix.spread_far()
    for_mix.end()
    keep_mix = load(sum_mix, sum_mix_hbm, local_sems, 5)
    wires.drain()
    for keep in (keep_out, keep_mix, keep_in):
        keep.wait()


def finish_kernel(
    sum_out, sum_mix, sum_in, new_head, stats,
    grad_in, grad_mix, grad_out, gain, head, bias, head_now, bias_now, mean, scale,
    out_b, mix_b, in_b, small_b, out_f, mix_f, in_f, sems,
):
    gets = []
    for n in range(8):
        r = pl.ds(n * 512, 512)
        gets.append(load(sum_in.at[pl.ds(n * 528, 512), :], in_b.at[r, :], sems, n))
    for n in range(8):
        gets.append(
            load(sum_in.at[pl.ds(n * 528 + 512, 16), :], small_b.at[pl.ds(n * 16, 16), :], sems, 8 + n)
        )
    for n in range(4):
        r = pl.ds(n * 64, 64)
        gets.append(load(sum_mix.at[r, :], mix_b.at[r, :], sems, 16 + n))
    for n in range(8):
        r = pl.ds(n * 512, 512)
        gets.append(load(sum_out.at[r, :], out_b.at[r, :], sems, 20 + n))
    puts = []
    for n in range(8):
        r = pl.ds(n * 512, 512)
        gets[n].wait()
        in_f[r, :] = in_b[r, :].astype(F32)
        puts.append(load(in_f.at[r, :], grad_in.at[r, :], sems, 28 + n))
    for n in range(4):
        r = pl.ds(n * 64, 64)
        gets[16 + n].wait()
        mix_f[r, :] = mix_b[r, :].astype(F32)
        puts.append(load(mix_f.at[r, :], grad_mix.at[r, :], sems, 36 + n))
    for n in range(8):
        r = pl.ds(n * 512, 512)
        gets[20 + n].wait()
        out_f[r, :] = out_b[r, :].astype(F32)
        puts.append(load(out_f.at[r, :], grad_out.at[r, :], sems, 40 + n))
    for n in range(8):
        gets[8 + n].wait()
    small = small_b[...].astype(F32)
    head[...] = small[0:75, :]
    bias[...] = small[80:81, 0:75]
    gain[...] = small[88:89, :]
    head_now[...] = new_head[0:75, :]
    values = pltpu.roll(stats[...], 128 - ACTIONS, 1)
    mean[...] = values[0:1, 0:TASKS]
    scale[...] = values[1:2, 0:TASKS]
    bias_now[...] = stats[2:3, 0:75]
    for put in puts:
        put.wait()


def hbm():
    return pl.BlockSpec(memory_space=pltpu.HBM)


def vmem():
    return pl.BlockSpec(memory_space=pltpu.VMEM)


def step_call(*arguments):
    v, h = vmem(), hbm()
    scratch = [
        ((528, 4096), BF16), ((4096, 256), BF16), ((256, 4096), BF16), ((4096, 256), BF16),
        ((512, 256), F32), ((512, 256), BF16), ((32, 4096), F32), ((1, 4096), F32),
        ((512, 4096), BF16),
        ((512, 256), F32), ((512, 256), BF16), ((512, 128), BF16), ((15, 32, 128), BF16),
        ((512, 128), BF16), ((8, 128), F32), ((7, 8, 128), F32),
        ((512, 256), BF16), ((4, 512, 256), BF16), ((256, 2048), BF16), ((32, 4096), F32),
        ((16, 4, 32, 256), BF16), ((3, 512, 1024), BF16), ((2048, 1024), BF16),
        ((128, 256), BF16), ((3, 32, 256), BF16),
        ((512, 4096), BF16), ((8, 32, 4096), BF16), ((7, 32, 4096), BF16),
        ((8, 32, 4096), BF16), ((7, 32, 4096), BF16), ((512, 4096), BF16),
        ((16, 8, 256), F32), ((15, 8, 256), F32),
        ((4096, 256), BF16), ((256, 1024), BF16), ((1056, 256), BF16),
        ((3, 2, 512, 256), BF16),
        ((512, 256), BF16), ((256, 512), BF16), ((528, 256), BF16),
        ((4096, 256), BF16), ((256, 4096), BF16), ((4224, 256), BF16),
    ]
    return pl.pallas_call(
        step_kernel,
        out_shape=[
            jax.ShapeDtypeStruct((4096, 256), BF16),
            jax.ShapeDtypeStruct((256, 4096), BF16),
            jax.ShapeDtypeStruct((4224, 256), BF16),
            jax.ShapeDtypeStruct((128, 256), BF16),
            jax.ShapeDtypeStruct((8, 128), F32),
        ],
        in_specs=[h, v, h, h, h, v, v, v, v, v, v, v],
        out_specs=[h, h, h, v, v],
        scratch_shapes=[pltpu.VMEM(*s) for s in scratch]
        + [pltpu.SemaphoreType.DMA((SENDS,)), pltpu.SemaphoreType.DMA((RECEIVES,)), pltpu.SemaphoreType.DMA((7,))],
        compiler_params=pltpu.CompilerParams(
            collective_id=0, has_side_effects=True, vmem_limit_bytes=63 * 2**20
        ),
        name="step",
    )(*arguments)


def finish_call(*arguments):
    v, h = vmem(), hbm()
    return pl.pallas_call(
        finish_kernel,
        out_shape=[
            jax.ShapeDtypeStruct((4096, 256), F32),
            jax.ShapeDtypeStruct((256, 4096), F32),
            jax.ShapeDtypeStruct((4096, 256), F32),
            jax.ShapeDtypeStruct((1, 256), F32),
            jax.ShapeDtypeStruct((75, 256), F32),
            jax.ShapeDtypeStruct((1, 75), F32),
            jax.ShapeDtypeStruct((75, 256), BF16),
            jax.ShapeDtypeStruct((1, 75), F32),
            jax.ShapeDtypeStruct((1, TASKS), F32),
            jax.ShapeDtypeStruct((1, TASKS), F32),
        ],
        in_specs=[h, h, h, v, v],
        out_specs=[h, h, h, v, v, v, v, v, v, v],
        scratch_shapes=[
            pltpu.VMEM((4096, 256), BF16),
            pltpu.VMEM((256, 4096), BF16),
            pltpu.VMEM((4096, 256), BF16),
            pltpu.VMEM((128, 256), BF16),
            pltpu.VMEM((4096, 256), F32),
            pltpu.VMEM((256, 4096), F32),
            pltpu.VMEM((4096, 256), F32),
            pltpu.SemaphoreType.DMA((48,)),
        ],
        compiler_params=pltpu.CompilerParams(vmem_limit_bytes=63 * 2**20),
        name="finish",
    )(*arguments)


def on_device(
    observations, gain, w_in, w_mix, w_out, w_head, head_bias, pop_mean, pop_scale,
    task_indices, actions, rewards, episode_ends, behaviour_log_prob,
):
    pad = (ACTIONS, 128 - ACTIONS - TASKS)
    vectors = jnp.stack(
        [
            jnp.pad(head_bias, (0, 128 - ACTIONS - TASKS)),
            jnp.pad(pop_mean, pad),
            jnp.pad(pop_scale, pad, constant_values=1.0),
        ]
    )
    sums = step_call(
        observations.reshape(512, 256),
        gain.reshape(1, 256),
        w_in,
        w_mix,
        w_out,
        w_head.T,
        vectors,
        task_indices.reshape(1, 32),
        actions.T,
        rewards.T,
        episode_ends.T,
        behaviour_log_prob.T,
    )
    (
        grad_in, grad_mix, grad_out, grad_gain, grad_head, grad_bias,
        new_head, new_bias, mean, scale,
    ) = finish_call(*sums)
    return (
        grad_in,
        grad_mix,
        grad_out,
        grad_gain.reshape(256),
        grad_head.T,
        grad_bias.reshape(75),
        new_head.T,
        new_bias.reshape(75),
        mean.reshape(TASKS),
        scale.reshape(TASKS),
    )


def solution(mesh):
    in_specs = (
        P("task", None, "tp"),
        P("tp"),
        P(None, "tp"),
        P("tp", None),
        P(None, "tp"),
        P("tp", None),
        P(),
        P(),
        P(),
        P("task"),
        P("task", None),
        P("task", None),
        P("task", None),
        P("task", None),
    )
    out_specs = (
        P(None, "tp"),
        P("tp", None),
        P(None, "tp"),
        P("tp"),
        P("tp", None),
        P(),
        P("tp", None),
        P(),
        P(),
        P(),
    )
    return jax.shard_map(
        on_device, mesh=mesh, in_specs=in_specs, out_specs=out_specs, check_vma=False
    )
```

```python
import jax
import jax.numpy as jnp
from jax import lax
from jax.experimental import pallas as pl
from jax.experimental.pallas import tpu as pltpu
from jax.sharding import PartitionSpec as P

ACTIONS = 18
TASKS = 57
DISCOUNT = 0.99
BASELINE_COST = 0.5
ENTROPY_COST = 0.01
POPART_PRIOR = 64.0
NORM_EPS = 1e-06
LOSS_WEIGHT = 256**-0.5
SENDS = 156
RECEIVES = 216


MESH = pl.DeviceIdType.MESH
F32 = jnp.float32
BF16 = jnp.bfloat16
HALVES = (0, 1)


def plus(a, b, n):
    return lax.rem(a + b, n)


class Place:
    def __init__(self):
        self.me = lax.axis_index("tp")
        self.z = self.me // 4
        self.x = lax.rem(self.me // 2, 2)
        self.c = lax.rem(self.me, 2)
        self.across = self.at(0, 1)
        self.up = self.at(1, 0)
        self.down = self.at(3, 0)
        self.partner = self.at(0, 0, 1)

    def at(self, dz, dx, dc=0):
        return (plus(self.z, dz, 4) * 2 + plus(self.x, dx, 2)) * 2 + plus(self.c, dc, 2)


class Wires:
    def __init__(self, send_sems, recv_sems):
        self.send_sems = send_sems
        self.recv_sems = recv_sems
        self.sent = []
        self.slots = 0

    def claim(self, count):
        first = self.slots
        self.slots += count
        return first

    def send(self, src, dst, slot, peer, axis="tp"):
        copy = pltpu.make_async_remote_copy(
            src_ref=src,
            dst_ref=dst,
            send_sem=self.send_sems.at[len(self.sent)],
            recv_sem=self.recv_sems.at[slot],
            device_id={axis: peer},
            device_id_type=MESH,
        )
        copy.start()
        self.sent.append(copy)

    def arrived(self, dst, slot, axis="tp"):
        pltpu.make_async_remote_copy(
            src_ref=dst,
            dst_ref=dst,
            send_sem=self.send_sems.at[0],
            recv_sem=self.recv_sems.at[slot],
            device_id={axis: lax.axis_index(axis)},
            device_id_type=MESH,
        ).wait_recv()

    def drain(self):
        for copy in self.sent:
            copy.wait_send()
        self.sent = []


class Gather:
    ACROSS, FROM_DOWN, FROM_UP, DOWN_ACROSS, UP_ACROSS, FAR, FAR_ACROSS, OWN = range(8)

    def __init__(self, place, wires, view, first):
        self.place = place
        self.wires = wires
        self.view = view
        self.first = first
        p = place
        self.block = {
            self.ACROSS: p.at(0, 1),
            self.FROM_DOWN: p.at(3, 0),
            self.FROM_UP: p.at(1, 0),
            self.DOWN_ACROSS: p.at(3, 1),
            self.UP_ACROSS: p.at(1, 1),
            self.FAR: p.at(2, 0),
            self.FAR_ACROSS: p.at(2, 1),
            self.OWN: p.me,
        }
        self.twin = {k: plus(b, 0, 16) + 1 - 2 * p.c for k, b in self.block.items()}

    def slot(self, kind, half):
        return self.first + kind * 2 + half

    def twin_slot(self, kind, half):
        return self.first + 14 + kind * 2 + half

    def pass_on(self, kind, half, peer, kind_there):
        v = self.view(self.block[kind], half)
        self.wires.send(v, v, self.slot(kind_there, half), peer)

    def to_twin(self, kind, half):
        v = self.view(self.block[kind], half)
        self.wires.send(v, v, self.twin_slot(kind, half), self.place.partner)

    def wait(self, kind, half):
        self.wires.arrived(self.view(self.block[kind], half), self.slot(kind, half))

    def wait_twin(self, *kinds):
        for kind in kinds:
            for half in HALVES:
                self.wires.arrived(
                    self.view(self.twin[kind], half), self.twin_slot(kind, half)
                )

    def open(self):
        p = self.place
        for half in HALVES:
            self.pass_on(self.OWN, half, p.up, self.FROM_DOWN)
            self.pass_on(self.OWN, half, p.down, self.FROM_UP)
            self.pass_on(self.OWN, half, p.across, self.ACROSS)
            self.to_twin(self.OWN, half)

    def middle(self):
        self.middle_near()
        self.middle_across()
        self.middle_far()

    def middle_near(self):
        p = self.place
        self.wait(self.FROM_DOWN, 0)
        self.pass_on(self.FROM_DOWN, 0, p.up, self.FAR)
        self.to_twin(self.FROM_DOWN, 0)
        self.wait(self.FROM_UP, 0)
        self.to_twin(self.FROM_UP, 0)
        self.wait(self.ACROSS, 0)
        self.pass_on(self.ACROSS, 0, p.down, self.UP_ACROSS)
        self.wait(self.FROM_UP, 1)
        self.pass_on(self.FROM_UP, 1, p.down, self.FAR)
        self.pass_on(self.ACROSS, 0, p.up, self.DOWN_ACROSS)
        self.to_twin(self.ACROSS, 0)
        self.to_twin(self.FROM_UP, 1)

    def middle_across(self):
        p = self.place
        self.wait(self.FROM_DOWN, 1)
        self.to_twin(self.FROM_DOWN, 1)
        self.wait(self.ACROSS, 1)
        self.pass_on(self.ACROSS, 1, p.up, self.DOWN_ACROSS)
        self.pass_on(self.ACROSS, 1, p.down, self.UP_ACROSS)
        self.to_twin(self.ACROSS, 1)

    def middle_far(self):
        for half in HALVES:
            self.wait(self.FAR, half)
            self.pass_on(self.FAR, half, self.place.across, self.FAR_ACROSS)
            self.to_twin(self.FAR, half)

    def late(self):
        for half in HALVES:
            for kind in (self.DOWN_ACROSS, self.UP_ACROSS):
                self.wait(kind, half)
                self.to_twin(kind, half)

    def last(self):
        for half in HALVES:
            self.wait(self.FAR_ACROSS, half)
            self.to_twin(self.FAR_ACROSS, half)


def half_cols(half):
    return pl.ds(half * 2048, 2048)


class Scatter:
    G, D, E, F, A, B, C = range(7)
    ORDER = ((2, 1), (1, 1), (3, 1), (1, 0), (3, 0), (2, 0), (0, 1), (0, 0))

    def __init__(self, place, wires, partial, twin_part, landing, first):
        self.place = place
        self.wires = wires
        self.partial = partial
        self.twin_part = twin_part
        self.landing = landing
        self.first = first

    def rows(self, where, dc=0):
        return pl.ds(pl.multiple_of(self.place.at(*where, dc) * 32, 32), 32)

    def mine(self, where, half):
        return self.partial.at[self.rows(where), half_cols(half)]

    def twins(self, where, half):
        return self.twin_part.at[self.ORDER.index(where), :, half_cols(half)]

    def land(self, kind, half):
        return self.landing.at[kind, :, half_cols(half)]

    def total(self, where, half, kinds=(), waited=()):
        slot = self.first + 14 + self.ORDER.index(where) * 2 + half
        if (where, half) not in self.seen:
            self.wires.arrived(self.twins(where, half), slot)
            self.seen.add((where, half))
        for kind in kinds:
            self.wires.arrived(self.land(kind, half), self.first + kind * 2 + half)
        value = self.mine(where, half)[...].astype(F32) + self.twins(where, half)[...].astype(F32)
        for kind in kinds:
            value = value + self.land(kind, half)[...].astype(F32)
        return value

    def forward(self, where, half, kinds, peer, kind_there):
        self.mine(where, half)[...] = self.total(where, half, kinds).astype(BF16)
        self.wires.send(
            self.mine(where, half),
            self.land(kind_there, half),
            self.first + kind_there * 2 + half,
            peer,
        )

    def open(self, produce, between=None):
        self.seen = set()
        p = self.place
        for half in HALVES:
            produce(half)
            for where in self.ORDER:
                self.wires.send(
                    self.partial.at[self.rows(where, 1), half_cols(half)],
                    self.twins(where, half),
                    self.first + 14 + self.ORDER.index(where) * 2 + half,
                    p.partner,
                )
            if half == 1 and between is not None:
                between()
            self.forward((2, 1), half, (), p.across, self.G)
            self.forward((1, 1), half, (), p.up, self.D)
            self.forward((3, 1), half, (), p.down, self.E)
        self.forward((1, 0), 1, (), p.up, self.B)
        self.forward((3, 0), 0, (), p.down, self.C)

    def finish_far(self):
        p = self.place
        self.forward((2, 0), 0, (self.G,), p.up, self.F)
        self.forward((2, 0), 1, (self.G,), p.down, self.F)

    def finish_across(self):
        for half in HALVES:
            self.forward((0, 1), half, (self.D, self.E), self.place.across, self.A)

    def finish_near(self):
        p = self.place
        self.forward((1, 0), 0, (self.F,), p.up, self.B)
        self.forward((3, 0), 1, (self.F,), p.down, self.C)

    def finish(self, store):
        for half in HALVES:
            store(half, self.total((0, 0), half, (self.A, self.B, self.C)))


def sigmoid(v):
    return 1.0 / (1.0 + jnp.exp(-v))


def dot(a, b, contract=((1,), (0,))):
    return lax.dot_general(a, b, (contract, ((), ())), preferred_element_type=F32)


def load(src, dst, sems, at):
    copy = pltpu.make_async_copy(src, dst, sems.at[at])
    copy.start()
    return copy


def wide_product(left, right, partial, half, transposed):
    def tile(n, carry):
        at = pl.multiple_of(half * 2048 + n * 256, 256)
        if transposed:
            value = dot(left[...], right[pl.ds(at, 256), :], ((1,), (1,)))
        else:
            value = dot(left[...], right[:, pl.ds(at, 256)])
        partial[:, pl.ds(at, 256)] = value.astype(BF16)
        return carry

    lax.fori_loop(0, 8, tile, 0)


def row_view(ref):
    return lambda block, half: ref.at[
        pl.ds(pl.multiple_of(block * 32, 32), 32), half_cols(half)
    ]


class TaskPlace:
    def __init__(self):
        task = lax.axis_index("task")
        self.xh = task // 4
        self.y = lax.rem(task, 4)
        self.up = self.xh * 4 + plus(self.y, 1, 4)
        self.down = self.xh * 4 + plus(self.y, 3, 4)
        self.across = (1 - self.xh) * 4 + self.y


class TaskSum:
    F, B, C = range(3)
    OWN, FROM_DOWN, FROM_UP, DOWN_ACROSS, UP_ACROSS, FAR, FAR_ACROSS = range(7)

    def __init__(self, place, wires, view, whole, land, land_x, result):
        self.place = place
        self.wires = wires
        self.view = view
        self.whole = whole
        self.land = land
        self.land_x = land_x
        self.result = result
        self.first = wires.claim(14)

    def slab(self, ref, dy, part):
        return self.view(ref, plus(self.place.y, dy, 4) * 2 + part)

    def post(self, src, dst, slot, peer):
        self.wires.send(src, dst, self.first + slot, peer, "task")

    def wait(self, dst, slot):
        self.wires.arrived(dst, self.first + slot, "task")

    def far(self):
        p = self.place
        self.post(self.slab(self.whole, 2, 0), self.land.at[self.F, 0], 0, p.up)
        self.post(self.slab(self.whole, 2, 1), self.land.at[self.F, 1], 1, p.down)

    def near(self):
        p = self.place
        self.post(self.slab(self.whole, 1, 1), self.land.at[self.B, 1], 3, p.up)
        self.post(self.slab(self.whole, 3, 0), self.land.at[self.C, 0], 4, p.down)

    def relay(self):
        p = self.place
        for dy, part, kind, slot, peer in ((1, 0, self.B, 2, p.up), (3, 1, self.C, 5, p.down)):
            self.wait(self.land.at[self.F, part], part)
            own = self.slab(self.whole, dy, part)
            total = own[...].astype(F32) + self.land[self.F, part].astype(F32)
            own[...] = total.astype(BF16)
            self.post(own, self.land.at[kind, part], slot, peer)

    def local(self, part):
        if self.land is None:
            return self.view(self.whole, part)[...].astype(F32)
        return (
            self.slab(self.whole, 0, part)[...].astype(F32)
            + self.land[self.B, part].astype(F32)
            + self.land[self.C, part].astype(F32)
        )

    def fold(self):
        if self.land is None:
            away = self.view(self.whole, 1 - self.place.xh)
            self.post(away, self.land_x, 6, self.place.across)
            return
        for kind, part, slot in ((self.B, 1, 3), (self.C, 0, 4), (self.B, 0, 2), (self.C, 1, 5)):
            self.wait(self.land.at[kind, part], slot)
        other = 1 - self.place.xh
        away = self.slab(self.whole, 0, other)
        away[...] = self.local(other).astype(BF16)
        self.post(away, self.land_x, 6, self.place.across)

    def pass_on(self, kind, peer, kind_there):
        v = self.held(kind)
        self.post(v, v, 6 + kind_there, peer)

    def held(self, kind):
        dy, across = {
            self.OWN: (0, 0),
            self.FROM_DOWN: (3, 0),
            self.FROM_UP: (1, 0),
            self.DOWN_ACROSS: (3, 1),
            self.UP_ACROSS: (1, 1),
            self.FAR: (2, 0),
            self.FAR_ACROSS: (2, 1),
        }[kind]
        xh = self.place.xh
        return self.slab(self.result, dy, 1 - xh if across else xh)

    def across_held(self):
        return self.slab(self.result, 0, 1 - self.place.xh)

    def finish(self):
        p = self.place
        self.wait(self.land_x, 6)
        own = self.held(self.OWN)
        own[...] = (self.local(p.xh) + self.land_x[...].astype(F32)).astype(BF16)
        self.post(own, own, 13, p.across)
        self.pass_on(self.OWN, p.up, self.FROM_DOWN)
        self.pass_on(self.OWN, p.down, self.FROM_UP)

    def get(self, kind):
        self.wait(self.held(kind), 6 + kind)

    def spread(self):
        p = self.place
        self.get(self.FROM_DOWN)
        self.pass_on(self.FROM_DOWN, p.up, self.FAR)
        self.get(self.FROM_UP)
        v = self.across_held()
        self.wait(v, 13)
        self.post(v, v, 6 + self.DOWN_ACROSS, p.up)
        self.post(v, v, 6 + self.UP_ACROSS, p.down)

    def spread_far(self):
        self.get(self.UP_ACROSS)
        self.pass_on(self.UP_ACROSS, self.place.down, self.FAR_ACROSS)
        self.get(self.DOWN_ACROSS)

    def end(self):
        self.get(self.FAR)
        self.get(self.FAR_ACROSS)


class RingGather:
    FROM_DOWN, FROM_UP, FAR = range(3)

    def __init__(self, place, wires, view, pieces):
        self.place = place
        self.wires = wires
        self.view = view
        self.pieces = pieces
        self.first = wires.claim(3 * pieces)

    def block(self, kind, piece):
        dy = {self.FROM_DOWN: 3, self.FROM_UP: 1, self.FAR: 2}[kind]
        return self.view(plus(self.place.y, dy, 4), piece)

    def post(self, v, kind, piece, peer):
        self.wires.send(v, v, self.first + kind * self.pieces + piece, peer, "task")

    def wait(self, kind, piece):
        self.wires.arrived(
            self.block(kind, piece), self.first + kind * self.pieces + piece, "task"
        )

    def open(self, piece):
        p = self.place
        v = self.view(p.y, piece)
        self.post(v, self.FROM_DOWN, piece, p.up)
        self.post(v, self.FROM_UP, piece, p.down)

    def relay(self, piece):
        kind = self.FROM_UP if piece % 2 else self.FROM_DOWN
        self.wait(kind, piece)
        peer = self.place.down if piece % 2 else self.place.up
        self.post(self.block(kind, piece), self.FAR, piece, peer)

    def end(self):
        for piece in range(self.pieces):
            self.wait(self.FROM_DOWN if piece % 2 else self.FROM_UP, piece)
            self.wait(self.FAR, piece)


class RingExchange:
    def __init__(self, place, wires, source, land):
        self.place = place
        self.wires = wires
        self.source = source
        self.land = land
        self.first = wires.claim(3)

    def open(self):
        p = self.place
        for dy in (2, 1, 3):
            y = plus(p.y, dy, 4)
            self.wires.send(
                self.source(y), self.land(4 - dy), self.first + 3 - dy, p.xh * 4 + y, "task"
            )

    def wait(self, dy):
        self.wires.arrived(self.land(dy), self.first + dy - 1, "task")


def slope(v):
    s = sigmoid(v)
    return s * (1.0 + v * (1.0 - s))


def slab_rows(height):
    return lambda ref, n: ref.at[pl.ds(pl.multiple_of(n * height, 16), height), :]


def slab_cols(ref, n):
    return ref.at[:, pl.ds(pl.multiple_of(n * 512, 512), 512)]


def popart_update(counts, totals, squares, pop_mean, pop_scale):
    mixing = counts / (counts + POPART_PRIOR)
    safe_counts = jnp.maximum(counts, 1.0)
    batch_mean = totals / safe_counts
    batch_square = squares / safe_counts
    updated_return_mean = (1.0 - mixing) * pop_mean + mixing * batch_mean
    mean_gap = batch_mean - pop_mean
    variance = (
        (1.0 - mixing) * pop_scale * pop_scale
        + mixing * (batch_square - batch_mean * batch_mean)
        + mixing * (1.0 - mixing) * mean_gap * mean_gap
    )
    return (updated_return_mean, jnp.sqrt(variance))


class AllPairs:
    def __init__(self, wires, axis, size, land):
        self.wires = wires
        self.axis = axis
        self.size = size
        self.here = lax.axis_index(axis)
        self.land = land
        self.first = wires.claim(size - 1)

    def post(self, peer_at, src):
        peer = plus(self.here, peer_at, self.size)
        self.wires.send(
            src(peer), self.land.at[peer_at - 1], self.first + peer_at - 1, peer, self.axis
        )

    def wait(self, peer_at):
        self.wires.arrived(self.land.at[peer_at - 1], self.first + peer_at - 1, self.axis)


def greet_everyone():
    barrier = pltpu.get_barrier_semaphore()
    for axis, size in (("tp", 16), ("task", 8)):
        here = lax.axis_index(axis)
        for hop in range(1, size):
            pl.semaphore_signal(
                barrier, inc=1, device_id={axis: plus(here, hop, size)}, device_id_type=MESH
            )
    pl.semaphore_wait(barrier, 22)


def lanes(shape):
    return lax.broadcasted_iota(jnp.int32, shape, 1)


def sublanes(shape):
    return lax.broadcasted_iota(jnp.int32, shape, 0)


def popart_rows(tasks, rewards, ends):
    factors = DISCOUNT * (1.0 - ends[...].astype(F32))
    gains = rewards[...]
    running = jnp.zeros((1, 32), F32)
    total = jnp.zeros((1, 32), F32)
    square = jnp.zeros((1, 32), F32)
    for t in range(14, -1, -1):
        running = gains[t : t + 1, :] + factors[t : t + 1, :] * running
        total = total + running
        square = square + running * running
    member = sublanes((128, 32)) == tasks[...] + ACTIONS
    diagonal = sublanes((128, 128)) == lanes((128, 128))
    rows = []
    for value in (jnp.full((1, 32), 15.0, F32), total, square):
        column = jnp.sum(jnp.where(member, value, 0.0), axis=1, keepdims=True)
        rows.append(jnp.sum(jnp.where(diagonal, column, 0.0), axis=0, keepdims=True))
    return jnp.concatenate([*rows, jnp.zeros((5, 128), F32)], axis=0)


def as_column(row):
    diagonal = sublanes((128, 128)) == lanes((128, 128))
    return jnp.sum(jnp.where(diagonal, row, 0.0), axis=1, keepdims=True)


def step_columns(ref, first_env):
    value = ref[...].astype(F32)
    value = jnp.concatenate([value, jnp.zeros((1, 32), F32)], axis=0)
    lane = lanes((16, 32))
    return jnp.concatenate(
        [
            jnp.sum(jnp.where(lane == first_env + e, value, 0.0), axis=1, keepdims=True)
            for e in (0, 1)
        ],
        axis=0,
    )


def loss_gradient(outputs, own, columns, mean, scale):
    action, reward, factor, behaviour = columns
    shape = (32, 128)
    lane = lanes(shape)
    frame = lax.rem(sublanes(shape), 16)
    live = frame < 15

    def later(value, by):
        return jnp.where(frame + by < 16, pltpu.roll(value, 32 - by, 0), 0.0)

    def over_lanes(mask, value):
        return jnp.broadcast_to(
            jnp.sum(jnp.where(mask, value, 0.0), axis=1, keepdims=True), shape
        )

    is_logit = lane < ACTIONS
    chosen = lane == action.astype(jnp.int32)
    log_total = jnp.log(over_lanes(is_logit, jnp.exp(jnp.where(is_logit, outputs, 0.0))))
    log_prob = jnp.where(is_logit, outputs - log_total, 0.0)
    log_policy = over_lanes(chosen, log_prob)
    env_mean = over_lanes(own, mean)
    env_scale = over_lanes(own, scale)
    norm_values = over_lanes(own, outputs)
    values = norm_values * env_scale + env_mean
    clipped = jnp.minimum(jnp.exp(log_policy - behaviour), 1.0)
    total = jnp.where(live, clipped * (reward + factor * later(values, 1) - values), 0.0)
    decay = jnp.where(live, factor * clipped, 0.0)
    for by in (1, 2, 4, 8):
        total = total + decay * later(total, by)
        decay = decay * later(decay, by)
    targets = values + total
    following = later(targets, 1)
    advantage = clipped * ((reward + factor * following - env_mean) / env_scale - norm_values)
    normed_targets = (targets - env_mean) / env_scale
    policy = jnp.where(is_logit, jnp.exp(log_prob), 0.0)
    entropy = -over_lanes(is_logit, policy * log_prob)
    d_logits = -advantage * (jnp.where(chosen, 1.0, 0.0) - policy) + ENTROPY_COST * policy * (
        log_prob + entropy
    )
    d_value = -BASELINE_COST * (normed_targets - norm_values)
    d = jnp.where(is_logit, d_logits, jnp.where(own, d_value, 0.0))
    return jnp.where(live, d * LOSS_WEIGHT, 0.0)


def step_kernel(
    own_tokens, gain, w_in, w_mix, w_out, head, head_bias, old_mean, old_scale, tasks, actions, rewards, ends, behaviour,
    sum_out_hbm, sum_mix_hbm, sum_in_hbm, new_head, stats,
    tokens, w_in_v, w_mix_v, w_out_v, pre_in, hidden_in, residual, gain_all, normed,
    pre_out, hidden_out, head_part, head_land, d_heads, stat_own, stat_land,
    d_pre_out, d_pre_in, hidden_t, d_normed,
    hidden_ring, far_tokens, residual_ring, small_own, small_land,
    partial, twin_part, landing, twin_part_b, landing_b, arrived, gain_parts, gain_land,
    whole_out, whole_mix, whole_in, land_out, x_out, x_mix, x_in,
    sum_out, sum_mix, sum_in,
    send_sems, recv_sems, local_sems,
):
    place = Place()
    task = TaskPlace()
    wires = Wires(send_sems, recv_sems)
    gather_a, gather_b, scatter_slots = wires.claim(30), wires.claim(30), wires.claim(30)
    me = place.me
    own_cols = pl.ds(pl.multiple_of(me * 256, 256), 256)
    first = load(own_tokens, tokens.at[pl.ds(0, 512), own_cols], local_sems, 0)
    g = gain[...]
    hi = g.astype(BF16).astype(F32)
    mid = (g - hi).astype(BF16).astype(F32)
    low = g - hi - mid
    row = sublanes((16, 256))
    rows = jnp.where(row == 0, hi, jnp.where(row == 1, mid, jnp.where(row == 2, low, 0.0)))
    tokens[pl.ds(512, 16), own_cols] = rows.astype(BF16)
    greet_everyone()
    first.wait()

    def token_view(block, half):
        rows = pl.ds(0, 256) if half == 0 else pl.ds(256, 272)
        return tokens.at[rows, pl.ds(pl.multiple_of(block * 256, 256), 256)]

    gather = Gather(place, wires, token_view, gather_a)
    gather.open()
    get_in = load(w_in, w_in_v, local_sems, 1)
    get_mix = load(w_mix, w_mix_v, local_sems, 2)
    get_out = load(w_out, w_out_v, local_sems, 3)

    stat_own[...] = popart_rows(tasks, rewards, ends)
    statistics = AllPairs(wires, "task", 8, stat_land)
    for hop in range(1, 8):
        statistics.post(hop, lambda peer: stat_own)
    gather.middle()

    def slab(dz, opening=False):
        at = pl.multiple_of(plus(place.z, dz, 4) * 1024, 1024)

        def tile(m, carry):
            r = pl.ds(pl.multiple_of(m * 128, 128), 128)
            value = dot(tokens[r, pl.ds(at, 1024)], w_in_v[pl.ds(at, 1024), :])
            pre_in[r, :] = value if opening else pre_in[r, :] + value
            return carry

        lax.fori_loop(0, 4, tile, 0)

    get_in.wait()
    gather.wait_twin(gather.OWN, gather.ACROSS)
    slab(0, True)
    gather.late()
    gather.wait_twin(gather.FROM_UP, gather.UP_ACROSS)
    slab(1)
    gather.last()
    gather.wait_twin(gather.FROM_DOWN, gather.DOWN_ACROSS)
    slab(3)
    gather.wait_twin(gather.FAR, gather.FAR_ACROSS)
    slab(2)

    def activate(m, carry):
        r = pl.ds(pl.multiple_of(m * 128, 128), 128)
        v = pre_in[r, :]
        hidden = (v * sigmoid(v)).astype(BF16)
        hidden_in[r, :] = hidden
        hidden_ring[pl.ds(m * 4, 4), task.y] = hidden.reshape(4, 32, 256)
        return carry

    lax.fori_loop(0, 4, activate, 0)
    get_mix.wait()
    scatter = Scatter(place, wires, partial, twin_part, landing, scatter_slots)
    scatter.open(lambda half: wide_product(hidden_in, w_mix_v, partial, half, False))

    for_hidden = RingGather(
        task, wires, lambda y, half: hidden_ring.at[pl.ds(half * 8, 8), y], 2
    )
    for_hidden.open(0)
    for_hidden.open(1)
    core_rows = pl.ds(pl.multiple_of(place.c * 256, 256), 256)
    twin_rows = pl.ds(pl.multiple_of(256 - place.c * 256, 256), 256)
    for_tokens = RingExchange(
        task,
        wires,
        lambda y: tokens.at[core_rows, pl.ds(pl.multiple_of(y * 1024, 1024), 1024)],
        lambda dy: far_tokens.at[dy - 1, core_rows, :],
    )
    for_tokens.open()
    token_slot = wires.claim(3)
    g3 = tokens[pl.ds(512, 16), :].astype(F32)
    gain_all[...] = g3[0:1, :] + g3[1:2, :] + g3[2:3, :]
    summed = stat_own[...]
    for hop in range(1, 8):
        statistics.wait(hop)
        summed = summed + stat_land[hop - 1]
    counts, totals, squares = summed[0:1, :], summed[1:2, :], summed[2:3, :]
    small_rows = (head_bias, old_mean, old_scale)
    bias, pop_mean, pop_scale = (
        jnp.concatenate(
            [ref[...], jnp.full((1, 128 - ref.shape[1]), fill, F32)], axis=1
        )
        for ref, fill in zip(small_rows, (0.0, 0.0, 1.0))
    )
    pop_mean, pop_scale = pltpu.roll(pop_mean, ACTIONS, 1), pltpu.roll(pop_scale, ACTIONS, 1)
    pop_scale = jnp.where(lanes((1, 128)) < ACTIONS, 1.0, pop_scale)
    mean, scale = popart_update(counts, totals, squares, pop_mean, pop_scale)
    is_value = lanes((1, 128)) >= ACTIONS
    ratio = jnp.where(is_value, pop_scale / scale, 1.0)
    new_bias = jnp.where(is_value, (pop_scale * bias + pop_mean - mean) / scale, bias)
    new_head[pl.ds(0, 75), :] = (head[...].astype(F32) * as_column(ratio)[0:75, :]).astype(BF16)
    new_head[pl.ds(75, 53), :] = jnp.zeros((53, 256), BF16)
    stats[...] = jnp.concatenate([mean, scale, new_bias, jnp.zeros((5, 128), F32)], axis=0)

    scatter.finish_far()
    scatter.finish_across()
    scatter.finish_near()
    first_env = me * 2
    columns = [
        step_columns(ref, first_env) for ref in (actions, rewards, ends, behaviour)
    ]
    columns[2] = DISCOUNT * (1.0 - columns[2])
    env = [
        jnp.sum(jnp.where(lanes((1, 32)) == first_env + e, tasks[...].astype(F32), 0.0), axis=1, keepdims=True)
        for e in (0, 1)
    ]
    game = jnp.where(sublanes((32, 128)) < 16, env[0], env[1])
    own_value = lanes((32, 128)) == game.astype(jnp.int32) + ACTIONS
    own_rows = pl.ds(pl.multiple_of(me * 32, 32), 32)

    def store(half, value):
        residual[:, half_cols(half)] = (
            value + tokens[own_rows, half_cols(half)].astype(F32)
        )

    scatter.finish(store)
    for m in range(2):
        v = residual[pl.ds(m * 16, 16), :]
        inverse = lax.rsqrt(jnp.mean(v * v, axis=1, keepdims=True) + NORM_EPS)
        normed[pl.ds(pl.multiple_of(me * 32 + m * 16, 16), 16), :] = (
            v * inverse * gain_all[...]
        ).astype(BF16)
    spread = Gather(place, wires, row_view(normed), gather_b)
    spread.open()
    for_hidden.relay(0)
    for_hidden.relay(1)
    heads = AllPairs(wires, "tp", 16, head_land)

    def out_slab(dz):
        start = plus(place.z, dz, 4) * 128
        rows = pl.ds(pl.multiple_of(start, 128), 128)
        v = dot(normed[rows, :], w_out_v[...])
        pre_out[rows, :] = v
        hidden_out[rows, :] = (v * sigmoid(v)).astype(BF16)
        head_part[rows, :] = dot(hidden_out[rows, :], new_head[...], ((1,), (1,))).astype(BF16)

    spread.middle()
    get_out.wait()
    spread.wait_twin(spread.OWN, spread.ACROSS)
    out_slab(0)
    spread.late()
    spread.wait_twin(spread.FROM_UP, spread.UP_ACROSS)
    out_slab(1)
    spread.last()
    spread.wait_twin(spread.FROM_DOWN, spread.DOWN_ACROSS)
    out_slab(3)
    spread.wait_twin(spread.FAR, spread.FAR_ACROSS)
    out_slab(2)

    def frames_of(ref):
        return lambda device: ref.at[pl.ds(pl.multiple_of(device * 32, 32), 32), :]

    for hop in range(1, 16):
        heads.post(hop, frames_of(head_part))
    for dy in (1, 2, 3):
        for_tokens.wait(dy)
        share = far_tokens.at[dy - 1, core_rows, :]
        wires.send(share, share, token_slot + dy - 1, place.partner)
    for_hidden.end()
    for b in range(4):
        hidden_t[:, b * 512 : b * 512 + 512] = (
            hidden_ring[b * 4 : b * 4 + 4].reshape(512, 256).T
        )
    outputs = head_part[own_rows, :].astype(F32)
    for hop in range(1, 16):
        heads.wait(hop)
        outputs = outputs + head_land[hop - 1].astype(F32)
    d_own = loss_gradient(outputs + new_bias, own_value, columns, mean, scale)
    d_heads[own_rows, :] = d_own.astype(BF16)
    d_slot = wires.claim(15)
    d_view = frames_of(d_heads)
    for hop in range(1, 16):
        wires.send(d_view(me), d_view(me), d_slot + hop - 1, plus(me, hop, 16))
    for hop in range(1, 16):
        wires.arrived(d_view(plus(me, 16 - hop, 16)), d_slot + hop - 1)
    wires.drain()

    def pre_gradient(m, carry):
        r = pl.ds(pl.multiple_of(m * 128, 128), 128)
        d_hidden = dot(d_heads[r, :], new_head[...])
        d_pre_out[r, :] = (d_hidden * slope(pre_out[r, :])).astype(BF16)
        return carry

    lax.fori_loop(0, 4, pre_gradient, 0)
    for_out = TaskSum(task, wires, slab_rows(512), whole_out, land_out, x_out, sum_out)
    for_mix = TaskSum(task, wires, slab_cols, whole_mix, None, x_mix, sum_mix)
    for_in = TaskSum(task, wires, slab_rows(528), whole_in, None, x_in, sum_in)

    def tall_product(left, right, whole, height, dy):
        k = plus(task.y, dy, 4)

        def tile(n, carry):
            feature = pl.multiple_of(k * 1024 + n * 256, 256)
            at = pl.multiple_of((k * 2 + n // 2) * height + lax.rem(n, 2) * 256, 16)
            value = dot(left[pl.ds(0, 512), pl.ds(feature, 256)], right[...], ((0,), (0,)))
            whole[pl.ds(at, 256), :] = value.astype(BF16)
            return carry

        lax.fori_loop(0, 4, tile, 0)

    def mix_product(part):
        def tile(n, carry):
            at = pl.multiple_of(part * 512 + n * 256, 256)
            whole_mix[:, pl.ds(at, 256)] = dot(
                hidden_t[...], residual_ring[:, pl.ds(at, 256)]
            ).astype(BF16)
            return carry

        lax.fori_loop(0, 2, tile, 0)

    def in_product(part):
        def tile(n, carry):
            at = pl.multiple_of(part * 512 + n * 256, 256)
            here = pl.ds(pl.multiple_of(task.y * 1024 + at, 256), 256)
            value = dot(tokens[pl.ds(0, 512), here], d_pre_in[task.y], ((0,), (0,)))
            for dy in (1, 2, 3):
                value = value + dot(
                    far_tokens[dy - 1, :, pl.ds(at, 256)],
                    d_pre_in[plus(task.y, dy, 4)],
                    ((0,), (0,)),
                )
            whole_in[pl.ds(pl.multiple_of(part * 528 + n * 256, 16), 256), :] = value.astype(BF16)
            return carry

        lax.fori_loop(0, 2, tile, 0)

    def out_product(dy):
        tall_product(normed, d_pre_out, whole_out, 512, dy)

    def out_first():
        out_product(2)
        for_out.far()

    scatter = Scatter(place, wires, partial, twin_part_b, landing_b, scatter_slots)
    scatter.open(lambda half: wide_product(d_pre_out, w_out_v, partial, half, True), out_first)
    out_product(1)
    out_product(3)
    for_out.near()
    scatter.finish_far()
    scatter.finish_across()
    out_product(0)
    for_out.relay()
    scatter.finish_near()

    def store(half, value):
        d_normed[:, half_cols(half)] = value

    scatter.finish(store)
    gain_rows = jnp.zeros((8, 4096), F32)
    for m in range(2):
        r = pl.ds(m * 16, 16)
        v = residual[r, :]
        inverse = lax.rsqrt(jnp.mean(v * v, axis=1, keepdims=True) + NORM_EPS)
        d = d_normed[r, :]
        scaled = d * gain_all[...]
        inner = jnp.sum(scaled * v, axis=1, keepdims=True)
        step = inverse * scaled - v * (inverse * inverse * inverse * inner * (1.0 / 4096))
        arrived[pl.ds(pl.multiple_of(me * 32 + m * 16, 16), 16), :] = step.astype(BF16)
        d_normed[r, :] = d * v * inverse
    gather = Gather(place, wires, row_view(arrived), gather_a)
    gather.open()
    ring_rows = lambda y: pl.ds(pl.multiple_of(me * 128 + y * 32, 32), 32)
    quarter = lambda y: pl.ds(pl.multiple_of(y * 1024, 1024), 1024)
    own32 = pl.ds(pl.multiple_of(me * 32, 32), 32)
    residual_ring[ring_rows(task.y), :] = arrived[own32, quarter(task.y)]
    for_residual = RingExchange(
        task,
        wires,
        lambda y: arrived.at[own32, quarter(y)],
        lambda dy: residual_ring.at[ring_rows(plus(task.y, dy, 4)), :],
    )
    for dy in (2, 1, 3):
        y = plus(task.y, dy, 4)
        wires.send(
            arrived.at[own32, quarter(y)],
            residual_ring.at[ring_rows(task.y), :],
            for_residual.first + 3 - dy,
            task.xh * 4 + y,
            "task",
        )
    for m in range(4):
        gain_rows = gain_rows + d_normed[pl.ds(m * 8, 8), :]
    for n in range(16):
        gain_parts[n] = gain_rows[:, n * 256 : n * 256 + 256]
    gains = AllPairs(wires, "tp", 16, gain_land)
    for hop in range(1, 16):
        gains.post(hop, lambda peer: gain_parts.at[peer])

    def hidden_slab(dz):
        rows = pl.ds(pl.multiple_of(plus(place.z, dz, 4) * 128, 128), 128)
        d = dot(arrived[rows, :], w_mix_v[...], ((1,), (1,)))
        d_pre_in[task.y, rows, :] = (d * slope(pre_in[rows, :])).astype(BF16)

    slabs = (0, 1, 3, 2)
    for_slope = RingGather(
        task,
        wires,
        lambda y, piece: d_pre_in.at[
            y, pl.ds(pl.multiple_of(plus(place.z, slabs[piece], 4) * 128, 128), 128), :
        ],
        4,
    )
    for_out.fold()
    gather.middle()
    for_out.finish()
    gather.wait_twin(gather.OWN, gather.ACROSS)
    hidden_slab(0)
    for_slope.open(0)
    gather.late()
    for dy in (1, 3, 2):
        for_residual.wait(dy)
    ring = Gather(
        place,
        wires,
        lambda block, half: residual_ring.at[
            pl.ds(pl.multiple_of(block * 128, 128), 128), pl.ds(half * 512, 512)
        ],
        gather_b,
    )
    ring.open()
    gather.wait_twin(gather.FROM_UP, gather.UP_ACROSS)
    hidden_slab(1)
    for_slope.open(1)
    gather.last()
    gather.wait_twin(gather.FROM_DOWN, gather.DOWN_ACROSS)
    hidden_slab(3)
    for_slope.open(2)
    for_slope.relay(0)
    gather.wait_twin(gather.FAR, gather.FAR_ACROSS)
    hidden_slab(2)
    for_slope.open(3)
    small = dot(d_heads[...], hidden_out[...], ((0,), (0,)))
    bias = jnp.sum(d_heads[...].astype(F32), axis=0, keepdims=True)
    gain_total = jnp.sum(gain_parts[me], axis=0, keepdims=True)
    for hop in range(1, 16):
        gains.wait(hop)
        gain_total = gain_total + jnp.sum(gain_land[hop - 1], axis=0, keepdims=True)
    row = sublanes((128, 256))
    bias = jnp.concatenate([bias, jnp.zeros((1, 128), F32)], axis=1)
    small_own[...] = jnp.where(
        row == 80, bias, jnp.where(row == 88, gain_total, small)
    ).astype(BF16)
    small_rows = lambda y: small_own.at[pl.ds(pl.multiple_of(y * 32, 32), 32), :]
    for_small = RingExchange(task, wires, small_rows, lambda dy: small_land.at[dy - 1])
    for_small.open()
    for_slope.relay(1)
    for_slope.relay(2)
    ring.middle_near()
    for_slope.relay(3)
    for_out.spread()
    ring.middle_across()
    for dy in (1, 2, 3):
        wires.arrived(far_tokens.at[dy - 1, twin_rows, :], token_slot + dy - 1)
    extra = small_rows(task.y)[...].astype(F32)
    for dy in (1, 3, 2):
        for_small.wait(dy)
        extra = extra + small_land[dy - 1].astype(F32)
    for part in (0, 1):
        whole_in[pl.ds(part * 528 + 512, 16), :] = extra[part * 16 : part * 16 + 16, :].astype(BF16)
    for_slope.end()
    in_product(1 - task.xh)
    for_in.fold()
    ring.middle_far()
    in_product(task.xh)
    ring.late()
    ring.last()
    ring.wait_twin(*range(8))
    mix_product(1 - task.xh)
    for_mix.fold()
    mix_product(task.xh)
    for_in.finish()
    for_out.spread_far()
    for_mix.finish()
    for_in.spread()
    for_out.end()
    keep_out = load(sum_out, sum_out_hbm, local_sems, 4)
    for_mix.spread()
    for_in.spread_far()
    for_in.end()
    keep_in = load(sum_in, sum_in_hbm, local_sems, 6)
    for_mix.spread_far()
    for_mix.end()
    keep_mix = load(sum_mix, sum_mix_hbm, local_sems, 5)
    wires.drain()
    for keep in (keep_out, keep_mix, keep_in):
        keep.wait()


def finish_kernel(
    sum_out, sum_mix, sum_in, new_head, stats,
    grad_in, grad_mix, grad_out, gain, head, bias, head_now, bias_now, mean, scale,
    out_b, mix_b, in_b, small_b, out_f, mix_f, in_f, sems,
):
    gets = []
    for n in range(8):
        r = pl.ds(n * 512, 512)
        gets.append(load(sum_in.at[pl.ds(n * 528, 512), :], in_b.at[r, :], sems, n))
    for n in range(8):
        gets.append(
            load(sum_in.at[pl.ds(n * 528 + 512, 16), :], small_b.at[pl.ds(n * 16, 16), :], sems, 8 + n)
        )
    for n in range(4):
        r = pl.ds(n * 64, 64)
        gets.append(load(sum_mix.at[r, :], mix_b.at[r, :], sems, 16 + n))
    for n in range(8):
        r = pl.ds(n * 512, 512)
        gets.append(load(sum_out.at[r, :], out_b.at[r, :], sems, 20 + n))
    puts = []
    for n in range(8):
        r = pl.ds(n * 512, 512)
        gets[n].wait()
        in_f[r, :] = in_b[r, :].astype(F32)
        puts.append(load(in_f.at[r, :], grad_in.at[r, :], sems, 28 + n))
    for n in range(4):
        r = pl.ds(n * 64, 64)
        gets[16 + n].wait()
        mix_f[r, :] = mix_b[r, :].astype(F32)
        puts.append(load(mix_f.at[r, :], grad_mix.at[r, :], sems, 36 + n))
    for n in range(8):
        r = pl.ds(n * 512, 512)
        gets[20 + n].wait()
        out_f[r, :] = out_b[r, :].astype(F32)
        puts.append(load(out_f.at[r, :], grad_out.at[r, :], sems, 40 + n))
    for n in range(8):
        gets[8 + n].wait()
    small = small_b[...].astype(F32)
    head[...] = small[0:75, :]
    bias[...] = small[80:81, 0:75]
    gain[...] = small[88:89, :]
    head_now[...] = new_head[0:75, :]
    values = pltpu.roll(stats[...], 128 - ACTIONS, 1)
    mean[...] = values[0:1, 0:TASKS]
    scale[...] = values[1:2, 0:TASKS]
    bias_now[...] = stats[2:3, 0:75]
    for put in puts:
        put.wait()


def hbm():
    return pl.BlockSpec(memory_space=pltpu.HBM)


def vmem():
    return pl.BlockSpec(memory_space=pltpu.VMEM)


def step_call(*arguments):
    v, h = vmem(), hbm()
    scratch = [
        ((528, 4096), BF16), ((4096, 256), BF16), ((256, 4096), BF16), ((4096, 256), BF16),
        ((512, 256), F32), ((512, 256), BF16), ((32, 4096), F32), ((1, 4096), F32),
        ((512, 4096), BF16),
        ((512, 256), F32), ((512, 256), BF16), ((512, 128), BF16), ((15, 32, 128), BF16),
        ((512, 128), BF16), ((8, 128), F32), ((7, 8, 128), F32),
        ((512, 256), BF16), ((4, 512, 256), BF16), ((256, 2048), BF16), ((32, 4096), F32),
        ((16, 4, 32, 256), BF16), ((3, 512, 1024), BF16), ((2048, 1024), BF16),
        ((128, 256), BF16), ((3, 32, 256), BF16),
        ((512, 4096), BF16), ((8, 32, 4096), BF16), ((7, 32, 4096), BF16),
        ((8, 32, 4096), BF16), ((7, 32, 4096), BF16), ((512, 4096), BF16),
        ((16, 8, 256), F32), ((15, 8, 256), F32),
        ((4096, 256), BF16), ((256, 1024), BF16), ((1056, 256), BF16),
        ((3, 2, 512, 256), BF16),
        ((512, 256), BF16), ((256, 512), BF16), ((528, 256), BF16),
        ((4096, 256), BF16), ((256, 4096), BF16), ((4224, 256), BF16),
    ]
    return pl.pallas_call(
        step_kernel,
        out_shape=[
            jax.ShapeDtypeStruct((4096, 256), BF16),
            jax.ShapeDtypeStruct((256, 4096), BF16),
            jax.ShapeDtypeStruct((4224, 256), BF16),
            jax.ShapeDtypeStruct((128, 256), BF16),
            jax.ShapeDtypeStruct((8, 128), F32),
        ],
        in_specs=[h, v, h, h, h, v, v, v, v, v, v, v, v, v],
        out_specs=[h, h, h, v, v],
        scratch_shapes=[pltpu.VMEM(*s) for s in scratch]
        + [pltpu.SemaphoreType.DMA((SENDS,)), pltpu.SemaphoreType.DMA((RECEIVES,)), pltpu.SemaphoreType.DMA((7,))],
        compiler_params=pltpu.CompilerParams(
            collective_id=0, has_side_effects=True, vmem_limit_bytes=63 * 2**20
        ),
        name="step",
    )(*arguments)


def finish_call(*arguments):
    v, h = vmem(), hbm()
    return pl.pallas_call(
        finish_kernel,
        out_shape=[
            jax.ShapeDtypeStruct((4096, 256), F32),
            jax.ShapeDtypeStruct((256, 4096), F32),
            jax.ShapeDtypeStruct((4096, 256), F32),
            jax.ShapeDtypeStruct((1, 256), F32),
            jax.ShapeDtypeStruct((75, 256), F32),
            jax.ShapeDtypeStruct((1, 75), F32),
            jax.ShapeDtypeStruct((75, 256), BF16),
            jax.ShapeDtypeStruct((1, 75), F32),
            jax.ShapeDtypeStruct((1, TASKS), F32),
            jax.ShapeDtypeStruct((1, TASKS), F32),
        ],
        in_specs=[h, h, h, v, v],
        out_specs=[h, h, h, v, v, v, v, v, v, v],
        scratch_shapes=[
            pltpu.VMEM((4096, 256), BF16),
            pltpu.VMEM((256, 4096), BF16),
            pltpu.VMEM((4096, 256), BF16),
            pltpu.VMEM((128, 256), BF16),
            pltpu.VMEM((4096, 256), F32),
            pltpu.VMEM((256, 4096), F32),
            pltpu.VMEM((4096, 256), F32),
            pltpu.SemaphoreType.DMA((48,)),
        ],
        compiler_params=pltpu.CompilerParams(vmem_limit_bytes=63 * 2**20),
        name="finish",
    )(*arguments)


def on_device(
    observations, gain, w_in, w_mix, w_out, w_head, head_bias, pop_mean, pop_scale,
    task_indices, actions, rewards, episode_ends, behaviour_log_prob,
):
    sums = step_call(
        observations.reshape(512, 256),
        gain.reshape(1, 256),
        w_in,
        w_mix,
        w_out,
        w_head.T,
        head_bias.reshape(1, ACTIONS + TASKS),
        pop_mean.reshape(1, TASKS),
        pop_scale.reshape(1, TASKS),
        task_indices.reshape(1, 32),
        actions.T,
        rewards.T,
        episode_ends.T,
        behaviour_log_prob.T,
    )
    (
        grad_in, grad_mix, grad_out, grad_gain, grad_head, grad_bias,
        new_head, new_bias, mean, scale,
    ) = finish_call(*sums)
    return (
        grad_in,
        grad_mix,
        grad_out,
        grad_gain.reshape(256),
        grad_head.T,
        grad_bias.reshape(75),
        new_head.T,
        new_bias.reshape(75),
        mean.reshape(TASKS),
        scale.reshape(TASKS),
    )


def solution(mesh):
    in_specs = (
        P("task", None, "tp"),
        P("tp"),
        P(None, "tp"),
        P("tp", None),
        P(None, "tp"),
        P("tp", None),
        P(),
        P(),
        P(),
        P("task"),
        P("task", None),
        P("task", None),
        P("task", None),
        P("task", None),
    )
    out_specs = (
        P(None, "tp"),
        P("tp", None),
        P(None, "tp"),
        P("tp"),
        P("tp", None),
        P(),
        P("tp", None),
        P(),
        P(),
        P(),
    )
    return jax.shard_map(
        on_device, mesh=mesh, in_specs=in_specs, out_specs=out_specs, check_vma=False
    )
```

```python
import jax
import jax.numpy as jnp
from jax import lax
from jax.experimental import pallas as pl
from jax.experimental.pallas import tpu as pltpu
from jax.sharding import PartitionSpec as P

ACTIONS = 18
TASKS = 57
DISCOUNT = 0.99
BASELINE_COST = 0.5
ENTROPY_COST = 0.01
POPART_PRIOR = 64.0
NORM_EPS = 1e-06
LOSS_WEIGHT = 256**-0.5
SENDS = 172
RECEIVES = 244


MESH = pl.DeviceIdType.MESH
F32 = jnp.float32
BF16 = jnp.bfloat16
HALVES = (0, 1)


def plus(a, b, n):
    return lax.rem(a + b, n)


class Place:
    def __init__(self):
        self.me = lax.axis_index("tp")
        self.z = self.me // 4
        self.x = lax.rem(self.me // 2, 2)
        self.c = lax.rem(self.me, 2)
        self.across = self.at(0, 1)
        self.up = self.at(1, 0)
        self.down = self.at(3, 0)
        self.partner = self.at(0, 0, 1)

    def at(self, dz, dx, dc=0):
        return (plus(self.z, dz, 4) * 2 + plus(self.x, dx, 2)) * 2 + plus(self.c, dc, 2)


class Wires:
    def __init__(self, send_sems, recv_sems):
        self.send_sems = send_sems
        self.recv_sems = recv_sems
        self.sent = []
        self.slots = 0

    def claim(self, count):
        first = self.slots
        self.slots += count
        return first

    def send(self, src, dst, slot, peer, axis="tp"):
        copy = pltpu.make_async_remote_copy(
            src_ref=src,
            dst_ref=dst,
            send_sem=self.send_sems.at[len(self.sent)],
            recv_sem=self.recv_sems.at[slot],
            device_id={axis: peer},
            device_id_type=MESH,
        )
        copy.start()
        self.sent.append(copy)

    def arrived(self, dst, slot, axis="tp"):
        pltpu.make_async_remote_copy(
            src_ref=dst,
            dst_ref=dst,
            send_sem=self.send_sems.at[0],
            recv_sem=self.recv_sems.at[slot],
            device_id={axis: lax.axis_index(axis)},
            device_id_type=MESH,
        ).wait_recv()

    def drain(self):
        for copy in self.sent:
            copy.wait_send()
        self.sent = []


class Gather:
    ACROSS, FROM_DOWN, FROM_UP, DOWN_ACROSS, UP_ACROSS, FAR, FAR_ACROSS, OWN = range(8)

    def __init__(self, place, wires, view, first, far_across_on_z=False):
        self.place = place
        self.wires = wires
        self.view = view
        self.first = first
        self.on_z = far_across_on_z
        p = place
        self.block = {
            self.ACROSS: p.at(0, 1),
            self.FROM_DOWN: p.at(3, 0),
            self.FROM_UP: p.at(1, 0),
            self.DOWN_ACROSS: p.at(3, 1),
            self.UP_ACROSS: p.at(1, 1),
            self.FAR: p.at(2, 0),
            self.FAR_ACROSS: p.at(2, 1),
            self.OWN: p.me,
        }
        self.twin = {k: plus(b, 0, 16) + 1 - 2 * p.c for k, b in self.block.items()}

    def slot(self, kind, half):
        return self.first + kind * 2 + half

    def twin_slot(self, kind, half):
        return self.first + 14 + kind * 2 + half

    def pass_on(self, kind, half, peer, kind_there):
        v = self.view(self.block[kind], half)
        self.wires.send(v, v, self.slot(kind_there, half), peer)

    def to_twin(self, kind, half):
        v = self.view(self.block[kind], half)
        self.wires.send(v, v, self.twin_slot(kind, half), self.place.partner)

    def wait(self, kind, half):
        self.wires.arrived(self.view(self.block[kind], half), self.slot(kind, half))

    def wait_twin(self, *kinds):
        for kind in kinds:
            for half in HALVES:
                self.wires.arrived(
                    self.view(self.twin[kind], half), self.twin_slot(kind, half)
                )

    def open(self):
        p = self.place
        for half in HALVES:
            self.pass_on(self.OWN, half, p.up, self.FROM_DOWN)
            self.pass_on(self.OWN, half, p.down, self.FROM_UP)
            self.pass_on(self.OWN, half, p.across, self.ACROSS)
            self.to_twin(self.OWN, half)

    def middle(self):
        self.middle_near()
        self.middle_across()
        self.middle_far()

    def middle_near(self):
        p = self.place
        self.wait(self.FROM_DOWN, 0)
        self.pass_on(self.FROM_DOWN, 0, p.up, self.FAR)
        self.to_twin(self.FROM_DOWN, 0)
        self.wait(self.FROM_UP, 0)
        self.to_twin(self.FROM_UP, 0)
        self.wait(self.ACROSS, 0)
        self.pass_on(self.ACROSS, 0, p.down, self.UP_ACROSS)
        self.wait(self.FROM_UP, 1)
        self.pass_on(self.FROM_UP, 1, p.down, self.FAR)
        self.pass_on(self.ACROSS, 0, p.up, self.DOWN_ACROSS)
        self.to_twin(self.ACROSS, 0)
        self.to_twin(self.FROM_UP, 1)

    def middle_across(self):
        p = self.place
        self.wait(self.FROM_DOWN, 1)
        self.to_twin(self.FROM_DOWN, 1)
        self.wait(self.ACROSS, 1)
        self.pass_on(self.ACROSS, 1, p.up, self.DOWN_ACROSS)
        self.pass_on(self.ACROSS, 1, p.down, self.UP_ACROSS)
        self.to_twin(self.ACROSS, 1)

    def middle_far(self):
        for half in HALVES:
            self.wait(self.FAR, half)
            if not self.on_z:
                self.pass_on(self.FAR, half, self.place.across, self.FAR_ACROSS)
            self.to_twin(self.FAR, half)

    def late(self):
        for half in HALVES:
            for kind in (self.DOWN_ACROSS, self.UP_ACROSS):
                self.wait(kind, half)
                if self.on_z and (kind == self.UP_ACROSS) == (half == 1):
                    peer = self.place.down if half else self.place.up
                    self.pass_on(kind, half, peer, self.FAR_ACROSS)
                self.to_twin(kind, half)

    def last(self):
        for half in HALVES:
            self.wait(self.FAR_ACROSS, half)
            self.to_twin(self.FAR_ACROSS, half)


def half_cols(half):
    return pl.ds(half * 2048, 2048)


class Scatter:
    G, D, E, F, A, B, C = range(7)
    ORDER = ((2, 1), (1, 1), (3, 1), (1, 0), (3, 0), (2, 0), (0, 1), (0, 0))

    def __init__(self, place, wires, partial, twin_part, landing, first):
        self.place = place
        self.wires = wires
        self.partial = partial
        self.twin_part = twin_part
        self.landing = landing
        self.first = first

    def rows(self, where, dc=0):
        return pl.ds(pl.multiple_of(self.place.at(*where, dc) * 32, 32), 32)

    def mine(self, where, half):
        return self.partial.at[self.rows(where), half_cols(half)]

    def twins(self, where, half):
        return self.twin_part.at[self.ORDER.index(where), :, half_cols(half)]

    def land(self, kind, half):
        return self.landing.at[kind, :, half_cols(half)]

    def total(self, where, half, kinds=(), waited=()):
        slot = self.first + 14 + self.ORDER.index(where) * 2 + half
        if (where, half) not in self.seen:
            self.wires.arrived(self.twins(where, half), slot)
            self.seen.add((where, half))
        for kind in kinds:
            self.wires.arrived(self.land(kind, half), self.first + kind * 2 + half)
        value = self.mine(where, half)[...].astype(F32) + self.twins(where, half)[...].astype(F32)
        for kind in kinds:
            value = value + self.land(kind, half)[...].astype(F32)
        return value

    def forward(self, where, half, kinds, peer, kind_there):
        self.mine(where, half)[...] = self.total(where, half, kinds).astype(BF16)
        self.wires.send(
            self.mine(where, half),
            self.land(kind_there, half),
            self.first + kind_there * 2 + half,
            peer,
        )

    def open(self, produce, between=None):
        self.seen = set()
        p = self.place
        for half in HALVES:
            produce(half)
            for where in self.ORDER:
                self.wires.send(
                    self.partial.at[self.rows(where, 1), half_cols(half)],
                    self.twins(where, half),
                    self.first + 14 + self.ORDER.index(where) * 2 + half,
                    p.partner,
                )
            if half == 1 and between is not None:
                between()
            self.forward((2, 1), half, (), p.across, self.G)
            self.forward((1, 1), half, (), p.up, self.D)
            self.forward((3, 1), half, (), p.down, self.E)
        self.forward((1, 0), 1, (), p.up, self.B)
        self.forward((3, 0), 0, (), p.down, self.C)

    def finish_far(self):
        p = self.place
        self.forward((2, 0), 0, (self.G,), p.up, self.F)
        self.forward((2, 0), 1, (self.G,), p.down, self.F)

    def finish_across(self):
        for half in HALVES:
            self.forward((0, 1), half, (self.D, self.E), self.place.across, self.A)

    def finish_near(self):
        p = self.place
        self.forward((1, 0), 0, (self.F,), p.up, self.B)
        self.forward((3, 0), 1, (self.F,), p.down, self.C)

    def finish(self, store):
        for half in HALVES:
            store(half, self.total((0, 0), half, (self.A, self.B, self.C)))


def sigmoid(v):
    return 1.0 / (1.0 + jnp.exp(-v))


def dot(a, b, contract=((1,), (0,))):
    return lax.dot_general(a, b, (contract, ((), ())), preferred_element_type=F32)


def load(src, dst, sems, at):
    copy = pltpu.make_async_copy(src, dst, sems.at[at])
    copy.start()
    return copy


def wide_product(left, right, partial, half, transposed):
    def tile(n, carry):
        at = pl.multiple_of(half * 2048 + n * 256, 256)
        if transposed:
            value = dot(left[...], right[pl.ds(at, 256), :], ((1,), (1,)))
        else:
            value = dot(left[...], right[:, pl.ds(at, 256)])
        partial[:, pl.ds(at, 256)] = value.astype(BF16)
        return carry

    lax.fori_loop(0, 8, tile, 0)


def row_view(ref):
    return lambda block, half: ref.at[
        pl.ds(pl.multiple_of(block * 32, 32), 32), half_cols(half)
    ]


class TaskPlace:
    def __init__(self):
        task = lax.axis_index("task")
        self.xh = task // 4
        self.y = lax.rem(task, 4)
        self.up = self.xh * 4 + plus(self.y, 1, 4)
        self.down = self.xh * 4 + plus(self.y, 3, 4)
        self.across = (1 - self.xh) * 4 + self.y


class TaskSum:
    F, B, C = range(3)
    OWN, FROM_DOWN, FROM_UP, DOWN_ACROSS, UP_ACROSS, FAR, FAR_ACROSS = range(7)

    def __init__(self, place, wires, view, whole, land, land_x, result):
        self.place = place
        self.wires = wires
        self.view = view
        self.whole = whole
        self.land = land
        self.land_x = land_x
        self.result = result
        self.first = wires.claim(14)

    def slab(self, ref, dy, part):
        return self.view(ref, plus(self.place.y, dy, 4) * 2 + part)

    def post(self, src, dst, slot, peer):
        self.wires.send(src, dst, self.first + slot, peer, "task")

    def wait(self, dst, slot):
        self.wires.arrived(dst, self.first + slot, "task")

    def far(self):
        p = self.place
        self.post(self.slab(self.whole, 2, 0), self.land.at[self.F, 0], 0, p.up)
        self.post(self.slab(self.whole, 2, 1), self.land.at[self.F, 1], 1, p.down)

    def near(self):
        p = self.place
        self.post(self.slab(self.whole, 1, 1), self.land.at[self.B, 1], 3, p.up)
        self.post(self.slab(self.whole, 3, 0), self.land.at[self.C, 0], 4, p.down)

    def relay(self):
        p = self.place
        for dy, part, kind, slot, peer in ((1, 0, self.B, 2, p.up), (3, 1, self.C, 5, p.down)):
            self.wait(self.land.at[self.F, part], part)
            own = self.slab(self.whole, dy, part)
            total = own[...].astype(F32) + self.land[self.F, part].astype(F32)
            own[...] = total.astype(BF16)
            self.post(own, self.land.at[kind, part], slot, peer)

    def local(self, part):
        if self.land is None:
            return self.view(self.whole, part)[...].astype(F32)
        return (
            self.slab(self.whole, 0, part)[...].astype(F32)
            + self.land[self.B, part].astype(F32)
            + self.land[self.C, part].astype(F32)
        )

    def fold(self):
        if self.land is None:
            away = self.view(self.whole, 1 - self.place.xh)
            self.post(away, self.land_x, 6, self.place.across)
            return
        for kind, part, slot in ((self.B, 1, 3), (self.C, 0, 4), (self.B, 0, 2), (self.C, 1, 5)):
            self.wait(self.land.at[kind, part], slot)
        other = 1 - self.place.xh
        away = self.slab(self.whole, 0, other)
        away[...] = self.local(other).astype(BF16)
        self.post(away, self.land_x, 6, self.place.across)

    def pass_on(self, kind, peer, kind_there):
        v = self.held(kind)
        self.post(v, v, 6 + kind_there, peer)

    def held(self, kind):
        dy, across = {
            self.OWN: (0, 0),
            self.FROM_DOWN: (3, 0),
            self.FROM_UP: (1, 0),
            self.DOWN_ACROSS: (3, 1),
            self.UP_ACROSS: (1, 1),
            self.FAR: (2, 0),
            self.FAR_ACROSS: (2, 1),
        }[kind]
        xh = self.place.xh
        return self.slab(self.result, dy, 1 - xh if across else xh)

    def across_held(self):
        return self.slab(self.result, 0, 1 - self.place.xh)

    def finish(self):
        p = self.place
        self.wait(self.land_x, 6)
        own = self.held(self.OWN)
        own[...] = (self.local(p.xh) + self.land_x[...].astype(F32)).astype(BF16)
        self.post(own, own, 13, p.across)
        self.pass_on(self.OWN, p.up, self.FROM_DOWN)
        self.pass_on(self.OWN, p.down, self.FROM_UP)

    def get(self, kind):
        self.wait(self.held(kind), 6 + kind)

    def spread(self):
        p = self.place
        self.get(self.FROM_DOWN)
        self.pass_on(self.FROM_DOWN, p.up, self.FAR)
        self.get(self.FROM_UP)
        v = self.across_held()
        self.wait(v, 13)
        self.post(v, v, 6 + self.DOWN_ACROSS, p.up)
        self.post(v, v, 6 + self.UP_ACROSS, p.down)

    def spread_far(self):
        self.get(self.UP_ACROSS)
        self.pass_on(self.UP_ACROSS, self.place.down, self.FAR_ACROSS)
        self.get(self.DOWN_ACROSS)

    def end(self):
        self.get(self.FAR)
        self.get(self.FAR_ACROSS)


class RingGather:
    FROM_DOWN, FROM_UP, FAR = range(3)

    def __init__(self, place, wires, view, pieces):
        self.place = place
        self.wires = wires
        self.view = view
        self.pieces = pieces
        self.first = wires.claim(3 * pieces)

    def block(self, kind, piece):
        dy = {self.FROM_DOWN: 3, self.FROM_UP: 1, self.FAR: 2}[kind]
        return self.view(plus(self.place.y, dy, 4), piece)

    def post(self, v, kind, piece, peer):
        self.wires.send(v, v, self.first + kind * self.pieces + piece, peer, "task")

    def wait(self, kind, piece):
        self.wires.arrived(
            self.block(kind, piece), self.first + kind * self.pieces + piece, "task"
        )

    def open(self, piece):
        p = self.place
        v = self.view(p.y, piece)
        self.post(v, self.FROM_DOWN, piece, p.up)
        self.post(v, self.FROM_UP, piece, p.down)

    def relay(self, piece):
        kind = self.FROM_UP if piece % 2 else self.FROM_DOWN
        self.wait(kind, piece)
        peer = self.place.down if piece % 2 else self.place.up
        self.post(self.block(kind, piece), self.FAR, piece, peer)

    def end(self):
        for piece in range(self.pieces):
            self.wait(self.FROM_DOWN if piece % 2 else self.FROM_UP, piece)
            self.wait(self.FAR, piece)


class RingExchange:
    def __init__(self, place, wires, source, land):
        self.place = place
        self.wires = wires
        self.source = source
        self.land = land
        self.first = wires.claim(3)

    def open(self):
        p = self.place
        for dy in (2, 1, 3):
            y = plus(p.y, dy, 4)
            self.wires.send(
                self.source(y), self.land(4 - dy), self.first + 3 - dy, p.xh * 4 + y, "task"
            )

    def wait(self, dy):
        self.wires.arrived(self.land(dy), self.first + dy - 1, "task")


def slope(v):
    s = sigmoid(v)
    return s * (1.0 + v * (1.0 - s))


def slab_rows(height):
    return lambda ref, n: ref.at[pl.ds(pl.multiple_of(n * height, 16), height), :]


def tall_piece(piece):
    size = 272 if piece else 256
    return lambda ref, n: ref.at[pl.ds(pl.multiple_of(n * 528 + piece * 256, 16), size), :]


def wide_piece(piece):
    return lambda ref, n: ref.at[:, pl.ds(pl.multiple_of(n * 512 + piece * 256, 256), 256)]


def popart_update(counts, totals, squares, pop_mean, pop_scale):
    mixing = counts / (counts + POPART_PRIOR)
    safe_counts = jnp.maximum(counts, 1.0)
    batch_mean = totals / safe_counts
    batch_square = squares / safe_counts
    updated_return_mean = (1.0 - mixing) * pop_mean + mixing * batch_mean
    mean_gap = batch_mean - pop_mean
    variance = (
        (1.0 - mixing) * pop_scale * pop_scale
        + mixing * (batch_square - batch_mean * batch_mean)
        + mixing * (1.0 - mixing) * mean_gap * mean_gap
    )
    return (updated_return_mean, jnp.sqrt(variance))


class AllPairs:
    def __init__(self, wires, axis, size, land):
        self.wires = wires
        self.axis = axis
        self.size = size
        self.here = lax.axis_index(axis)
        self.land = land
        self.first = wires.claim(size - 1)

    def post(self, peer_at, src):
        peer = plus(self.here, peer_at, self.size)
        self.wires.send(
            src(peer), self.land.at[peer_at - 1], self.first + peer_at - 1, peer, self.axis
        )

    def wait(self, peer_at):
        self.wires.arrived(self.land.at[peer_at - 1], self.first + peer_at - 1, self.axis)


def greet_everyone():
    barrier = pltpu.get_barrier_semaphore()
    for axis, size in (("tp", 16), ("task", 8)):
        here = lax.axis_index(axis)
        for hop in range(1, size):
            pl.semaphore_signal(
                barrier, inc=1, device_id={axis: plus(here, hop, size)}, device_id_type=MESH
            )
    pl.semaphore_wait(barrier, 22)


def lanes(shape):
    return lax.broadcasted_iota(jnp.int32, shape, 1)


def sublanes(shape):
    return lax.broadcasted_iota(jnp.int32, shape, 0)


def popart_rows(tasks, rewards, ends):
    factors = DISCOUNT * (1.0 - ends[...].astype(F32))
    gains = rewards[...]
    running = jnp.zeros((1, 32), F32)
    total = jnp.zeros((1, 32), F32)
    square = jnp.zeros((1, 32), F32)
    for t in range(14, -1, -1):
        running = gains[t : t + 1, :] + factors[t : t + 1, :] * running
        total = total + running
        square = square + running * running
    member = sublanes((128, 32)) == tasks[...] + ACTIONS
    diagonal = sublanes((128, 128)) == lanes((128, 128))
    rows = []
    for value in (jnp.full((1, 32), 15.0, F32), total, square):
        column = jnp.sum(jnp.where(member, value, 0.0), axis=1, keepdims=True)
        rows.append(jnp.sum(jnp.where(diagonal, column, 0.0), axis=0, keepdims=True))
    return jnp.concatenate([*rows, jnp.zeros((5, 128), F32)], axis=0)


def as_column(row):
    diagonal = sublanes((128, 128)) == lanes((128, 128))
    return jnp.sum(jnp.where(diagonal, row, 0.0), axis=1, keepdims=True)


def step_columns(ref, first_env):
    value = ref[...].astype(F32)
    value = jnp.concatenate([value, jnp.zeros((1, 32), F32)], axis=0)
    lane = lanes((16, 32))
    return jnp.concatenate(
        [
            jnp.sum(jnp.where(lane == first_env + e, value, 0.0), axis=1, keepdims=True)
            for e in (0, 1)
        ],
        axis=0,
    )


def loss_gradient(outputs, own, columns, mean, scale):
    action, reward, factor, behaviour = columns
    shape = (32, 128)
    lane = lanes(shape)
    frame = lax.rem(sublanes(shape), 16)
    live = frame < 15

    def later(value, by):
        return jnp.where(frame + by < 16, pltpu.roll(value, 32 - by, 0), 0.0)

    def over_lanes(mask, value):
        return jnp.broadcast_to(
            jnp.sum(jnp.where(mask, value, 0.0), axis=1, keepdims=True), shape
        )

    is_logit = lane < ACTIONS
    chosen = lane == action.astype(jnp.int32)
    log_total = jnp.log(over_lanes(is_logit, jnp.exp(jnp.where(is_logit, outputs, 0.0))))
    log_prob = jnp.where(is_logit, outputs - log_total, 0.0)
    log_policy = over_lanes(chosen, log_prob)
    env_mean = over_lanes(own, mean)
    env_scale = over_lanes(own, scale)
    norm_values = over_lanes(own, outputs)
    values = norm_values * env_scale + env_mean
    clipped = jnp.minimum(jnp.exp(log_policy - behaviour), 1.0)
    total = jnp.where(live, clipped * (reward + factor * later(values, 1) - values), 0.0)
    decay = jnp.where(live, factor * clipped, 0.0)
    for by in (1, 2, 4, 8):
        total = total + decay * later(total, by)
        decay = decay * later(decay, by)
    targets = values + total
    following = later(targets, 1)
    advantage = clipped * ((reward + factor * following - env_mean) / env_scale - norm_values)
    normed_targets = (targets - env_mean) / env_scale
    policy = jnp.where(is_logit, jnp.exp(log_prob), 0.0)
    entropy = -over_lanes(is_logit, policy * log_prob)
    d_logits = -advantage * (jnp.where(chosen, 1.0, 0.0) - policy) + ENTROPY_COST * policy * (
        log_prob + entropy
    )
    d_value = -BASELINE_COST * (normed_targets - norm_values)
    d = jnp.where(is_logit, d_logits, jnp.where(own, d_value, 0.0))
    return jnp.where(live, d * LOSS_WEIGHT, 0.0)


def step_kernel(
    own_tokens, gain, w_in, w_mix, w_out, head, head_bias, old_mean, old_scale, tasks, actions, rewards, ends, behaviour,
    sum_out_hbm, sum_mix_hbm, sum_in_hbm, new_head, stats,
    tokens, w_in_v, w_mix_v, w_out_v, pre_in, hidden_in, residual, gain_all, normed,
    pre_out, hidden_out, head_part, head_land, d_heads, stat_own, stat_land,
    d_pre_out, d_pre_in, hidden_t, d_normed,
    hidden_ring, far_tokens, residual_ring, small_own, small_land,
    partial, twin_part, landing, twin_part_b, landing_b, arrived, gain_parts, gain_land,
    whole_out, whole_mix, whole_in, land_out, x_out, x_mix, x_in,
    sum_out, sum_mix, sum_in,
    send_sems, recv_sems, local_sems,
):
    place = Place()
    task = TaskPlace()
    wires = Wires(send_sems, recv_sems)
    gather_a, gather_b, scatter_slots = wires.claim(30), wires.claim(30), wires.claim(30)
    me = place.me
    own_cols = pl.ds(pl.multiple_of(me * 256, 256), 256)
    first = load(own_tokens, tokens.at[pl.ds(0, 512), own_cols], local_sems, 0)
    g = gain[...]
    hi = g.astype(BF16).astype(F32)
    mid = (g - hi).astype(BF16).astype(F32)
    low = g - hi - mid
    row = sublanes((16, 256))
    rows = jnp.where(row == 0, hi, jnp.where(row == 1, mid, jnp.where(row == 2, low, 0.0)))
    tokens[pl.ds(512, 16), own_cols] = rows.astype(BF16)
    greet_everyone()
    first.wait()

    def token_view(block, half):
        rows = pl.ds(0, 256) if half == 0 else pl.ds(256, 272)
        return tokens.at[rows, pl.ds(pl.multiple_of(block * 256, 256), 256)]

    gather = Gather(place, wires, token_view, gather_a)
    gather.open()
    get_in = load(w_in, w_in_v, local_sems, 1)
    get_mix = load(w_mix, w_mix_v, local_sems, 2)
    get_out = load(w_out, w_out_v, local_sems, 3)

    stat_own[...] = popart_rows(tasks, rewards, ends)
    statistics = AllPairs(wires, "task", 8, stat_land)
    for hop in range(1, 8):
        statistics.post(hop, lambda peer: stat_own)
    gather.middle()

    def slab(dz, opening=False):
        at = pl.multiple_of(plus(place.z, dz, 4) * 1024, 1024)

        def tile(m, carry):
            r = pl.ds(pl.multiple_of(m * 128, 128), 128)
            value = dot(tokens[r, pl.ds(at, 1024)], w_in_v[pl.ds(at, 1024), :])
            pre_in[r, :] = value if opening else pre_in[r, :] + value
            return carry

        lax.fori_loop(0, 4, tile, 0)

    get_in.wait()
    gather.wait_twin(gather.OWN, gather.ACROSS)
    slab(0, True)
    gather.late()
    gather.wait_twin(gather.FROM_UP, gather.UP_ACROSS)
    slab(1)
    gather.last()
    gather.wait_twin(gather.FROM_DOWN, gather.DOWN_ACROSS)
    slab(3)
    gather.wait_twin(gather.FAR, gather.FAR_ACROSS)
    slab(2)

    def activate(m, carry):
        r = pl.ds(pl.multiple_of(m * 128, 128), 128)
        v = pre_in[r, :]
        hidden = (v * sigmoid(v)).astype(BF16)
        hidden_in[r, :] = hidden
        hidden_ring[pl.ds(m * 4, 4), task.y] = hidden.reshape(4, 32, 256)
        return carry

    lax.fori_loop(0, 4, activate, 0)
    get_mix.wait()
    scatter = Scatter(place, wires, partial, twin_part, landing, scatter_slots)
    scatter.open(lambda half: wide_product(hidden_in, w_mix_v, partial, half, False))

    for_hidden = RingGather(
        task, wires, lambda y, half: hidden_ring.at[pl.ds(half * 8, 8), y], 2
    )
    for_hidden.open(0)
    for_hidden.open(1)
    core_rows = pl.ds(pl.multiple_of(place.c * 256, 256), 256)
    twin_rows = pl.ds(pl.multiple_of(256 - place.c * 256, 256), 256)
    for_tokens = RingExchange(
        task,
        wires,
        lambda y: tokens.at[core_rows, pl.ds(pl.multiple_of(y * 1024, 1024), 1024)],
        lambda dy: far_tokens.at[dy - 1, core_rows, :],
    )
    for_tokens.open()
    token_slot = wires.claim(3)
    g3 = tokens[pl.ds(512, 16), :].astype(F32)
    gain_all[...] = g3[0:1, :] + g3[1:2, :] + g3[2:3, :]
    summed = stat_own[...]
    for hop in range(1, 8):
        statistics.wait(hop)
        summed = summed + stat_land[hop - 1]
    counts, totals, squares = summed[0:1, :], summed[1:2, :], summed[2:3, :]
    small_rows = (head_bias, old_mean, old_scale)
    bias, pop_mean, pop_scale = (
        jnp.concatenate(
            [ref[...], jnp.full((1, 128 - ref.shape[1]), fill, F32)], axis=1
        )
        for ref, fill in zip(small_rows, (0.0, 0.0, 1.0))
    )
    pop_mean, pop_scale = pltpu.roll(pop_mean, ACTIONS, 1), pltpu.roll(pop_scale, ACTIONS, 1)
    pop_scale = jnp.where(lanes((1, 128)) < ACTIONS, 1.0, pop_scale)
    mean, scale = popart_update(counts, totals, squares, pop_mean, pop_scale)
    is_value = lanes((1, 128)) >= ACTIONS
    ratio = jnp.where(is_value, pop_scale / scale, 1.0)
    new_bias = jnp.where(is_value, (pop_scale * bias + pop_mean - mean) / scale, bias)
    new_head[pl.ds(0, 75), :] = (head[...].astype(F32) * as_column(ratio)[0:75, :]).astype(BF16)
    new_head[pl.ds(75, 53), :] = jnp.zeros((53, 256), BF16)
    stats[...] = jnp.concatenate([mean, scale, new_bias, jnp.zeros((5, 128), F32)], axis=0)

    scatter.finish_far()
    scatter.finish_across()
    scatter.finish_near()
    first_env = me * 2
    columns = [
        step_columns(ref, first_env) for ref in (actions, rewards, ends, behaviour)
    ]
    columns[2] = DISCOUNT * (1.0 - columns[2])
    env = [
        jnp.sum(jnp.where(lanes((1, 32)) == first_env + e, tasks[...].astype(F32), 0.0), axis=1, keepdims=True)
        for e in (0, 1)
    ]
    game = jnp.where(sublanes((32, 128)) < 16, env[0], env[1])
    own_value = lanes((32, 128)) == game.astype(jnp.int32) + ACTIONS
    own_rows = pl.ds(pl.multiple_of(me * 32, 32), 32)

    def store(half, value):
        residual[:, half_cols(half)] = (
            value + tokens[own_rows, half_cols(half)].astype(F32)
        )

    scatter.finish(store)
    for m in range(2):
        v = residual[pl.ds(m * 16, 16), :]
        inverse = lax.rsqrt(jnp.mean(v * v, axis=1, keepdims=True) + NORM_EPS)
        normed[pl.ds(pl.multiple_of(me * 32 + m * 16, 16), 16), :] = (
            v * inverse * gain_all[...]
        ).astype(BF16)
    spread = Gather(place, wires, row_view(normed), gather_b)
    spread.open()
    for_hidden.relay(0)
    for_hidden.relay(1)
    heads = AllPairs(wires, "tp", 16, head_land)

    def out_slab(dz):
        start = plus(place.z, dz, 4) * 128
        rows = pl.ds(pl.multiple_of(start, 128), 128)
        v = dot(normed[rows, :], w_out_v[...])
        pre_out[rows, :] = v
        hidden_out[rows, :] = (v * sigmoid(v)).astype(BF16)
        head_part[rows, :] = dot(hidden_out[rows, :], new_head[...], ((1,), (1,))).astype(BF16)

    spread.middle()
    get_out.wait()
    spread.wait_twin(spread.OWN, spread.ACROSS)
    out_slab(0)
    spread.late()
    spread.wait_twin(spread.FROM_UP, spread.UP_ACROSS)
    out_slab(1)
    spread.last()
    spread.wait_twin(spread.FROM_DOWN, spread.DOWN_ACROSS)
    out_slab(3)
    spread.wait_twin(spread.FAR, spread.FAR_ACROSS)
    out_slab(2)

    def frames_of(ref):
        return lambda device: ref.at[pl.ds(pl.multiple_of(device * 32, 32), 32), :]

    for hop in range(1, 16):
        heads.post(hop, frames_of(head_part))
    for dy in (1, 2, 3):
        for_tokens.wait(dy)
        share = far_tokens.at[dy - 1, core_rows, :]
        wires.send(share, share, token_slot + dy - 1, place.partner)
    for_hidden.end()
    for b in range(4):
        hidden_t[:, b * 512 : b * 512 + 512] = (
            hidden_ring[b * 4 : b * 4 + 4].reshape(512, 256).T
        )
    outputs = head_part[own_rows, :].astype(F32)
    for hop in range(1, 16):
        heads.wait(hop)
        outputs = outputs + head_land[hop - 1].astype(F32)
    d_own = loss_gradient(outputs + new_bias, own_value, columns, mean, scale)
    d_heads[own_rows, :] = d_own.astype(BF16)
    d_slot = wires.claim(15)
    d_view = frames_of(d_heads)
    for hop in range(1, 16):
        wires.send(d_view(me), d_view(me), d_slot + hop - 1, plus(me, hop, 16))
    for hop in range(1, 16):
        wires.arrived(d_view(plus(me, 16 - hop, 16)), d_slot + hop - 1)
    wires.drain()

    def pre_gradient(m, carry):
        r = pl.ds(pl.multiple_of(m * 128, 128), 128)
        d_hidden = dot(d_heads[r, :], new_head[...])
        d_pre_out[r, :] = (d_hidden * slope(pre_out[r, :])).astype(BF16)
        return carry

    lax.fori_loop(0, 4, pre_gradient, 0)
    for_out = TaskSum(task, wires, slab_rows(512), whole_out, land_out, x_out, sum_out)
    mixes = [
        TaskSum(task, wires, wide_piece(n), whole_mix, None, x_mix.at[n], sum_mix) for n in (0, 1)
    ]
    x_pieces = (x_in.at[pl.ds(0, 256), :], x_in.at[pl.ds(256, 272), :])
    ins = [
        TaskSum(task, wires, tall_piece(n), whole_in, None, x_pieces[n], sum_in) for n in (0, 1)
    ]

    def tall_product(left, right, whole, height, dy):
        k = plus(task.y, dy, 4)

        def tile(n, carry):
            feature = pl.multiple_of(k * 1024 + n * 256, 256)
            at = pl.multiple_of((k * 2 + n // 2) * height + lax.rem(n, 2) * 256, 16)
            value = dot(left[pl.ds(0, 512), pl.ds(feature, 256)], right[...], ((0,), (0,)))
            whole[pl.ds(at, 256), :] = value.astype(BF16)
            return carry

        lax.fori_loop(0, 4, tile, 0)

    def mix_product(part, n):
        at = pl.multiple_of(part * 512 + n * 256, 256)
        whole_mix[:, pl.ds(at, 256)] = dot(
            hidden_t[...], residual_ring[:, pl.ds(at, 256)]
        ).astype(BF16)

    def in_product(part, n):
        at = pl.multiple_of(part * 512 + n * 256, 256)
        here = pl.ds(pl.multiple_of(task.y * 1024 + at, 256), 256)
        value = dot(tokens[pl.ds(0, 512), here], d_pre_in[task.y], ((0,), (0,)))
        for dy in (1, 2, 3):
            value = value + dot(
                far_tokens[dy - 1, :, pl.ds(at, 256)],
                d_pre_in[plus(task.y, dy, 4)],
                ((0,), (0,)),
            )
        whole_in[pl.ds(pl.multiple_of(part * 528 + n * 256, 16), 256), :] = value.astype(BF16)

    def out_product(dy):
        tall_product(normed, d_pre_out, whole_out, 512, dy)

    def out_first():
        out_product(2)
        for_out.far()

    scatter = Scatter(place, wires, partial, twin_part_b, landing_b, scatter_slots)
    scatter.open(lambda half: wide_product(d_pre_out, w_out_v, partial, half, True), out_first)
    out_product(1)
    out_product(3)
    for_out.near()
    scatter.finish_far()
    scatter.finish_across()
    out_product(0)
    for_out.relay()
    scatter.finish_near()

    def store(half, value):
        d_normed[:, half_cols(half)] = value

    scatter.finish(store)
    gain_rows = jnp.zeros((8, 4096), F32)
    for m in range(2):
        r = pl.ds(m * 16, 16)
        v = residual[r, :]
        inverse = lax.rsqrt(jnp.mean(v * v, axis=1, keepdims=True) + NORM_EPS)
        d = d_normed[r, :]
        scaled = d * gain_all[...]
        inner = jnp.sum(scaled * v, axis=1, keepdims=True)
        step = inverse * scaled - v * (inverse * inverse * inverse * inner * (1.0 / 4096))
        arrived[pl.ds(pl.multiple_of(me * 32 + m * 16, 16), 16), :] = step.astype(BF16)
        d_normed[r, :] = d * v * inverse
    gather = Gather(place, wires, row_view(arrived), gather_a)
    gather.open()
    ring_rows = lambda y: pl.ds(pl.multiple_of(me * 128 + y * 32, 32), 32)
    quarter = lambda y: pl.ds(pl.multiple_of(y * 1024, 1024), 1024)
    own32 = pl.ds(pl.multiple_of(me * 32, 32), 32)
    residual_ring[ring_rows(task.y), :] = arrived[own32, quarter(task.y)]
    for_residual = RingExchange(
        task,
        wires,
        lambda y: arrived.at[own32, quarter(y)],
        lambda dy: residual_ring.at[ring_rows(plus(task.y, dy, 4)), :],
    )
    for dy in (2, 1, 3):
        y = plus(task.y, dy, 4)
        wires.send(
            arrived.at[own32, quarter(y)],
            residual_ring.at[ring_rows(task.y), :],
            for_residual.first + 3 - dy,
            task.xh * 4 + y,
            "task",
        )
    for m in range(4):
        gain_rows = gain_rows + d_normed[pl.ds(m * 8, 8), :]
    for n in range(16):
        gain_parts[n] = gain_rows[:, n * 256 : n * 256 + 256]
    gains = AllPairs(wires, "tp", 16, gain_land)
    for hop in range(1, 16):
        gains.post(hop, lambda peer: gain_parts.at[peer])

    def hidden_slab(dz):
        rows = pl.ds(pl.multiple_of(plus(place.z, dz, 4) * 128, 128), 128)
        d = dot(arrived[rows, :], w_mix_v[...], ((1,), (1,)))
        d_pre_in[task.y, rows, :] = (d * slope(pre_in[rows, :])).astype(BF16)

    slabs = (0, 1, 3, 2)
    for_slope = RingGather(
        task,
        wires,
        lambda y, piece: d_pre_in.at[
            y, pl.ds(pl.multiple_of(plus(place.z, slabs[piece], 4) * 128, 128), 128), :
        ],
        4,
    )
    for_out.fold()
    gather.middle()
    for_out.finish()
    gather.wait_twin(gather.OWN, gather.ACROSS)
    hidden_slab(0)
    for_slope.open(0)
    gather.late()
    for dy in (1, 3, 2):
        for_residual.wait(dy)
    ring = Gather(
        place,
        wires,
        lambda block, half: residual_ring.at[
            pl.ds(pl.multiple_of(block * 128, 128), 128), pl.ds(half * 512, 512)
        ],
        gather_b,
        True,
    )
    ring.open()
    gather.wait_twin(gather.FROM_UP, gather.UP_ACROSS)
    hidden_slab(1)
    for_slope.open(1)
    gather.last()
    gather.wait_twin(gather.FROM_DOWN, gather.DOWN_ACROSS)
    hidden_slab(3)
    for_slope.open(2)
    for_slope.relay(0)
    gather.wait_twin(gather.FAR, gather.FAR_ACROSS)
    hidden_slab(2)
    for_slope.open(3)
    small = dot(d_heads[...], hidden_out[...], ((0,), (0,)))
    bias = jnp.sum(d_heads[...].astype(F32), axis=0, keepdims=True)
    gain_total = jnp.sum(gain_parts[me], axis=0, keepdims=True)
    for hop in range(1, 16):
        gains.wait(hop)
        gain_total = gain_total + jnp.sum(gain_land[hop - 1], axis=0, keepdims=True)
    row = sublanes((128, 256))
    bias = jnp.concatenate([bias, jnp.zeros((1, 128), F32)], axis=1)
    small_own[...] = jnp.where(
        row == 80, bias, jnp.where(row == 88, gain_total, small)
    ).astype(BF16)
    small_rows = lambda y: small_own.at[pl.ds(pl.multiple_of(y * 32, 32), 32), :]
    for_small = RingExchange(task, wires, small_rows, lambda dy: small_land.at[dy - 1])
    for_small.open()
    for_slope.relay(1)
    for_slope.relay(2)
    ring.middle_near()
    for_slope.relay(3)
    for_out.spread()
    ring.middle_across()
    for dy in (1, 2, 3):
        wires.arrived(far_tokens.at[dy - 1, twin_rows, :], token_slot + dy - 1)
    extra = small_rows(task.y)[...].astype(F32)
    for dy in (1, 3, 2):
        for_small.wait(dy)
        extra = extra + small_land[dy - 1].astype(F32)
    for part in (0, 1):
        whole_in[pl.ds(part * 528 + 512, 16), :] = extra[part * 16 : part * 16 + 16, :].astype(BF16)
    for_slope.end()
    in_product(1 - task.xh, 0)
    ins[0].fold()
    in_product(1 - task.xh, 1)
    ins[1].fold()
    ring.middle_far()
    in_product(task.xh, 0)
    ring.late()
    in_product(task.xh, 1)
    ins[0].finish()
    ring.last()
    ins[1].finish()
    ring.wait_twin(*range(8))
    mix_product(1 - task.xh, 0)
    mixes[0].fold()
    mix_product(1 - task.xh, 1)
    mixes[1].fold()
    mix_product(task.xh, 0)
    mix_product(task.xh, 1)
    for_out.spread_far()
    ins[0].spread()
    ins[1].spread()
    mixes[0].finish()
    ins[0].spread_far()
    mixes[1].finish()
    ins[1].spread_far()
    mixes[0].spread()
    mixes[1].spread()
    for_out.end()
    keep_out = load(sum_out, sum_out_hbm, local_sems, 4)
    mixes[0].spread_far()
    mixes[1].spread_far()
    ins[0].end()
    ins[1].end()
    keep_in = load(sum_in, sum_in_hbm, local_sems, 6)
    mixes[0].end()
    mixes[1].end()
    keep_mix = load(sum_mix, sum_mix_hbm, local_sems, 5)
    wires.drain()
    for keep in (keep_out, keep_mix, keep_in):
        keep.wait()


def finish_kernel(
    sum_out, sum_mix, sum_in, new_head, stats,
    grad_in, grad_mix, grad_out, gain, head, bias, head_now, bias_now, mean, scale,
    out_b, mix_b, in_b, small_b, out_f, mix_f, in_f, sems,
):
    gets = []
    for n in range(8):
        r = pl.ds(n * 512, 512)
        gets.append(load(sum_in.at[pl.ds(n * 528, 512), :], in_b.at[r, :], sems, n))
    for n in range(8):
        gets.append(
            load(sum_in.at[pl.ds(n * 528 + 512, 16), :], small_b.at[pl.ds(n * 16, 16), :], sems, 8 + n)
        )
    for n in range(4):
        r = pl.ds(n * 64, 64)
        gets.append(load(sum_mix.at[r, :], mix_b.at[r, :], sems, 16 + n))
    for n in range(8):
        r = pl.ds(n * 512, 512)
        gets.append(load(sum_out.at[r, :], out_b.at[r, :], sems, 20 + n))
    puts = []
    for n in range(8):
        r = pl.ds(n * 512, 512)
        gets[n].wait()
        in_f[r, :] = in_b[r, :].astype(F32)
        puts.append(load(in_f.at[r, :], grad_in.at[r, :], sems, 28 + n))
    for n in range(4):
        r = pl.ds(n * 64, 64)
        gets[16 + n].wait()
        mix_f[r, :] = mix_b[r, :].astype(F32)
        puts.append(load(mix_f.at[r, :], grad_mix.at[r, :], sems, 36 + n))
    for n in range(8):
        r = pl.ds(n * 512, 512)
        gets[20 + n].wait()
        out_f[r, :] = out_b[r, :].astype(F32)
        puts.append(load(out_f.at[r, :], grad_out.at[r, :], sems, 40 + n))
    for n in range(8):
        gets[8 + n].wait()
    small = small_b[...].astype(F32)
    head[...] = small[0:75, :]
    bias[...] = small[80:81, 0:75]
    gain[...] = small[88:89, :]
    head_now[...] = new_head[0:75, :]
    values = pltpu.roll(stats[...], 128 - ACTIONS, 1)
    mean[...] = values[0:1, 0:TASKS]
    scale[...] = values[1:2, 0:TASKS]
    bias_now[...] = stats[2:3, 0:75]
    for put in puts:
        put.wait()


def hbm():
    return pl.BlockSpec(memory_space=pltpu.HBM)


def vmem():
    return pl.BlockSpec(memory_space=pltpu.VMEM)


def step_call(*arguments):
    v, h = vmem(), hbm()
    scratch = [
        ((528, 4096), BF16), ((4096, 256), BF16), ((256, 4096), BF16), ((4096, 256), BF16),
        ((512, 256), F32), ((512, 256), BF16), ((32, 4096), F32), ((1, 4096), F32),
        ((512, 4096), BF16),
        ((512, 256), F32), ((512, 256), BF16), ((512, 128), BF16), ((15, 32, 128), BF16),
        ((512, 128), BF16), ((8, 128), F32), ((7, 8, 128), F32),
        ((512, 256), BF16), ((4, 512, 256), BF16), ((256, 2048), BF16), ((32, 4096), F32),
        ((16, 4, 32, 256), BF16), ((3, 512, 1024), BF16), ((2048, 1024), BF16),
        ((128, 256), BF16), ((3, 32, 256), BF16),
        ((512, 4096), BF16), ((8, 32, 4096), BF16), ((7, 32, 4096), BF16),
        ((8, 32, 4096), BF16), ((7, 32, 4096), BF16), ((512, 4096), BF16),
        ((16, 8, 256), F32), ((15, 8, 256), F32),
        ((4096, 256), BF16), ((256, 1024), BF16), ((1056, 256), BF16),
        ((3, 2, 512, 256), BF16),
        ((512, 256), BF16), ((2, 256, 256), BF16), ((528, 256), BF16),
        ((4096, 256), BF16), ((256, 4096), BF16), ((4224, 256), BF16),
    ]
    return pl.pallas_call(
        step_kernel,
        out_shape=[
            jax.ShapeDtypeStruct((4096, 256), BF16),
            jax.ShapeDtypeStruct((256, 4096), BF16),
            jax.ShapeDtypeStruct((4224, 256), BF16),
            jax.ShapeDtypeStruct((128, 256), BF16),
            jax.ShapeDtypeStruct((8, 128), F32),
        ],
        in_specs=[h, v, h, h, h, v, v, v, v, v, v, v, v, v],
        out_specs=[h, h, h, v, v],
        scratch_shapes=[pltpu.VMEM(*s) for s in scratch]
        + [pltpu.SemaphoreType.DMA((SENDS,)), pltpu.SemaphoreType.DMA((RECEIVES,)), pltpu.SemaphoreType.DMA((7,))],
        compiler_params=pltpu.CompilerParams(
            collective_id=0, has_side_effects=True, vmem_limit_bytes=63 * 2**20
        ),
        name="step",
    )(*arguments)


def finish_call(*arguments):
    v, h = vmem(), hbm()
    return pl.pallas_call(
        finish_kernel,
        out_shape=[
            jax.ShapeDtypeStruct((4096, 256), F32),
            jax.ShapeDtypeStruct((256, 4096), F32),
            jax.ShapeDtypeStruct((4096, 256), F32),
            jax.ShapeDtypeStruct((1, 256), F32),
            jax.ShapeDtypeStruct((75, 256), F32),
            jax.ShapeDtypeStruct((1, 75), F32),
            jax.ShapeDtypeStruct((75, 256), BF16),
            jax.ShapeDtypeStruct((1, 75), F32),
            jax.ShapeDtypeStruct((1, TASKS), F32),
            jax.ShapeDtypeStruct((1, TASKS), F32),
        ],
        in_specs=[h, h, h, v, v],
        out_specs=[h, h, h, v, v, v, v, v, v, v],
        scratch_shapes=[
            pltpu.VMEM((4096, 256), BF16),
            pltpu.VMEM((256, 4096), BF16),
            pltpu.VMEM((4096, 256), BF16),
            pltpu.VMEM((128, 256), BF16),
            pltpu.VMEM((4096, 256), F32),
            pltpu.VMEM((256, 4096), F32),
            pltpu.VMEM((4096, 256), F32),
            pltpu.SemaphoreType.DMA((48,)),
        ],
        compiler_params=pltpu.CompilerParams(vmem_limit_bytes=63 * 2**20),
        name="finish",
    )(*arguments)


def on_device(
    observations, gain, w_in, w_mix, w_out, w_head, head_bias, pop_mean, pop_scale,
    task_indices, actions, rewards, episode_ends, behaviour_log_prob,
):
    sums = step_call(
        observations.reshape(512, 256),
        gain.reshape(1, 256),
        w_in,
        w_mix,
        w_out,
        w_head.T,
        head_bias.reshape(1, ACTIONS + TASKS),
        pop_mean.reshape(1, TASKS),
        pop_scale.reshape(1, TASKS),
        task_indices.reshape(1, 32),
        actions.T,
        rewards.T,
        episode_ends.T,
        behaviour_log_prob.T,
    )
    (
        grad_in, grad_mix, grad_out, grad_gain, grad_head, grad_bias,
        new_head, new_bias, mean, scale,
    ) = finish_call(*sums)
    return (
        grad_in,
        grad_mix,
        grad_out,
        grad_gain.reshape(256),
        grad_head.T,
        grad_bias.reshape(75),
        new_head.T,
        new_bias.reshape(75),
        mean.reshape(TASKS),
        scale.reshape(TASKS),
    )


def solution(mesh):
    in_specs = (
        P("task", None, "tp"),
        P("tp"),
        P(None, "tp"),
        P("tp", None),
        P(None, "tp"),
        P("tp", None),
        P(),
        P(),
        P(),
        P("task"),
        P("task", None),
        P("task", None),
        P("task", None),
        P("task", None),
    )
    out_specs = (
        P(None, "tp"),
        P("tp", None),
        P(None, "tp"),
        P("tp"),
        P("tp", None),
        P(),
        P("tp", None),
        P(),
        P(),
        P(),
    )
    return jax.shard_map(
        on_device, mesh=mesh, in_specs=in_specs, out_specs=out_specs, check_vma=False
    )
```

```python
import jax
import jax.numpy as jnp
from jax import lax
from jax.experimental import pallas as pl
from jax.experimental.pallas import tpu as pltpu
from jax.sharding import PartitionSpec as P

ACTIONS = 18
TASKS = 57
DISCOUNT = 0.99
BASELINE_COST = 0.5
ENTROPY_COST = 0.01
POPART_PRIOR = 64.0
NORM_EPS = 1e-06
LOSS_WEIGHT = 256**-0.5
SENDS = 176
RECEIVES = 218


MESH = pl.DeviceIdType.MESH
F32 = jnp.float32
BF16 = jnp.bfloat16
HALVES = (0, 1)


def plus(a, b, n):
    return lax.rem(a + b, n)


class Place:
    def __init__(self):
        self.me = lax.axis_index("tp")
        self.z = self.me // 4
        self.x = lax.rem(self.me // 2, 2)
        self.c = lax.rem(self.me, 2)
        self.across = self.at(0, 1)
        self.up = self.at(1, 0)
        self.down = self.at(3, 0)
        self.partner = self.at(0, 0, 1)

    def at(self, dz, dx, dc=0):
        return (plus(self.z, dz, 4) * 2 + plus(self.x, dx, 2)) * 2 + plus(self.c, dc, 2)


class Wires:
    def __init__(self, send_sems, recv_sems):
        self.send_sems = send_sems
        self.recv_sems = recv_sems
        self.sent = []
        self.slots = 0

    def claim(self, count):
        first = self.slots
        self.slots += count
        return first

    def send(self, src, dst, slot, peer, axis="tp"):
        copy = pltpu.make_async_remote_copy(
            src_ref=src,
            dst_ref=dst,
            send_sem=self.send_sems.at[len(self.sent)],
            recv_sem=self.recv_sems.at[slot],
            device_id={axis: peer},
            device_id_type=MESH,
        )
        copy.start()
        self.sent.append(copy)

    def arrived(self, dst, slot, axis="tp"):
        pltpu.make_async_remote_copy(
            src_ref=dst,
            dst_ref=dst,
            send_sem=self.send_sems.at[0],
            recv_sem=self.recv_sems.at[slot],
            device_id={axis: lax.axis_index(axis)},
            device_id_type=MESH,
        ).wait_recv()

    def drain(self):
        for copy in self.sent:
            copy.wait_send()
        self.sent = []


class Gather:
    ACROSS, FROM_DOWN, FROM_UP, DOWN_ACROSS, UP_ACROSS, FAR, FAR_ACROSS, OWN = range(8)

    def __init__(self, place, wires, view, first, far_across_on_z=False):
        self.place = place
        self.wires = wires
        self.view = view
        self.first = first
        self.on_z = far_across_on_z
        p = place
        self.block = {
            self.ACROSS: p.at(0, 1),
            self.FROM_DOWN: p.at(3, 0),
            self.FROM_UP: p.at(1, 0),
            self.DOWN_ACROSS: p.at(3, 1),
            self.UP_ACROSS: p.at(1, 1),
            self.FAR: p.at(2, 0),
            self.FAR_ACROSS: p.at(2, 1),
            self.OWN: p.me,
        }
        self.twin = {k: plus(b, 0, 16) + 1 - 2 * p.c for k, b in self.block.items()}

    def slot(self, kind, half):
        return self.first + kind * 2 + half

    def twin_slot(self, kind, half):
        return self.first + 14 + kind * 2 + half

    def pass_on(self, kind, half, peer, kind_there):
        v = self.view(self.block[kind], half)
        self.wires.send(v, v, self.slot(kind_there, half), peer)

    def to_twin(self, kind, half):
        v = self.view(self.block[kind], half)
        self.wires.send(v, v, self.twin_slot(kind, half), self.place.partner)

    def wait(self, kind, half):
        self.wires.arrived(self.view(self.block[kind], half), self.slot(kind, half))

    def wait_twin(self, *kinds):
        for kind in kinds:
            for half in HALVES:
                self.wires.arrived(
                    self.view(self.twin[kind], half), self.twin_slot(kind, half)
                )

    def open(self):
        p = self.place
        for half in HALVES:
            self.pass_on(self.OWN, half, p.up, self.FROM_DOWN)
            self.pass_on(self.OWN, half, p.down, self.FROM_UP)
            self.pass_on(self.OWN, half, p.across, self.ACROSS)
            self.to_twin(self.OWN, half)

    def middle(self):
        self.middle_near()
        self.middle_across()
        self.middle_far()

    def middle_near(self):
        p = self.place
        self.wait(self.FROM_DOWN, 0)
        self.pass_on(self.FROM_DOWN, 0, p.up, self.FAR)
        self.to_twin(self.FROM_DOWN, 0)
        self.wait(self.FROM_UP, 0)
        self.to_twin(self.FROM_UP, 0)
        self.wait(self.ACROSS, 0)
        self.pass_on(self.ACROSS, 0, p.down, self.UP_ACROSS)
        self.wait(self.FROM_UP, 1)
        self.pass_on(self.FROM_UP, 1, p.down, self.FAR)
        self.pass_on(self.ACROSS, 0, p.up, self.DOWN_ACROSS)
        self.to_twin(self.ACROSS, 0)
        self.to_twin(self.FROM_UP, 1)

    def middle_across(self):
        p = self.place
        self.wait(self.FROM_DOWN, 1)
        self.to_twin(self.FROM_DOWN, 1)
        self.wait(self.ACROSS, 1)
        self.pass_on(self.ACROSS, 1, p.up, self.DOWN_ACROSS)
        self.pass_on(self.ACROSS, 1, p.down, self.UP_ACROSS)
        self.to_twin(self.ACROSS, 1)

    def middle_far(self):
        for half in HALVES:
            self.wait(self.FAR, half)
            if not self.on_z:
                self.pass_on(self.FAR, half, self.place.across, self.FAR_ACROSS)
            self.to_twin(self.FAR, half)

    def late(self):
        for half in HALVES:
            for kind in (self.DOWN_ACROSS, self.UP_ACROSS):
                self.wait(kind, half)
                if self.on_z and (kind == self.UP_ACROSS) == (half == 1):
                    peer = self.place.down if half else self.place.up
                    self.pass_on(kind, half, peer, self.FAR_ACROSS)
                self.to_twin(kind, half)

    def last(self):
        for half in HALVES:
            self.wait(self.FAR_ACROSS, half)
            self.to_twin(self.FAR_ACROSS, half)


def half_cols(half):
    return pl.ds(half * 2048, 2048)


class Scatter:
    G, D, E, F, A, B, C = range(7)
    ORDER = ((2, 1), (1, 1), (3, 1), (1, 0), (3, 0), (2, 0), (0, 1), (0, 0))

    def __init__(self, place, wires, partial, twin_part, landing, first):
        self.place = place
        self.wires = wires
        self.partial = partial
        self.twin_part = twin_part
        self.landing = landing
        self.first = first

    def rows(self, where, dc=0):
        return pl.ds(pl.multiple_of(self.place.at(*where, dc) * 32, 32), 32)

    def mine(self, where, half):
        return self.partial.at[self.rows(where), half_cols(half)]

    def twins(self, where, half):
        return self.twin_part.at[self.ORDER.index(where), :, half_cols(half)]

    def land(self, kind, half):
        return self.landing.at[kind, :, half_cols(half)]

    def total(self, where, half, kinds=(), waited=()):
        slot = self.first + 14 + self.ORDER.index(where) * 2 + half
        if (where, half) not in self.seen:
            self.wires.arrived(self.twins(where, half), slot)
            self.seen.add((where, half))
        for kind in kinds:
            self.wires.arrived(self.land(kind, half), self.first + kind * 2 + half)
        value = self.mine(where, half)[...].astype(F32) + self.twins(where, half)[...].astype(F32)
        for kind in kinds:
            value = value + self.land(kind, half)[...].astype(F32)
        return value

    def forward(self, where, half, kinds, peer, kind_there):
        self.mine(where, half)[...] = self.total(where, half, kinds).astype(BF16)
        self.wires.send(
            self.mine(where, half),
            self.land(kind_there, half),
            self.first + kind_there * 2 + half,
            peer,
        )

    def open(self, produce, between=None):
        self.seen = set()
        p = self.place
        for half in HALVES:
            produce(half)
            for where in self.ORDER:
                self.wires.send(
                    self.partial.at[self.rows(where, 1), half_cols(half)],
                    self.twins(where, half),
                    self.first + 14 + self.ORDER.index(where) * 2 + half,
                    p.partner,
                )
            if half == 1 and between is not None:
                between()
            self.forward((2, 1), half, (), p.across, self.G)
            self.forward((1, 1), half, (), p.up, self.D)
            self.forward((3, 1), half, (), p.down, self.E)
        self.forward((1, 0), 1, (), p.up, self.B)
        self.forward((3, 0), 0, (), p.down, self.C)

    def finish_far(self):
        p = self.place
        self.forward((2, 0), 0, (self.G,), p.up, self.F)
        self.forward((2, 0), 1, (self.G,), p.down, self.F)

    def finish_across(self):
        for half in HALVES:
            self.forward((0, 1), half, (self.D, self.E), self.place.across, self.A)

    def finish_near(self):
        p = self.place
        self.forward((1, 0), 0, (self.F,), p.up, self.B)
        self.forward((3, 0), 1, (self.F,), p.down, self.C)

    def finish(self, store):
        for half in HALVES:
            store(half, self.total((0, 0), half, (self.A, self.B, self.C)))


def sigmoid(v):
    return 1.0 / (1.0 + jnp.exp(-v))


def dot(a, b, contract=((1,), (0,))):
    return lax.dot_general(a, b, (contract, ((), ())), preferred_element_type=F32)


def load(src, dst, sems, at):
    copy = pltpu.make_async_copy(src, dst, sems.at[at])
    copy.start()
    return copy


def wide_product(left, right, partial, half, transposed):
    def tile(n, carry):
        at = pl.multiple_of(half * 2048 + n * 256, 256)
        if transposed:
            value = dot(left[...], right[pl.ds(at, 256), :], ((1,), (1,)))
        else:
            value = dot(left[...], right[:, pl.ds(at, 256)])
        partial[:, pl.ds(at, 256)] = value.astype(BF16)
        return carry

    lax.fori_loop(0, 8, tile, 0)


def row_view(ref):
    return lambda block, half: ref.at[
        pl.ds(pl.multiple_of(block * 32, 32), 32), half_cols(half)
    ]


class TaskPlace:
    def __init__(self):
        task = lax.axis_index("task")
        self.xh = task // 4
        self.y = lax.rem(task, 4)
        self.up = self.xh * 4 + plus(self.y, 1, 4)
        self.down = self.xh * 4 + plus(self.y, 3, 4)
        self.across = (1 - self.xh) * 4 + self.y


class TaskSum:
    F, B, C = range(3)
    OWN, FROM_DOWN, FROM_UP, DOWN_ACROSS, UP_ACROSS, FAR, FAR_ACROSS = range(7)

    def __init__(self, place, wires, view, whole, land, land_x, result):
        self.place = place
        self.wires = wires
        self.view = view
        self.whole = whole
        self.land = land
        self.land_x = land_x
        self.result = result
        self.first = wires.claim(8) - 6 if land is None else wires.claim(14)

    def slab(self, ref, dy, part):
        return self.view(ref, plus(self.place.y, dy, 4) * 2 + part)

    def post(self, src, dst, slot, peer):
        self.wires.send(src, dst, self.first + slot, peer, "task")

    def wait(self, dst, slot):
        self.wires.arrived(dst, self.first + slot, "task")

    def far(self):
        p = self.place
        self.post(self.slab(self.whole, 2, 0), self.land.at[self.F, 0], 0, p.up)
        self.post(self.slab(self.whole, 2, 1), self.land.at[self.F, 1], 1, p.down)

    def near(self):
        p = self.place
        self.post(self.slab(self.whole, 1, 1), self.land.at[self.B, 1], 3, p.up)
        self.post(self.slab(self.whole, 3, 0), self.land.at[self.C, 0], 4, p.down)

    def relay(self):
        p = self.place
        for dy, part, kind, slot, peer in ((1, 0, self.B, 2, p.up), (3, 1, self.C, 5, p.down)):
            self.wait(self.land.at[self.F, part], part)
            own = self.slab(self.whole, dy, part)
            total = own[...].astype(F32) + self.land[self.F, part].astype(F32)
            own[...] = total.astype(BF16)
            self.post(own, self.land.at[kind, part], slot, peer)

    def local(self, part):
        if self.land is None:
            return self.view(self.whole, part)[...].astype(F32)
        return (
            self.slab(self.whole, 0, part)[...].astype(F32)
            + self.land[self.B, part].astype(F32)
            + self.land[self.C, part].astype(F32)
        )

    def fold(self):
        if self.land is None:
            away = self.view(self.whole, 1 - self.place.xh)
            self.post(away, self.land_x, 6, self.place.across)
            return
        for kind, part, slot in ((self.B, 1, 3), (self.C, 0, 4), (self.B, 0, 2), (self.C, 1, 5)):
            self.wait(self.land.at[kind, part], slot)
        other = 1 - self.place.xh
        away = self.slab(self.whole, 0, other)
        away[...] = self.local(other).astype(BF16)
        self.post(away, self.land_x, 6, self.place.across)

    def pass_on(self, kind, peer, kind_there):
        v = self.held(kind)
        self.post(v, v, 6 + kind_there, peer)

    def held(self, kind):
        dy, across = {
            self.OWN: (0, 0),
            self.FROM_DOWN: (3, 0),
            self.FROM_UP: (1, 0),
            self.DOWN_ACROSS: (3, 1),
            self.UP_ACROSS: (1, 1),
            self.FAR: (2, 0),
            self.FAR_ACROSS: (2, 1),
        }[kind]
        xh = self.place.xh
        return self.slab(self.result, dy, 1 - xh if across else xh)

    def across_held(self):
        return self.slab(self.result, 0, 1 - self.place.xh)

    def finish(self):
        p = self.place
        self.wait(self.land_x, 6)
        own = self.held(self.OWN)
        own[...] = (self.local(p.xh) + self.land_x[...].astype(F32)).astype(BF16)
        self.post(own, own, 13, p.across)
        self.pass_on(self.OWN, p.up, self.FROM_DOWN)
        self.pass_on(self.OWN, p.down, self.FROM_UP)

    def get(self, kind):
        self.wait(self.held(kind), 6 + kind)

    def spread(self):
        p = self.place
        self.get(self.FROM_DOWN)
        self.pass_on(self.FROM_DOWN, p.up, self.FAR)
        self.get(self.FROM_UP)
        v = self.across_held()
        self.wait(v, 13)
        self.post(v, v, 6 + self.DOWN_ACROSS, p.up)
        self.post(v, v, 6 + self.UP_ACROSS, p.down)

    def spread_far(self):
        self.get(self.UP_ACROSS)
        self.pass_on(self.UP_ACROSS, self.place.down, self.FAR_ACROSS)
        self.get(self.DOWN_ACROSS)

    def end(self):
        self.get(self.FAR)
        self.get(self.FAR_ACROSS)


class RingFirst:
    FROM_DOWN, FROM_UP, FAR, OWN = range(4)

    def __init__(self, sums):
        self.sums = sums
        self.place = sums.place
        self.first = sums.wires.claim(14)

    def halves(self, dy, across, half):
        xh = self.place.xh
        slab = self.sums.slab(self.sums.result, dy, 1 - xh if across else xh)
        return slab.at[:, pl.ds(half * 128, 128)]

    def held(self, kind, half):
        return self.halves({self.FROM_DOWN: 3, self.FROM_UP: 1, self.FAR: 2}[kind], 0, half)

    def along(self, v, kind, half, peer):
        self.sums.wires.send(v, v, self.first + kind * 2 + half, peer, "task")

    def over(self, dy):
        whole = self.sums.slab(self.sums.result, dy, self.place.xh)
        self.sums.wires.send(whole, whole, self.first + 6 + dy, self.place.across, "task")

    def wait(self, kind, half):
        self.sums.wires.arrived(self.held(kind, half), self.first + kind * 2 + half, "task")

    def finish(self):
        p, sums = self.place, self.sums
        sums.wait(sums.land_x, 6)
        own = sums.held(sums.OWN)
        own[...] = (sums.local(p.xh) + sums.land_x[...].astype(F32)).astype(BF16)
        for up_half, down_half in ((0, 1), (1, 0)):
            self.along(self.halves(0, 0, up_half), self.FROM_DOWN, up_half, p.up)
            self.along(self.halves(0, 0, down_half), self.FROM_UP, down_half, p.down)
        self.over(0)

    def relay(self):
        for kind, half, peer in (
            (self.FROM_DOWN, 0, self.place.up), (self.FROM_UP, 1, self.place.down)
        ):
            self.wait(kind, half)
            self.along(self.held(kind, half), self.FAR, half, peer)

    def cross(self):
        self.wait(self.FROM_DOWN, 1)
        self.over(3)
        self.wait(self.FROM_UP, 0)
        self.over(1)

    def cross_far(self):
        self.wait(self.FAR, 0)
        self.wait(self.FAR, 1)
        self.over(2)

    def end(self):
        for dy in range(4):
            whole = self.sums.slab(self.sums.result, dy, 1 - self.place.xh)
            self.sums.wires.arrived(whole, self.first + 6 + dy, "task")


class RingGather:
    FROM_DOWN, FROM_UP, FAR = range(3)

    def __init__(self, place, wires, view, pieces):
        self.place = place
        self.wires = wires
        self.view = view
        self.pieces = pieces
        self.first = wires.claim(3 * pieces)

    def block(self, kind, piece):
        dy = {self.FROM_DOWN: 3, self.FROM_UP: 1, self.FAR: 2}[kind]
        return self.view(plus(self.place.y, dy, 4), piece)

    def post(self, v, kind, piece, peer):
        self.wires.send(v, v, self.first + kind * self.pieces + piece, peer, "task")

    def wait(self, kind, piece):
        self.wires.arrived(
            self.block(kind, piece), self.first + kind * self.pieces + piece, "task"
        )

    def open(self, piece):
        p = self.place
        v = self.view(p.y, piece)
        self.post(v, self.FROM_DOWN, piece, p.up)
        self.post(v, self.FROM_UP, piece, p.down)

    def relay(self, piece):
        kind = self.FROM_UP if piece % 2 else self.FROM_DOWN
        self.wait(kind, piece)
        peer = self.place.down if piece % 2 else self.place.up
        self.post(self.block(kind, piece), self.FAR, piece, peer)

    def end(self):
        for piece in range(self.pieces):
            self.wait(self.FROM_DOWN if piece % 2 else self.FROM_UP, piece)
            self.wait(self.FAR, piece)


class RingExchange:
    def __init__(self, place, wires, source, land):
        self.place = place
        self.wires = wires
        self.source = source
        self.land = land
        self.first = wires.claim(3)

    def open(self):
        p = self.place
        for dy in (2, 1, 3):
            y = plus(p.y, dy, 4)
            self.wires.send(
                self.source(y), self.land(4 - dy), self.first + 3 - dy, p.xh * 4 + y, "task"
            )

    def wait(self, dy):
        self.wires.arrived(self.land(dy), self.first + dy - 1, "task")


def slope(v):
    s = sigmoid(v)
    return s * (1.0 + v * (1.0 - s))


def slab_rows(height):
    return lambda ref, n: ref.at[pl.ds(pl.multiple_of(n * height, 16), height), :]


def tall_piece(piece):
    size = 272 if piece else 256
    return lambda ref, n: ref.at[pl.ds(pl.multiple_of(n * 528 + piece * 256, 16), size), :]


def wide_piece(piece):
    return lambda ref, n: ref.at[:, pl.ds(pl.multiple_of(n * 512 + piece * 256, 256), 256)]


def popart_update(counts, totals, squares, pop_mean, pop_scale):
    mixing = counts / (counts + POPART_PRIOR)
    safe_counts = jnp.maximum(counts, 1.0)
    batch_mean = totals / safe_counts
    batch_square = squares / safe_counts
    updated_return_mean = (1.0 - mixing) * pop_mean + mixing * batch_mean
    mean_gap = batch_mean - pop_mean
    variance = (
        (1.0 - mixing) * pop_scale * pop_scale
        + mixing * (batch_square - batch_mean * batch_mean)
        + mixing * (1.0 - mixing) * mean_gap * mean_gap
    )
    return (updated_return_mean, jnp.sqrt(variance))


class AllPairs:
    def __init__(self, wires, axis, size, land, first=None):
        self.wires = wires
        self.axis = axis
        self.size = size
        self.here = lax.axis_index(axis)
        self.land = land
        self.first = wires.claim(size - 1) if first is None else first

    def post(self, peer_at, src):
        peer = plus(self.here, peer_at, self.size)
        self.wires.send(
            src(peer), self.land.at[peer_at - 1], self.first + peer_at - 1, peer, self.axis
        )

    def wait(self, peer_at):
        self.wires.arrived(self.land.at[peer_at - 1], self.first + peer_at - 1, self.axis)


def greet_everyone():
    barrier = pltpu.get_barrier_semaphore()
    for axis, size in (("tp", 16), ("task", 8)):
        here = lax.axis_index(axis)
        for hop in range(1, size):
            pl.semaphore_signal(
                barrier, inc=1, device_id={axis: plus(here, hop, size)}, device_id_type=MESH
            )
    pl.semaphore_wait(barrier, 22)


def lanes(shape):
    return lax.broadcasted_iota(jnp.int32, shape, 1)


def sublanes(shape):
    return lax.broadcasted_iota(jnp.int32, shape, 0)


def popart_rows(tasks, rewards, ends):
    factors = DISCOUNT * (1.0 - ends[...].astype(F32))
    gains = rewards[...]
    running = jnp.zeros((1, 32), F32)
    total = jnp.zeros((1, 32), F32)
    square = jnp.zeros((1, 32), F32)
    for t in range(14, -1, -1):
        running = gains[t : t + 1, :] + factors[t : t + 1, :] * running
        total = total + running
        square = square + running * running
    member = sublanes((128, 32)) == tasks[...] + ACTIONS
    diagonal = sublanes((128, 128)) == lanes((128, 128))
    rows = []
    for value in (jnp.full((1, 32), 15.0, F32), total, square):
        column = jnp.sum(jnp.where(member, value, 0.0), axis=1, keepdims=True)
        rows.append(jnp.sum(jnp.where(diagonal, column, 0.0), axis=0, keepdims=True))
    return jnp.concatenate([*rows, jnp.zeros((5, 128), F32)], axis=0)


def as_column(row):
    diagonal = sublanes((128, 128)) == lanes((128, 128))
    return jnp.sum(jnp.where(diagonal, row, 0.0), axis=1, keepdims=True)


def step_columns(ref, first_env):
    value = ref[...].astype(F32)
    value = jnp.concatenate([value, jnp.zeros((1, 32), F32)], axis=0)
    lane = lanes((16, 32))
    return jnp.concatenate(
        [
            jnp.sum(jnp.where(lane == first_env + e, value, 0.0), axis=1, keepdims=True)
            for e in (0, 1)
        ],
        axis=0,
    )


def loss_gradient(outputs, own, columns, mean, scale):
    action, reward, factor, behaviour = columns
    shape = (32, 128)
    lane = lanes(shape)
    frame = lax.rem(sublanes(shape), 16)
    live = frame < 15

    def later(value, by):
        return jnp.where(frame + by < 16, pltpu.roll(value, 32 - by, 0), 0.0)

    def over_lanes(mask, value):
        return jnp.broadcast_to(
            jnp.sum(jnp.where(mask, value, 0.0), axis=1, keepdims=True), shape
        )

    is_logit = lane < ACTIONS
    chosen = lane == action.astype(jnp.int32)
    log_total = jnp.log(over_lanes(is_logit, jnp.exp(jnp.where(is_logit, outputs, 0.0))))
    log_prob = jnp.where(is_logit, outputs - log_total, 0.0)
    log_policy = over_lanes(chosen, log_prob)
    env_mean = over_lanes(own, mean)
    env_scale = over_lanes(own, scale)
    norm_values = over_lanes(own, outputs)
    values = norm_values * env_scale + env_mean
    clipped = jnp.minimum(jnp.exp(log_policy - behaviour), 1.0)
    total = jnp.where(live, clipped * (reward + factor * later(values, 1) - values), 0.0)
    decay = jnp.where(live, factor * clipped, 0.0)
    for by in (1, 2, 4, 8):
        total = total + decay * later(total, by)
        decay = decay * later(decay, by)
    targets = values + total
    following = later(targets, 1)
    advantage = clipped * ((reward + factor * following - env_mean) / env_scale - norm_values)
    normed_targets = (targets - env_mean) / env_scale
    policy = jnp.where(is_logit, jnp.exp(log_prob), 0.0)
    entropy = -over_lanes(is_logit, policy * log_prob)
    d_logits = -advantage * (jnp.where(chosen, 1.0, 0.0) - policy) + ENTROPY_COST * policy * (
        log_prob + entropy
    )
    d_value = -BASELINE_COST * (normed_targets - norm_values)
    d = jnp.where(is_logit, d_logits, jnp.where(own, d_value, 0.0))
    return jnp.where(live, d * LOSS_WEIGHT, 0.0)


def step_kernel(
    own_tokens, gain, w_in, w_mix, w_out, head, head_bias, old_mean, old_scale, tasks, actions, rewards, ends, behaviour,
    sum_out_hbm, sum_mix_hbm, sum_in_hbm, new_head, stats,
    tokens, w_in_v, w_mix_v, w_out_v, pre_in, hidden_in, residual, gain_all, normed,
    pre_out, hidden_out, head_part, head_land, d_heads, stat_own, stat_land,
    d_pre_out, d_pre_in, hidden_t, d_normed,
    hidden_ring, far_tokens, residual_ring, small_own, small_land,
    partial, twin_part, landing, twin_part_b, landing_b, arrived, gain_parts, gain_land,
    whole_out, whole_mix, whole_in, land_out, x_out, x_mix, x_in,
    sum_out, sum_mix, sum_in,
    send_sems, recv_sems, local_sems,
):
    place = Place()
    task = TaskPlace()
    wires = Wires(send_sems, recv_sems)
    gather_a, gather_b, scatter_slots = wires.claim(30), wires.claim(30), wires.claim(30)
    me = place.me
    own_cols = pl.ds(pl.multiple_of(me * 256, 256), 256)
    first = load(own_tokens, tokens.at[pl.ds(0, 512), own_cols], local_sems, 0)
    g = gain[...]
    hi = g.astype(BF16).astype(F32)
    mid = (g - hi).astype(BF16).astype(F32)
    low = g - hi - mid
    row = sublanes((16, 256))
    rows = jnp.where(row == 0, hi, jnp.where(row == 1, mid, jnp.where(row == 2, low, 0.0)))
    tokens[pl.ds(512, 16), own_cols] = rows.astype(BF16)
    greet_everyone()
    first.wait()

    def token_view(block, half):
        rows = pl.ds(0, 256) if half == 0 else pl.ds(256, 272)
        return tokens.at[rows, pl.ds(pl.multiple_of(block * 256, 256), 256)]

    gather = Gather(place, wires, token_view, gather_a)
    gather.open()
    get_in = load(w_in, w_in_v, local_sems, 1)
    get_mix = load(w_mix, w_mix_v, local_sems, 2)
    get_out = load(w_out, w_out_v, local_sems, 3)

    stat_own[...] = popart_rows(tasks, rewards, ends)
    statistics = AllPairs(wires, "task", 8, stat_land)
    for hop in range(1, 8):
        statistics.post(hop, lambda peer: stat_own)
    gather.middle()

    def slab(dz, opening=False):
        at = pl.multiple_of(plus(place.z, dz, 4) * 1024, 1024)

        def tile(m, carry):
            r = pl.ds(pl.multiple_of(m * 128, 128), 128)
            value = dot(tokens[r, pl.ds(at, 1024)], w_in_v[pl.ds(at, 1024), :])
            pre_in[r, :] = value if opening else pre_in[r, :] + value
            return carry

        lax.fori_loop(0, 4, tile, 0)

    get_in.wait()
    gather.wait_twin(gather.OWN, gather.ACROSS)
    slab(0, True)
    gather.late()
    gather.wait_twin(gather.FROM_UP, gather.UP_ACROSS)
    slab(1)
    gather.last()
    gather.wait_twin(gather.FROM_DOWN, gather.DOWN_ACROSS)
    slab(3)
    gather.wait_twin(gather.FAR, gather.FAR_ACROSS)
    slab(2)

    def activate(m, carry):
        r = pl.ds(pl.multiple_of(m * 128, 128), 128)
        v = pre_in[r, :]
        hidden = (v * sigmoid(v)).astype(BF16)
        hidden_in[r, :] = hidden
        hidden_ring[pl.ds(m * 4, 4), task.y] = hidden.reshape(4, 32, 256)
        return carry

    lax.fori_loop(0, 4, activate, 0)
    get_mix.wait()
    scatter = Scatter(place, wires, partial, twin_part, landing, scatter_slots)
    scatter.open(lambda half: wide_product(hidden_in, w_mix_v, partial, half, False))

    for_hidden = RingGather(
        task, wires, lambda y, half: hidden_ring.at[pl.ds(half * 8, 8), y], 2
    )
    for_hidden.open(0)
    for_hidden.open(1)
    core_rows = pl.ds(pl.multiple_of(place.c * 256, 256), 256)
    twin_rows = pl.ds(pl.multiple_of(256 - place.c * 256, 256), 256)
    for_tokens = RingExchange(
        task,
        wires,
        lambda y: tokens.at[core_rows, pl.ds(pl.multiple_of(y * 1024, 1024), 1024)],
        lambda dy: far_tokens.at[dy - 1, core_rows, :],
    )
    for_tokens.open()
    token_slot = wires.claim(3)
    g3 = tokens[pl.ds(512, 16), :].astype(F32)
    gain_all[...] = g3[0:1, :] + g3[1:2, :] + g3[2:3, :]
    summed = stat_own[...]
    for hop in range(1, 8):
        statistics.wait(hop)
        summed = summed + stat_land[hop - 1]
    counts, totals, squares = summed[0:1, :], summed[1:2, :], summed[2:3, :]
    small_rows = (head_bias, old_mean, old_scale)
    bias, pop_mean, pop_scale = (
        jnp.concatenate(
            [ref[...], jnp.full((1, 128 - ref.shape[1]), fill, F32)], axis=1
        )
        for ref, fill in zip(small_rows, (0.0, 0.0, 1.0))
    )
    pop_mean, pop_scale = pltpu.roll(pop_mean, ACTIONS, 1), pltpu.roll(pop_scale, ACTIONS, 1)
    pop_scale = jnp.where(lanes((1, 128)) < ACTIONS, 1.0, pop_scale)
    mean, scale = popart_update(counts, totals, squares, pop_mean, pop_scale)
    is_value = lanes((1, 128)) >= ACTIONS
    ratio = jnp.where(is_value, pop_scale / scale, 1.0)
    new_bias = jnp.where(is_value, (pop_scale * bias + pop_mean - mean) / scale, bias)
    new_head[pl.ds(0, 75), :] = (head[...].astype(F32) * as_column(ratio)[0:75, :]).astype(BF16)
    new_head[pl.ds(75, 53), :] = jnp.zeros((53, 256), BF16)
    stats[...] = jnp.concatenate([mean, scale, new_bias, jnp.zeros((5, 128), F32)], axis=0)

    scatter.finish_far()
    scatter.finish_across()
    scatter.finish_near()
    first_env = me * 2
    columns = [
        step_columns(ref, first_env) for ref in (actions, rewards, ends, behaviour)
    ]
    columns[2] = DISCOUNT * (1.0 - columns[2])
    env = [
        jnp.sum(jnp.where(lanes((1, 32)) == first_env + e, tasks[...].astype(F32), 0.0), axis=1, keepdims=True)
        for e in (0, 1)
    ]
    game = jnp.where(sublanes((32, 128)) < 16, env[0], env[1])
    own_value = lanes((32, 128)) == game.astype(jnp.int32) + ACTIONS
    own_rows = pl.ds(pl.multiple_of(me * 32, 32), 32)

    def store(half, value):
        residual[:, half_cols(half)] = (
            value + tokens[own_rows, half_cols(half)].astype(F32)
        )

    scatter.finish(store)
    for m in range(2):
        v = residual[pl.ds(m * 16, 16), :]
        inverse = lax.rsqrt(jnp.mean(v * v, axis=1, keepdims=True) + NORM_EPS)
        normed[pl.ds(pl.multiple_of(me * 32 + m * 16, 16), 16), :] = (
            v * inverse * gain_all[...]
        ).astype(BF16)
    spread = Gather(place, wires, row_view(normed), gather_b)
    spread.open()
    for_hidden.relay(0)
    for_hidden.relay(1)
    heads = AllPairs(wires, "tp", 16, head_land)

    def out_slab(dz):
        start = plus(place.z, dz, 4) * 128
        rows = pl.ds(pl.multiple_of(start, 128), 128)
        v = dot(normed[rows, :], w_out_v[...])
        pre_out[rows, :] = v
        hidden_out[rows, :] = (v * sigmoid(v)).astype(BF16)
        head_part[rows, :] = dot(hidden_out[rows, :], new_head[...], ((1,), (1,))).astype(BF16)

    spread.middle()
    get_out.wait()
    spread.wait_twin(spread.OWN, spread.ACROSS)
    out_slab(0)
    spread.late()
    spread.wait_twin(spread.FROM_UP, spread.UP_ACROSS)
    out_slab(1)
    spread.last()
    spread.wait_twin(spread.FROM_DOWN, spread.DOWN_ACROSS)
    out_slab(3)
    spread.wait_twin(spread.FAR, spread.FAR_ACROSS)
    out_slab(2)

    def frames_of(ref):
        return lambda device: ref.at[pl.ds(pl.multiple_of(device * 32, 32), 32), :]

    for hop in range(1, 16):
        heads.post(hop, frames_of(head_part))
    for dy in (1, 2, 3):
        for_tokens.wait(dy)
        share = far_tokens.at[dy - 1, core_rows, :]
        wires.send(share, share, token_slot + dy - 1, place.partner)
    for_hidden.end()
    for b in range(4):
        hidden_t[:, b * 512 : b * 512 + 512] = (
            hidden_ring[b * 4 : b * 4 + 4].reshape(512, 256).T
        )
    outputs = head_part[own_rows, :].astype(F32)
    for hop in range(1, 16):
        heads.wait(hop)
        outputs = outputs + head_land[hop - 1].astype(F32)
    d_own = loss_gradient(outputs + new_bias, own_value, columns, mean, scale)
    d_heads[own_rows, :] = d_own.astype(BF16)
    d_slot = wires.claim(15)
    d_view = frames_of(d_heads)
    for hop in range(1, 16):
        wires.send(d_view(me), d_view(me), d_slot + hop - 1, plus(me, hop, 16))
    for hop in range(1, 16):
        wires.arrived(d_view(plus(me, 16 - hop, 16)), d_slot + hop - 1)
    wires.drain()

    def pre_gradient(m, carry):
        r = pl.ds(pl.multiple_of(m * 128, 128), 128)
        d_hidden = dot(d_heads[r, :], new_head[...])
        d_pre_out[r, :] = (d_hidden * slope(pre_out[r, :])).astype(BF16)
        return carry

    lax.fori_loop(0, 4, pre_gradient, 0)
    for_out = TaskSum(task, wires, slab_rows(512), whole_out, land_out, x_out, sum_out)
    mixes = [
        TaskSum(task, wires, wide_piece(n), whole_mix, None, x_mix.at[n], sum_mix) for n in (0, 1)
    ]
    last_mix = RingFirst(mixes[1])
    x_pieces = (x_in.at[pl.ds(0, 256), :], x_in.at[pl.ds(256, 272), :])
    ins = [
        TaskSum(task, wires, tall_piece(n), whole_in, None, x_pieces[n], sum_in) for n in (0, 1)
    ]

    def tall_product(left, right, whole, height, dy):
        k = plus(task.y, dy, 4)

        def tile(n, carry):
            feature = pl.multiple_of(k * 1024 + n * 256, 256)
            at = pl.multiple_of((k * 2 + n // 2) * height + lax.rem(n, 2) * 256, 16)
            value = dot(left[pl.ds(0, 512), pl.ds(feature, 256)], right[...], ((0,), (0,)))
            whole[pl.ds(at, 256), :] = value.astype(BF16)
            return carry

        lax.fori_loop(0, 4, tile, 0)

    def mix_product(part, n):
        at = pl.multiple_of(part * 512 + n * 256, 256)
        whole_mix[:, pl.ds(at, 256)] = dot(
            hidden_t[...], residual_ring[:, pl.ds(at, 256)]
        ).astype(BF16)

    def in_product(part, n):
        at = pl.multiple_of(part * 512 + n * 256, 256)
        here = pl.ds(pl.multiple_of(task.y * 1024 + at, 256), 256)
        value = dot(tokens[pl.ds(0, 512), here], d_pre_in[task.y], ((0,), (0,)))
        for dy in (1, 2, 3):
            value = value + dot(
                far_tokens[dy - 1, :, pl.ds(at, 256)],
                d_pre_in[plus(task.y, dy, 4)],
                ((0,), (0,)),
            )
        whole_in[pl.ds(pl.multiple_of(part * 528 + n * 256, 16), 256), :] = value.astype(BF16)

    def out_product(dy):
        tall_product(normed, d_pre_out, whole_out, 512, dy)

    def out_first():
        out_product(2)
        for_out.far()

    scatter = Scatter(place, wires, partial, twin_part_b, landing_b, scatter_slots)
    scatter.open(lambda half: wide_product(d_pre_out, w_out_v, partial, half, True), out_first)
    out_product(1)
    out_product(3)
    for_out.near()
    scatter.finish_far()
    scatter.finish_across()
    out_product(0)
    for_out.relay()
    scatter.finish_near()

    def store(half, value):
        d_normed[:, half_cols(half)] = value

    scatter.finish(store)
    gain_rows = jnp.zeros((8, 4096), F32)
    for m in range(2):
        r = pl.ds(m * 16, 16)
        v = residual[r, :]
        inverse = lax.rsqrt(jnp.mean(v * v, axis=1, keepdims=True) + NORM_EPS)
        d = d_normed[r, :]
        scaled = d * gain_all[...]
        inner = jnp.sum(scaled * v, axis=1, keepdims=True)
        step = inverse * scaled - v * (inverse * inverse * inverse * inner * (1.0 / 4096))
        arrived[pl.ds(pl.multiple_of(me * 32 + m * 16, 16), 16), :] = step.astype(BF16)
        d_normed[r, :] = d * v * inverse
    gather = Gather(place, wires, row_view(arrived), gather_a)
    gather.open()
    ring_rows = lambda y: pl.ds(pl.multiple_of(me * 128 + y * 32, 32), 32)
    quarter = lambda y: pl.ds(pl.multiple_of(y * 1024, 1024), 1024)
    own32 = pl.ds(pl.multiple_of(me * 32, 32), 32)
    residual_ring[ring_rows(task.y), :] = arrived[own32, quarter(task.y)]
    for_residual = RingExchange(
        task,
        wires,
        lambda y: arrived.at[own32, quarter(y)],
        lambda dy: residual_ring.at[ring_rows(plus(task.y, dy, 4)), :],
    )
    for dy in (2, 1, 3):
        y = plus(task.y, dy, 4)
        wires.send(
            arrived.at[own32, quarter(y)],
            residual_ring.at[ring_rows(task.y), :],
            for_residual.first + 3 - dy,
            task.xh * 4 + y,
            "task",
        )
    for m in range(4):
        gain_rows = gain_rows + d_normed[pl.ds(m * 8, 8), :]
    for n in range(16):
        gain_parts[n] = gain_rows[:, n * 256 : n * 256 + 256]
    gains = AllPairs(wires, "tp", 16, gain_land, heads.first)
    for hop in range(1, 16):
        gains.post(hop, lambda peer: gain_parts.at[peer])

    def hidden_slab(dz):
        rows = pl.ds(pl.multiple_of(plus(place.z, dz, 4) * 128, 128), 128)
        d = dot(arrived[rows, :], w_mix_v[...], ((1,), (1,)))
        d_pre_in[task.y, rows, :] = (d * slope(pre_in[rows, :])).astype(BF16)

    slabs = (0, 1, 3, 2)
    for_slope = RingGather(
        task,
        wires,
        lambda y, piece: d_pre_in.at[
            y, pl.ds(pl.multiple_of(plus(place.z, slabs[piece], 4) * 128, 128), 128), :
        ],
        4,
    )
    for_out.fold()
    gather.middle()
    for_out.finish()
    gather.wait_twin(gather.OWN, gather.ACROSS)
    hidden_slab(0)
    for_slope.open(0)
    gather.late()
    for dy in (1, 3, 2):
        for_residual.wait(dy)
    ring = Gather(
        place,
        wires,
        lambda block, half: residual_ring.at[
            pl.ds(pl.multiple_of(block * 128, 128), 128), pl.ds(half * 512, 512)
        ],
        gather_b,
        True,
    )
    ring.open()
    gather.wait_twin(gather.FROM_UP, gather.UP_ACROSS)
    hidden_slab(1)
    for_slope.open(1)
    gather.last()
    gather.wait_twin(gather.FROM_DOWN, gather.DOWN_ACROSS)
    hidden_slab(3)
    for_slope.open(2)
    for_slope.relay(0)
    gather.wait_twin(gather.FAR, gather.FAR_ACROSS)
    hidden_slab(2)
    for_slope.open(3)
    small = dot(d_heads[...], hidden_out[...], ((0,), (0,)))
    bias = jnp.sum(d_heads[...].astype(F32), axis=0, keepdims=True)
    gain_total = jnp.sum(gain_parts[me], axis=0, keepdims=True)
    for hop in range(1, 16):
        gains.wait(hop)
        gain_total = gain_total + jnp.sum(gain_land[hop - 1], axis=0, keepdims=True)
    row = sublanes((128, 256))
    bias = jnp.concatenate([bias, jnp.zeros((1, 128), F32)], axis=1)
    small_own[...] = jnp.where(
        row == 80, bias, jnp.where(row == 88, gain_total, small)
    ).astype(BF16)
    small_rows = lambda y: small_own.at[pl.ds(pl.multiple_of(y * 32, 32), 32), :]
    for_small = RingExchange(task, wires, small_rows, lambda dy: small_land.at[dy - 1])
    for_small.open()
    for_slope.relay(1)
    for_slope.relay(2)
    for_slope.relay(3)
    ring.middle_near()
    for_out.spread()
    ring.middle_across()
    for dy in (1, 2, 3):
        wires.arrived(far_tokens.at[dy - 1, twin_rows, :], token_slot + dy - 1)
    extra = small_rows(task.y)[...].astype(F32)
    for dy in (1, 3, 2):
        for_small.wait(dy)
        extra = extra + small_land[dy - 1].astype(F32)
    for part in (0, 1):
        whole_in[pl.ds(part * 528 + 512, 16), :] = extra[part * 16 : part * 16 + 16, :].astype(BF16)
    for_slope.end()
    in_product(1 - task.xh, 0)
    ins[0].fold()
    in_product(1 - task.xh, 1)
    ins[1].fold()
    ring.middle_far()
    in_product(task.xh, 0)
    ring.late()
    in_product(task.xh, 1)
    ins[0].finish()
    ring.last()
    ins[1].finish()
    ring.wait_twin(*range(8))
    mix_product(1 - task.xh, 0)
    mixes[0].fold()
    mix_product(1 - task.xh, 1)
    mixes[1].fold()
    mix_product(task.xh, 0)
    mix_product(task.xh, 1)
    for_out.spread_far()
    ins[0].spread()
    ins[1].spread()
    mixes[0].finish()
    ins[0].spread_far()
    last_mix.finish()
    ins[1].spread_far()
    mixes[0].spread()
    last_mix.relay()
    last_mix.cross()
    for_out.end()
    keep_out = load(sum_out, sum_out_hbm, local_sems, 4)
    mixes[0].spread_far()
    last_mix.cross_far()
    ins[0].end()
    ins[1].end()
    keep_in = load(sum_in, sum_in_hbm, local_sems, 6)
    mixes[0].end()
    last_mix.end()
    keep_mix = load(sum_mix, sum_mix_hbm, local_sems, 5)
    wires.drain()
    for keep in (keep_out, keep_mix, keep_in):
        keep.wait()


def finish_kernel(
    sum_out, sum_mix, sum_in, new_head, stats,
    grad_in, grad_mix, grad_out, gain, head, bias, head_now, bias_now, mean, scale,
    out_b, mix_b, in_b, small_b, out_f, mix_f, in_f, sems,
):
    gets = []
    for n in range(8):
        r = pl.ds(n * 512, 512)
        gets.append(load(sum_in.at[pl.ds(n * 528, 512), :], in_b.at[r, :], sems, n))
    for n in range(8):
        gets.append(
            load(sum_in.at[pl.ds(n * 528 + 512, 16), :], small_b.at[pl.ds(n * 16, 16), :], sems, 8 + n)
        )
    for n in range(4):
        r = pl.ds(n * 64, 64)
        gets.append(load(sum_mix.at[r, :], mix_b.at[r, :], sems, 16 + n))
    for n in range(8):
        r = pl.ds(n * 512, 512)
        gets.append(load(sum_out.at[r, :], out_b.at[r, :], sems, 20 + n))
    puts = []
    for n in range(8):
        r = pl.ds(n * 512, 512)
        gets[n].wait()
        in_f[r, :] = in_b[r, :].astype(F32)
        puts.append(load(in_f.at[r, :], grad_in.at[r, :], sems, 28 + n))
    for n in range(4):
        r = pl.ds(n * 64, 64)
        gets[16 + n].wait()
        mix_f[r, :] = mix_b[r, :].astype(F32)
        puts.append(load(mix_f.at[r, :], grad_mix.at[r, :], sems, 36 + n))
    for n in range(8):
        r = pl.ds(n * 512, 512)
        gets[20 + n].wait()
        out_f[r, :] = out_b[r, :].astype(F32)
        puts.append(load(out_f.at[r, :], grad_out.at[r, :], sems, 40 + n))
    for n in range(8):
        gets[8 + n].wait()
    small = small_b[...].astype(F32)
    head[...] = small[0:75, :]
    bias[...] = small[80:81, 0:75]
    gain[...] = small[88:89, :]
    head_now[...] = new_head[0:75, :]
    values = pltpu.roll(stats[...], 128 - ACTIONS, 1)
    mean[...] = values[0:1, 0:TASKS]
    scale[...] = values[1:2, 0:TASKS]
    bias_now[...] = stats[2:3, 0:75]
    for put in puts:
        put.wait()


def hbm():
    return pl.BlockSpec(memory_space=pltpu.HBM)


def vmem():
    return pl.BlockSpec(memory_space=pltpu.VMEM)


def step_call(*arguments):
    v, h = vmem(), hbm()
    scratch = [
        ((528, 4096), BF16), ((4096, 256), BF16), ((256, 4096), BF16), ((4096, 256), BF16),
        ((512, 256), F32), ((512, 256), BF16), ((32, 4096), F32), ((1, 4096), F32),
        ((512, 4096), BF16),
        ((512, 256), F32), ((512, 256), BF16), ((512, 128), BF16), ((15, 32, 128), BF16),
        ((512, 128), BF16), ((8, 128), F32), ((7, 8, 128), F32),
        ((512, 256), BF16), ((4, 512, 256), BF16), ((256, 2048), BF16), ((32, 4096), F32),
        ((16, 4, 32, 256), BF16), ((3, 512, 1024), BF16), ((2048, 1024), BF16),
        ((128, 256), BF16), ((3, 32, 256), BF16),
        ((512, 4096), BF16), ((8, 32, 4096), BF16), ((7, 32, 4096), BF16),
        ((8, 32, 4096), BF16), ((7, 32, 4096), BF16), ((512, 4096), BF16),
        ((16, 8, 256), F32), ((15, 8, 256), F32),
        ((4096, 256), BF16), ((256, 1024), BF16), ((1056, 256), BF16),
        ((3, 2, 512, 256), BF16),
        ((512, 256), BF16), ((2, 256, 256), BF16), ((528, 256), BF16),
        ((4096, 256), BF16), ((256, 4096), BF16), ((4224, 256), BF16),
    ]
    return pl.pallas_call(
        step_kernel,
        out_shape=[
            jax.ShapeDtypeStruct((4096, 256), BF16),
            jax.ShapeDtypeStruct((256, 4096), BF16),
            jax.ShapeDtypeStruct((4224, 256), BF16),
            jax.ShapeDtypeStruct((128, 256), BF16),
            jax.ShapeDtypeStruct((8, 128), F32),
        ],
        in_specs=[h, v, h, h, h, v, v, v, v, v, v, v, v, v],
        out_specs=[h, h, h, v, v],
        scratch_shapes=[pltpu.VMEM(*s) for s in scratch]
        + [pltpu.SemaphoreType.DMA((SENDS,)), pltpu.SemaphoreType.DMA((RECEIVES,)), pltpu.SemaphoreType.DMA((7,))],
        compiler_params=pltpu.CompilerParams(
            collective_id=0, has_side_effects=True, vmem_limit_bytes=63 * 2**20
        ),
        name="step",
    )(*arguments)


def finish_call(*arguments):
    v, h = vmem(), hbm()
    return pl.pallas_call(
        finish_kernel,
        out_shape=[
            jax.ShapeDtypeStruct((4096, 256), F32),
            jax.ShapeDtypeStruct((256, 4096), F32),
            jax.ShapeDtypeStruct((4096, 256), F32),
            jax.ShapeDtypeStruct((1, 256), F32),
            jax.ShapeDtypeStruct((75, 256), F32),
            jax.ShapeDtypeStruct((1, 75), F32),
            jax.ShapeDtypeStruct((75, 256), BF16),
            jax.ShapeDtypeStruct((1, 75), F32),
            jax.ShapeDtypeStruct((1, TASKS), F32),
            jax.ShapeDtypeStruct((1, TASKS), F32),
        ],
        in_specs=[h, h, h, v, v],
        out_specs=[h, h, h, v, v, v, v, v, v, v],
        scratch_shapes=[
            pltpu.VMEM((4096, 256), BF16),
            pltpu.VMEM((256, 4096), BF16),
            pltpu.VMEM((4096, 256), BF16),
            pltpu.VMEM((128, 256), BF16),
            pltpu.VMEM((4096, 256), F32),
            pltpu.VMEM((256, 4096), F32),
            pltpu.VMEM((4096, 256), F32),
            pltpu.SemaphoreType.DMA((48,)),
        ],
        compiler_params=pltpu.CompilerParams(vmem_limit_bytes=63 * 2**20),
        name="finish",
    )(*arguments)


def on_device(
    observations, gain, w_in, w_mix, w_out, w_head, head_bias, pop_mean, pop_scale,
    task_indices, actions, rewards, episode_ends, behaviour_log_prob,
):
    sums = step_call(
        observations.reshape(512, 256),
        gain.reshape(1, 256),
        w_in,
        w_mix,
        w_out,
        w_head.T,
        head_bias.reshape(1, ACTIONS + TASKS),
        pop_mean.reshape(1, TASKS),
        pop_scale.reshape(1, TASKS),
        task_indices.reshape(1, 32),
        actions.T,
        rewards.T,
        episode_ends.T,
        behaviour_log_prob.T,
    )
    (
        grad_in, grad_mix, grad_out, grad_gain, grad_head, grad_bias,
        new_head, new_bias, mean, scale,
    ) = finish_call(*sums)
    return (
        grad_in,
        grad_mix,
        grad_out,
        grad_gain.reshape(256),
        grad_head.T,
        grad_bias.reshape(75),
        new_head.T,
        new_bias.reshape(75),
        mean.reshape(TASKS),
        scale.reshape(TASKS),
    )


def solution(mesh):
    in_specs = (
        P("task", None, "tp"),
        P("tp"),
        P(None, "tp"),
        P("tp", None),
        P(None, "tp"),
        P("tp", None),
        P(),
        P(),
        P(),
        P("task"),
        P("task", None),
        P("task", None),
        P("task", None),
        P("task", None),
    )
    out_specs = (
        P(None, "tp"),
        P("tp", None),
        P(None, "tp"),
        P("tp"),
        P("tp", None),
        P(),
        P("tp", None),
        P(),
        P(),
        P(),
    )
    return jax.shard_map(
        on_device, mesh=mesh, in_specs=in_specs, out_specs=out_specs, check_vma=False
    )
```

```python
import jax
import jax.numpy as jnp
from jax import lax
from jax.experimental import pallas as pl
from jax.experimental.pallas import tpu as pltpu
from jax.sharding import PartitionSpec as P

ACTIONS = 18
TASKS = 57
DISCOUNT = 0.99
BASELINE_COST = 0.5
ENTROPY_COST = 0.01
POPART_PRIOR = 64.0
NORM_EPS = 1e-06
LOSS_WEIGHT = 256**-0.5
SENDS = 144
RECEIVES = 217


MESH = pl.DeviceIdType.MESH
F32 = jnp.float32
BF16 = jnp.bfloat16
HALVES = (0, 1)


def plus(a, b, n):
    return lax.rem(a + b, n)


class Place:
    def __init__(self):
        self.me = lax.axis_index("tp")
        self.z = self.me // 4
        self.x = lax.rem(self.me // 2, 2)
        self.c = lax.rem(self.me, 2)
        self.across = self.at(0, 1)
        self.up = self.at(1, 0)
        self.down = self.at(3, 0)
        self.partner = self.at(0, 0, 1)

    def at(self, dz, dx, dc=0):
        return (plus(self.z, dz, 4) * 2 + plus(self.x, dx, 2)) * 2 + plus(self.c, dc, 2)


class Wires:
    def __init__(self, send_sems, recv_sems):
        self.send_sems = send_sems
        self.recv_sems = recv_sems
        self.sent = []
        self.free = list(range(SENDS))
        self.slots = 0

    def claim(self, count):
        first = self.slots
        self.slots += count
        return first

    def send(self, src, dst, slot, peer, axis="tp"):
        at = self.free.pop(0)
        copy = pltpu.make_async_remote_copy(
            src_ref=src,
            dst_ref=dst,
            send_sem=self.send_sems.at[at],
            recv_sem=self.recv_sems.at[slot],
            device_id={axis: peer},
            device_id_type=MESH,
        )
        copy.start()
        self.sent.append((copy, at, axis))

    def arrived(self, dst, slot, axis="tp"):
        pltpu.make_async_remote_copy(
            src_ref=dst,
            dst_ref=dst,
            send_sem=self.send_sems.at[0],
            recv_sem=self.recv_sems.at[slot],
            device_id={axis: lax.axis_index(axis)},
            device_id_type=MESH,
        ).wait_recv()

    def drain(self, axes=("tp", "task")):
        kept = []
        for copy, at, axis in self.sent:
            if axis in axes:
                copy.wait_send()
                self.free.append(at)
            else:
                kept.append((copy, at, axis))
        self.sent = kept


class Gather:
    ACROSS, FROM_DOWN, FROM_UP, DOWN_ACROSS, UP_ACROSS, FAR, FAR_ACROSS, OWN = range(8)

    def __init__(self, place, wires, view, first, far_across_on_z=False):
        self.place = place
        self.wires = wires
        self.view = view
        self.first = first
        self.on_z = far_across_on_z
        p = place
        self.block = {
            self.ACROSS: p.at(0, 1),
            self.FROM_DOWN: p.at(3, 0),
            self.FROM_UP: p.at(1, 0),
            self.DOWN_ACROSS: p.at(3, 1),
            self.UP_ACROSS: p.at(1, 1),
            self.FAR: p.at(2, 0),
            self.FAR_ACROSS: p.at(2, 1),
            self.OWN: p.me,
        }
        self.twin = {k: plus(b, 0, 16) + 1 - 2 * p.c for k, b in self.block.items()}

    def slot(self, kind, half):
        return self.first + kind * 2 + half

    def twin_slot(self, kind, half):
        return self.first + 14 + kind * 2 + half

    def pass_on(self, kind, half, peer, kind_there):
        v = self.view(self.block[kind], half)
        self.wires.send(v, v, self.slot(kind_there, half), peer)

    def to_twin(self, kind, half):
        v = self.view(self.block[kind], half)
        self.wires.send(v, v, self.twin_slot(kind, half), self.place.partner)

    def wait(self, kind, half):
        self.wires.arrived(self.view(self.block[kind], half), self.slot(kind, half))

    def wait_twin(self, *kinds):
        for kind in kinds:
            for half in HALVES:
                self.wires.arrived(
                    self.view(self.twin[kind], half), self.twin_slot(kind, half)
                )

    def open(self):
        p = self.place
        for half in HALVES:
            self.pass_on(self.OWN, half, p.up, self.FROM_DOWN)
            self.pass_on(self.OWN, half, p.down, self.FROM_UP)
            self.pass_on(self.OWN, half, p.across, self.ACROSS)
            self.to_twin(self.OWN, half)

    def middle(self):
        self.middle_near()
        self.middle_across()
        self.middle_far()

    def middle_near(self):
        p = self.place
        self.wait(self.FROM_DOWN, 0)
        self.pass_on(self.FROM_DOWN, 0, p.up, self.FAR)
        self.to_twin(self.FROM_DOWN, 0)
        self.wait(self.FROM_UP, 0)
        self.to_twin(self.FROM_UP, 0)
        self.wait(self.ACROSS, 0)
        self.pass_on(self.ACROSS, 0, p.down, self.UP_ACROSS)
        self.wait(self.FROM_UP, 1)
        self.pass_on(self.FROM_UP, 1, p.down, self.FAR)
        self.pass_on(self.ACROSS, 0, p.up, self.DOWN_ACROSS)
        self.to_twin(self.ACROSS, 0)
        self.to_twin(self.FROM_UP, 1)

    def middle_across(self):
        p = self.place
        self.wait(self.FROM_DOWN, 1)
        self.to_twin(self.FROM_DOWN, 1)
        self.wait(self.ACROSS, 1)
        self.pass_on(self.ACROSS, 1, p.up, self.DOWN_ACROSS)
        self.pass_on(self.ACROSS, 1, p.down, self.UP_ACROSS)
        self.to_twin(self.ACROSS, 1)

    def middle_far(self):
        for half in HALVES:
            self.wait(self.FAR, half)
            if not self.on_z:
                self.pass_on(self.FAR, half, self.place.across, self.FAR_ACROSS)
            self.to_twin(self.FAR, half)

    def late(self):
        for half in HALVES:
            for kind in (self.DOWN_ACROSS, self.UP_ACROSS):
                self.wait(kind, half)
                if self.on_z and (kind == self.UP_ACROSS) == (half == 1):
                    peer = self.place.down if half else self.place.up
                    self.pass_on(kind, half, peer, self.FAR_ACROSS)
                self.to_twin(kind, half)

    def last(self):
        for half in HALVES:
            self.wait(self.FAR_ACROSS, half)
            self.to_twin(self.FAR_ACROSS, half)


def half_cols(half):
    return pl.ds(half * 2048, 2048)


class Scatter:
    G, D, E, F, A, B, C = range(7)
    ORDER = ((2, 1), (1, 1), (3, 1), (1, 0), (3, 0), (2, 0), (0, 1), (0, 0))

    def __init__(self, place, wires, partial, twin_part, landing, first):
        self.place = place
        self.wires = wires
        self.partial = partial
        self.twin_part = twin_part
        self.landing = landing
        self.first = first

    def rows(self, where, dc=0):
        return pl.ds(pl.multiple_of(self.place.at(*where, dc) * 32, 32), 32)

    def mine(self, where, half):
        return self.partial.at[self.rows(where), half_cols(half)]

    def twins(self, where, half):
        return self.twin_part.at[self.ORDER.index(where), :, half_cols(half)]

    def land(self, kind, half):
        return self.landing.at[kind, :, half_cols(half)]

    def total(self, where, half, kinds=(), waited=()):
        slot = self.first + 14 + self.ORDER.index(where) * 2 + half
        if (where, half) not in self.seen:
            self.wires.arrived(self.twins(where, half), slot)
            self.seen.add((where, half))
        for kind in kinds:
            self.wires.arrived(self.land(kind, half), self.first + kind * 2 + half)
        value = self.mine(where, half)[...].astype(F32) + self.twins(where, half)[...].astype(F32)
        for kind in kinds:
            value = value + self.land(kind, half)[...].astype(F32)
        return value

    def forward(self, where, half, kinds, peer, kind_there):
        self.mine(where, half)[...] = self.total(where, half, kinds).astype(BF16)
        self.wires.send(
            self.mine(where, half),
            self.land(kind_there, half),
            self.first + kind_there * 2 + half,
            peer,
        )

    def open(self, produce, between=None):
        self.seen = set()
        p = self.place
        for half in HALVES:
            produce(half)
            for where in self.ORDER:
                self.wires.send(
                    self.partial.at[self.rows(where, 1), half_cols(half)],
                    self.twins(where, half),
                    self.first + 14 + self.ORDER.index(where) * 2 + half,
                    p.partner,
                )
            if half == 1 and between is not None:
                between()
            self.forward((2, 1), half, (), p.across, self.G)
            self.forward((1, 1), half, (), p.up, self.D)
            self.forward((3, 1), half, (), p.down, self.E)
        self.forward((1, 0), 1, (), p.up, self.B)
        self.forward((3, 0), 0, (), p.down, self.C)

    def finish_far(self):
        p = self.place
        self.forward((2, 0), 0, (self.G,), p.up, self.F)
        self.forward((2, 0), 1, (self.G,), p.down, self.F)

    def finish_across(self):
        for half in HALVES:
            self.forward((0, 1), half, (self.D, self.E), self.place.across, self.A)

    def finish_near(self):
        p = self.place
        self.forward((1, 0), 0, (self.F,), p.up, self.B)
        self.forward((3, 0), 1, (self.F,), p.down, self.C)

    def finish(self, store):
        for half in HALVES:
            store(half, self.total((0, 0), half, (self.A, self.B, self.C)))


def sigmoid(v):
    return 1.0 / (1.0 + jnp.exp(-v))


def dot(a, b, contract=((1,), (0,))):
    return lax.dot_general(a, b, (contract, ((), ())), preferred_element_type=F32)


def load(src, dst, sems, at):
    copy = pltpu.make_async_copy(src, dst, sems.at[at])
    copy.start()
    return copy


def wide_product(left, right, partial, half, transposed):
    def tile(n, carry):
        at = pl.multiple_of(half * 2048 + n * 256, 256)
        if transposed:
            value = dot(left[...], right[pl.ds(at, 256), :], ((1,), (1,)))
        else:
            value = dot(left[...], right[:, pl.ds(at, 256)])
        partial[:, pl.ds(at, 256)] = value.astype(BF16)
        return carry

    lax.fori_loop(0, 8, tile, 0)


def row_view(ref):
    return lambda block, half: ref.at[
        pl.ds(pl.multiple_of(block * 32, 32), 32), half_cols(half)
    ]


class TaskPlace:
    def __init__(self):
        task = lax.axis_index("task")
        self.xh = task // 4
        self.y = lax.rem(task, 4)
        self.up = self.xh * 4 + plus(self.y, 1, 4)
        self.down = self.xh * 4 + plus(self.y, 3, 4)
        self.across = (1 - self.xh) * 4 + self.y


class TaskSum:
    F, B, C = range(3)
    OWN, FROM_DOWN, FROM_UP, DOWN_ACROSS, UP_ACROSS, FAR, FAR_ACROSS = range(7)

    def __init__(self, place, wires, view, whole, land, land_x, result):
        self.place = place
        self.wires = wires
        self.view = view
        self.whole = whole
        self.land = land
        self.land_x = land_x
        self.result = result
        self.first = wires.claim(8) - 6 if land is None else wires.claim(14)

    def slab(self, ref, dy, part):
        return self.view(ref, plus(self.place.y, dy, 4) * 2 + part)

    def post(self, src, dst, slot, peer):
        self.wires.send(src, dst, self.first + slot, peer, "task")

    def wait(self, dst, slot):
        self.wires.arrived(dst, self.first + slot, "task")

    def far(self):
        p = self.place
        self.post(self.slab(self.whole, 2, 0), self.land.at[self.F, 0], 0, p.up)
        self.post(self.slab(self.whole, 2, 1), self.land.at[self.F, 1], 1, p.down)

    def near(self):
        p = self.place
        self.post(self.slab(self.whole, 1, 1), self.land.at[self.B, 1], 3, p.up)
        self.post(self.slab(self.whole, 3, 0), self.land.at[self.C, 0], 4, p.down)

    def relay(self):
        p = self.place
        for dy, part, kind, slot, peer in ((1, 0, self.B, 2, p.up), (3, 1, self.C, 5, p.down)):
            self.wait(self.land.at[self.F, part], part)
            own = self.slab(self.whole, dy, part)
            total = own[...].astype(F32) + self.land[self.F, part].astype(F32)
            own[...] = total.astype(BF16)
            self.post(own, self.land.at[kind, part], slot, peer)

    def local(self, part):
        if self.land is None:
            return self.view(self.whole, part)[...].astype(F32)
        return (
            self.slab(self.whole, 0, part)[...].astype(F32)
            + self.land[self.B, part].astype(F32)
            + self.land[self.C, part].astype(F32)
        )

    def fold(self):
        if self.land is None:
            away = self.view(self.whole, 1 - self.place.xh)
            self.post(away, self.land_x, 6, self.place.across)
            return
        for kind, part, slot in ((self.B, 1, 3), (self.C, 0, 4), (self.B, 0, 2), (self.C, 1, 5)):
            self.wait(self.land.at[kind, part], slot)
        other = 1 - self.place.xh
        away = self.slab(self.whole, 0, other)
        away[...] = self.local(other).astype(BF16)
        self.post(away, self.land_x, 6, self.place.across)

    def pass_on(self, kind, peer, kind_there):
        v = self.held(kind)
        self.post(v, v, 6 + kind_there, peer)

    def held(self, kind):
        dy, across = {
            self.OWN: (0, 0),
            self.FROM_DOWN: (3, 0),
            self.FROM_UP: (1, 0),
            self.DOWN_ACROSS: (3, 1),
            self.UP_ACROSS: (1, 1),
            self.FAR: (2, 0),
            self.FAR_ACROSS: (2, 1),
        }[kind]
        xh = self.place.xh
        return self.slab(self.result, dy, 1 - xh if across else xh)

    def across_held(self):
        return self.slab(self.result, 0, 1 - self.place.xh)

    def finish(self):
        p = self.place
        self.wait(self.land_x, 6)
        own = self.held(self.OWN)
        own[...] = (self.local(p.xh) + self.land_x[...].astype(F32)).astype(BF16)
        self.post(own, own, 13, p.across)
        self.pass_on(self.OWN, p.up, self.FROM_DOWN)
        self.pass_on(self.OWN, p.down, self.FROM_UP)

    def get(self, kind):
        self.wait(self.held(kind), 6 + kind)

    def spread(self):
        p = self.place
        self.get(self.FROM_DOWN)
        self.pass_on(self.FROM_DOWN, p.up, self.FAR)
        self.get(self.FROM_UP)
        v = self.across_held()
        self.wait(v, 13)
        self.post(v, v, 6 + self.DOWN_ACROSS, p.up)
        self.post(v, v, 6 + self.UP_ACROSS, p.down)

    def spread_far(self):
        self.get(self.UP_ACROSS)
        self.pass_on(self.UP_ACROSS, self.place.down, self.FAR_ACROSS)
        self.get(self.DOWN_ACROSS)

    def end(self):
        self.get(self.FAR)
        self.get(self.FAR_ACROSS)


class RingFirst:
    FROM_DOWN, FROM_UP, FAR, OWN = range(4)

    def __init__(self, sums):
        self.sums = sums
        self.place = sums.place
        self.first = sums.wires.claim(14)

    def halves(self, dy, across, half):
        xh = self.place.xh
        slab = self.sums.slab(self.sums.result, dy, 1 - xh if across else xh)
        return slab.at[:, pl.ds(half * 128, 128)]

    def held(self, kind, half):
        return self.halves({self.FROM_DOWN: 3, self.FROM_UP: 1, self.FAR: 2}[kind], 0, half)

    def along(self, v, kind, half, peer):
        self.sums.wires.send(v, v, self.first + kind * 2 + half, peer, "task")

    def over(self, dy):
        whole = self.sums.slab(self.sums.result, dy, self.place.xh)
        self.sums.wires.send(whole, whole, self.first + 6 + dy, self.place.across, "task")

    def wait(self, kind, half):
        self.sums.wires.arrived(self.held(kind, half), self.first + kind * 2 + half, "task")

    def finish(self):
        p, sums = self.place, self.sums
        sums.wait(sums.land_x, 6)
        own = sums.held(sums.OWN)
        own[...] = (sums.local(p.xh) + sums.land_x[...].astype(F32)).astype(BF16)
        for up_half, down_half in ((0, 1), (1, 0)):
            self.along(self.halves(0, 0, up_half), self.FROM_DOWN, up_half, p.up)
            self.along(self.halves(0, 0, down_half), self.FROM_UP, down_half, p.down)
        self.over(0)

    def relay(self):
        for kind, half, peer in (
            (self.FROM_DOWN, 0, self.place.up), (self.FROM_UP, 1, self.place.down)
        ):
            self.wait(kind, half)
            self.along(self.held(kind, half), self.FAR, half, peer)

    def cross(self):
        self.wait(self.FROM_DOWN, 1)
        self.over(3)
        self.wait(self.FROM_UP, 0)
        self.over(1)

    def cross_far(self):
        self.wait(self.FAR, 0)
        self.wait(self.FAR, 1)
        self.over(2)

    def end(self):
        for dy in range(4):
            whole = self.sums.slab(self.sums.result, dy, 1 - self.place.xh)
            self.sums.wires.arrived(whole, self.first + 6 + dy, "task")


class RingGather:
    FROM_DOWN, FROM_UP, FAR = range(3)

    def __init__(self, place, wires, view, pieces):
        self.place = place
        self.wires = wires
        self.view = view
        self.pieces = pieces
        self.first = wires.claim(3 * pieces)

    def block(self, kind, piece):
        dy = {self.FROM_DOWN: 3, self.FROM_UP: 1, self.FAR: 2}[kind]
        return self.view(plus(self.place.y, dy, 4), piece)

    def post(self, v, kind, piece, peer):
        self.wires.send(v, v, self.first + kind * self.pieces + piece, peer, "task")

    def wait(self, kind, piece):
        self.wires.arrived(
            self.block(kind, piece), self.first + kind * self.pieces + piece, "task"
        )

    def open(self, piece):
        p = self.place
        v = self.view(p.y, piece)
        self.post(v, self.FROM_DOWN, piece, p.up)
        self.post(v, self.FROM_UP, piece, p.down)

    def relay(self, piece):
        kind = self.FROM_UP if piece % 2 else self.FROM_DOWN
        self.wait(kind, piece)
        peer = self.place.down if piece % 2 else self.place.up
        self.post(self.block(kind, piece), self.FAR, piece, peer)

    def end(self):
        for piece in range(self.pieces):
            self.wait(self.FROM_DOWN if piece % 2 else self.FROM_UP, piece)
            self.wait(self.FAR, piece)


class RingExchange:
    def __init__(self, place, wires, source, land):
        self.place = place
        self.wires = wires
        self.source = source
        self.land = land
        self.first = wires.claim(3)

    def open(self):
        p = self.place
        for dy in (2, 1, 3):
            y = plus(p.y, dy, 4)
            self.wires.send(
                self.source(y), self.land(4 - dy), self.first + 3 - dy, p.xh * 4 + y, "task"
            )

    def wait(self, dy):
        self.wires.arrived(self.land(dy), self.first + dy - 1, "task")


def slope(v):
    s = sigmoid(v)
    return s * (1.0 + v * (1.0 - s))


def slab_rows(height):
    return lambda ref, n: ref.at[pl.ds(pl.multiple_of(n * height, 16), height), :]


def tall_piece(piece):
    size = 272 if piece else 256
    return lambda ref, n: ref.at[pl.ds(pl.multiple_of(n * 528 + piece * 256, 16), size), :]


def wide_piece(piece):
    return lambda ref, n: ref.at[:, pl.ds(pl.multiple_of(n * 512 + piece * 256, 256), 256)]


def popart_update(counts, totals, squares, pop_mean, pop_scale):
    mixing = counts / (counts + POPART_PRIOR)
    safe_counts = jnp.maximum(counts, 1.0)
    batch_mean = totals / safe_counts
    batch_square = squares / safe_counts
    updated_return_mean = (1.0 - mixing) * pop_mean + mixing * batch_mean
    mean_gap = batch_mean - pop_mean
    variance = (
        (1.0 - mixing) * pop_scale * pop_scale
        + mixing * (batch_square - batch_mean * batch_mean)
        + mixing * (1.0 - mixing) * mean_gap * mean_gap
    )
    return (updated_return_mean, jnp.sqrt(variance))


class AllPairs:
    def __init__(self, wires, axis, size, land, first=None):
        self.wires = wires
        self.axis = axis
        self.size = size
        self.here = lax.axis_index(axis)
        self.land = land
        self.first = wires.claim(size - 1) if first is None else first

    def post(self, peer_at, src):
        peer = plus(self.here, peer_at, self.size)
        self.wires.send(
            src(peer), self.land.at[peer_at - 1], self.first + peer_at - 1, peer, self.axis
        )

    def wait(self, peer_at):
        self.wires.arrived(self.land.at[peer_at - 1], self.first + peer_at - 1, self.axis)


def greet_everyone():
    barrier = pltpu.get_barrier_semaphore()
    for axis, size in (("tp", 16), ("task", 8)):
        here = lax.axis_index(axis)
        for hop in range(1, size):
            pl.semaphore_signal(
                barrier, inc=1, device_id={axis: plus(here, hop, size)}, device_id_type=MESH
            )
    pl.semaphore_wait(barrier, 22)


def lanes(shape):
    return lax.broadcasted_iota(jnp.int32, shape, 1)


def sublanes(shape):
    return lax.broadcasted_iota(jnp.int32, shape, 0)


def popart_rows(tasks, rewards, ends):
    factors = DISCOUNT * (1.0 - ends[...].astype(F32))
    gains = rewards[...]
    running = jnp.zeros((1, 32), F32)
    total = jnp.zeros((1, 32), F32)
    square = jnp.zeros((1, 32), F32)
    for t in range(14, -1, -1):
        running = gains[t : t + 1, :] + factors[t : t + 1, :] * running
        total = total + running
        square = square + running * running
    member = sublanes((128, 32)) == tasks[...] + ACTIONS
    diagonal = sublanes((128, 128)) == lanes((128, 128))
    rows = []
    for value in (jnp.full((1, 32), 15.0, F32), total, square):
        column = jnp.sum(jnp.where(member, value, 0.0), axis=1, keepdims=True)
        rows.append(jnp.sum(jnp.where(diagonal, column, 0.0), axis=0, keepdims=True))
    return jnp.concatenate([*rows, jnp.zeros((5, 128), F32)], axis=0)


def as_column(row):
    diagonal = sublanes((128, 128)) == lanes((128, 128))
    return jnp.sum(jnp.where(diagonal, row, 0.0), axis=1, keepdims=True)


def step_columns(ref, first_env):
    value = ref[...].astype(F32)
    value = jnp.concatenate([value, jnp.zeros((1, 32), F32)], axis=0)
    lane = lanes((16, 32))
    return jnp.concatenate(
        [
            jnp.sum(jnp.where(lane == first_env + e, value, 0.0), axis=1, keepdims=True)
            for e in (0, 1)
        ],
        axis=0,
    )


def loss_gradient(outputs, own, columns, mean, scale):
    action, reward, factor, behaviour = columns
    shape = (32, 128)
    lane = lanes(shape)
    frame = lax.rem(sublanes(shape), 16)
    live = frame < 15

    def later(value, by):
        return jnp.where(frame + by < 16, pltpu.roll(value, 32 - by, 0), 0.0)

    def over_lanes(mask, value):
        return jnp.broadcast_to(
            jnp.sum(jnp.where(mask, value, 0.0), axis=1, keepdims=True), shape
        )

    is_logit = lane < ACTIONS
    chosen = lane == action.astype(jnp.int32)
    log_total = jnp.log(over_lanes(is_logit, jnp.exp(jnp.where(is_logit, outputs, 0.0))))
    log_prob = jnp.where(is_logit, outputs - log_total, 0.0)
    log_policy = over_lanes(chosen, log_prob)
    env_mean = over_lanes(own, mean)
    env_scale = over_lanes(own, scale)
    norm_values = over_lanes(own, outputs)
    values = norm_values * env_scale + env_mean
    clipped = jnp.minimum(jnp.exp(log_policy - behaviour), 1.0)
    total = jnp.where(live, clipped * (reward + factor * later(values, 1) - values), 0.0)
    decay = jnp.where(live, factor * clipped, 0.0)
    for by in (1, 2, 4, 8):
        total = total + decay * later(total, by)
        decay = decay * later(decay, by)
    targets = values + total
    following = later(targets, 1)
    advantage = clipped * ((reward + factor * following - env_mean) / env_scale - norm_values)
    normed_targets = (targets - env_mean) / env_scale
    policy = jnp.where(is_logit, jnp.exp(log_prob), 0.0)
    entropy = -over_lanes(is_logit, policy * log_prob)
    d_logits = -advantage * (jnp.where(chosen, 1.0, 0.0) - policy) + ENTROPY_COST * policy * (
        log_prob + entropy
    )
    d_value = -BASELINE_COST * (normed_targets - norm_values)
    d = jnp.where(is_logit, d_logits, jnp.where(own, d_value, 0.0))
    return jnp.where(live, d * LOSS_WEIGHT, 0.0)


def step_kernel(
    own_tokens, gain, w_in, w_mix, w_out, head, head_bias, old_mean, old_scale, tasks, actions, rewards, ends, behaviour,
    sum_out_hbm, sum_mix_hbm, sum_in_hbm, new_head, stats,
    tokens, w_in_v, w_mix_v, w_out_v, pre_in, hidden_in, residual, gain_all, normed,
    pre_out, hidden_out, head_part, head_land, d_heads, stat_own, stat_land,
    d_pre_out, d_pre_in, hidden_t, d_normed,
    hidden_ring, far_tokens, residual_ring, small_own, small_land,
    partial, twin_part, landing, twin_part_b, landing_b, arrived, gain_parts, gain_land,
    whole_out, whole_mix, whole_in, land_out, x_out, x_mix, x_in,
    sum_out, sum_mix, sum_in,
    send_sems, recv_sems, local_sems,
):
    place = Place()
    task = TaskPlace()
    wires = Wires(send_sems, recv_sems)
    gather_a, gather_b, scatter_slots = wires.claim(30), wires.claim(30), wires.claim(30)
    me = place.me
    own_cols = pl.ds(pl.multiple_of(me * 256, 256), 256)
    first = load(own_tokens, tokens.at[pl.ds(0, 512), own_cols], local_sems, 0)
    g = gain[...]
    hi = g.astype(BF16).astype(F32)
    mid = (g - hi).astype(BF16).astype(F32)
    low = g - hi - mid
    row = sublanes((16, 256))
    rows = jnp.where(row == 0, hi, jnp.where(row == 1, mid, jnp.where(row == 2, low, 0.0)))
    tokens[pl.ds(512, 16), own_cols] = rows.astype(BF16)
    greet_everyone()
    first.wait()

    def token_view(block, half):
        rows = pl.ds(0, 256) if half == 0 else pl.ds(256, 272)
        return tokens.at[rows, pl.ds(pl.multiple_of(block * 256, 256), 256)]

    gather = Gather(place, wires, token_view, gather_a)
    gather.open()
    get_in = load(w_in, w_in_v, local_sems, 1)
    get_mix = load(w_mix, w_mix_v, local_sems, 2)
    get_out = load(w_out, w_out_v, local_sems, 3)

    stat_own[...] = popart_rows(tasks, rewards, ends)
    statistics = AllPairs(wires, "task", 8, stat_land)
    for hop in range(1, 8):
        statistics.post(hop, lambda peer: stat_own)
    gather.middle()

    def slab(dz, opening=False):
        at = pl.multiple_of(plus(place.z, dz, 4) * 1024, 1024)

        def tile(m, carry):
            r = pl.ds(pl.multiple_of(m * 128, 128), 128)
            value = dot(tokens[r, pl.ds(at, 1024)], w_in_v[pl.ds(at, 1024), :])
            pre_in[r, :] = value if opening else pre_in[r, :] + value
            return carry

        lax.fori_loop(0, 4, tile, 0)

    get_in.wait()
    gather.wait_twin(gather.OWN, gather.ACROSS)
    slab(0, True)
    gather.late()
    gather.wait_twin(gather.FROM_UP, gather.UP_ACROSS)
    slab(1)
    gather.last()
    gather.wait_twin(gather.FROM_DOWN, gather.DOWN_ACROSS)
    slab(3)
    gather.wait_twin(gather.FAR, gather.FAR_ACROSS)
    slab(2)

    def activate(m, carry):
        r = pl.ds(pl.multiple_of(m * 128, 128), 128)
        v = pre_in[r, :]
        hidden = (v * sigmoid(v)).astype(BF16)
        hidden_in[r, :] = hidden
        hidden_ring[pl.ds(m * 4, 4), task.y] = hidden.reshape(4, 32, 256)
        return carry

    lax.fori_loop(0, 4, activate, 0)
    get_mix.wait()
    wires.drain(("tp",))
    scatter = Scatter(place, wires, partial, twin_part, landing, scatter_slots)
    scatter.open(lambda half: wide_product(hidden_in, w_mix_v, partial, half, False))

    for_hidden = RingGather(
        task, wires, lambda y, half: hidden_ring.at[pl.ds(half * 8, 8), y], 2
    )
    for_hidden.open(0)
    for_hidden.open(1)
    core_rows = pl.ds(pl.multiple_of(place.c * 256, 256), 256)
    twin_rows = pl.ds(pl.multiple_of(256 - place.c * 256, 256), 256)
    for_tokens = RingExchange(
        task,
        wires,
        lambda y: tokens.at[core_rows, pl.ds(pl.multiple_of(y * 1024, 1024), 1024)],
        lambda dy: far_tokens.at[dy - 1, core_rows, :],
    )
    for_tokens.open()
    token_slot = wires.claim(3)
    g3 = tokens[pl.ds(512, 16), :].astype(F32)
    gain_all[...] = g3[0:1, :] + g3[1:2, :] + g3[2:3, :]
    summed = stat_own[...]
    for hop in range(1, 8):
        statistics.wait(hop)
        summed = summed + stat_land[hop - 1]
    counts, totals, squares = summed[0:1, :], summed[1:2, :], summed[2:3, :]
    small_rows = (head_bias, old_mean, old_scale)
    bias, pop_mean, pop_scale = (
        jnp.concatenate(
            [ref[...], jnp.full((1, 128 - ref.shape[1]), fill, F32)], axis=1
        )
        for ref, fill in zip(small_rows, (0.0, 0.0, 1.0))
    )
    pop_mean, pop_scale = pltpu.roll(pop_mean, ACTIONS, 1), pltpu.roll(pop_scale, ACTIONS, 1)
    pop_scale = jnp.where(lanes((1, 128)) < ACTIONS, 1.0, pop_scale)
    mean, scale = popart_update(counts, totals, squares, pop_mean, pop_scale)
    is_value = lanes((1, 128)) >= ACTIONS
    ratio = jnp.where(is_value, pop_scale / scale, 1.0)
    new_bias = jnp.where(is_value, (pop_scale * bias + pop_mean - mean) / scale, bias)
    new_head[pl.ds(0, 75), :] = (head[...].astype(F32) * as_column(ratio)[0:75, :]).astype(BF16)
    new_head[pl.ds(75, 53), :] = jnp.zeros((53, 256), BF16)
    stats[...] = jnp.concatenate([mean, scale, new_bias, jnp.zeros((5, 128), F32)], axis=0)

    scatter.finish_far()
    scatter.finish_across()
    scatter.finish_near()
    first_env = me * 2
    columns = [
        step_columns(ref, first_env) for ref in (actions, rewards, ends, behaviour)
    ]
    columns[2] = DISCOUNT * (1.0 - columns[2])
    env = [
        jnp.sum(jnp.where(lanes((1, 32)) == first_env + e, tasks[...].astype(F32), 0.0), axis=1, keepdims=True)
        for e in (0, 1)
    ]
    game = jnp.where(sublanes((32, 128)) < 16, env[0], env[1])
    own_value = lanes((32, 128)) == game.astype(jnp.int32) + ACTIONS
    own_rows = pl.ds(pl.multiple_of(me * 32, 32), 32)

    def store(half, value):
        residual[:, half_cols(half)] = (
            value + tokens[own_rows, half_cols(half)].astype(F32)
        )

    scatter.finish(store)
    for m in range(2):
        v = residual[pl.ds(m * 16, 16), :]
        inverse = lax.rsqrt(jnp.mean(v * v, axis=1, keepdims=True) + NORM_EPS)
        normed[pl.ds(pl.multiple_of(me * 32 + m * 16, 16), 16), :] = (
            v * inverse * gain_all[...]
        ).astype(BF16)
    spread = Gather(place, wires, row_view(normed), gather_b)
    spread.open()
    for_hidden.relay(0)
    for_hidden.relay(1)
    heads = AllPairs(wires, "tp", 16, head_land)

    def out_slab(dz):
        start = plus(place.z, dz, 4) * 128
        rows = pl.ds(pl.multiple_of(start, 128), 128)
        v = dot(normed[rows, :], w_out_v[...])
        pre_out[rows, :] = v
        hidden_out[rows, :] = (v * sigmoid(v)).astype(BF16)
        head_part[rows, :] = dot(hidden_out[rows, :], new_head[...], ((1,), (1,))).astype(BF16)

    spread.middle()
    get_out.wait()
    spread.wait_twin(spread.OWN, spread.ACROSS)
    out_slab(0)
    spread.late()
    spread.wait_twin(spread.FROM_UP, spread.UP_ACROSS)
    out_slab(1)
    spread.last()
    spread.wait_twin(spread.FROM_DOWN, spread.DOWN_ACROSS)
    out_slab(3)
    spread.wait_twin(spread.FAR, spread.FAR_ACROSS)
    out_slab(2)

    def frames_of(ref):
        return lambda device: ref.at[pl.ds(pl.multiple_of(device * 32, 32), 32), :]

    for hop in range(1, 16):
        heads.post(hop, frames_of(head_part))
    for dy in (1, 2, 3):
        for_tokens.wait(dy)
        share = far_tokens.at[dy - 1, core_rows, :]
        wires.send(share, share, token_slot + dy - 1, place.partner)
    for_hidden.end()
    for b in range(4):
        hidden_t[:, b * 512 : b * 512 + 512] = (
            hidden_ring[b * 4 : b * 4 + 4].reshape(512, 256).T
        )
    outputs = head_part[own_rows, :].astype(F32)
    for hop in range(1, 16):
        heads.wait(hop)
        outputs = outputs + head_land[hop - 1].astype(F32)
    d_own = loss_gradient(outputs + new_bias, own_value, columns, mean, scale)
    d_heads[own_rows, :] = d_own.astype(BF16)
    d_slot = wires.claim(15)
    d_view = frames_of(d_heads)
    for hop in range(1, 16):
        wires.send(d_view(me), d_view(me), d_slot + hop - 1, plus(me, hop, 16))
    for hop in range(1, 16):
        wires.arrived(d_view(plus(me, 16 - hop, 16)), d_slot + hop - 1)
    wires.drain()

    def pre_gradient(m, carry):
        r = pl.ds(pl.multiple_of(m * 128, 128), 128)
        d_hidden = dot(d_heads[r, :], new_head[...])
        d_pre_out[r, :] = (d_hidden * slope(pre_out[r, :])).astype(BF16)
        return carry

    lax.fori_loop(0, 4, pre_gradient, 0)
    for_out = TaskSum(task, wires, slab_rows(512), whole_out, land_out, x_out, sum_out)
    mixes = [
        TaskSum(task, wires, wide_piece(n), whole_mix, None, x_mix.at[n], sum_mix) for n in (0, 1)
    ]
    last_mix = RingFirst(mixes[1])
    x_pieces = (x_in.at[pl.ds(0, 256), :], x_in.at[pl.ds(256, 272), :])
    ins = [
        TaskSum(task, wires, tall_piece(n), whole_in, None, x_pieces[n], sum_in) for n in (0, 1)
    ]

    def tall_product(left, right, whole, height, dy):
        k = plus(task.y, dy, 4)

        def tile(n, carry):
            feature = pl.multiple_of(k * 1024 + n * 256, 256)
            at = pl.multiple_of((k * 2 + n // 2) * height + lax.rem(n, 2) * 256, 16)
            value = dot(left[pl.ds(0, 512), pl.ds(feature, 256)], right[...], ((0,), (0,)))
            whole[pl.ds(at, 256), :] = value.astype(BF16)
            return carry

        lax.fori_loop(0, 4, tile, 0)

    def mix_product(part, n):
        at = pl.multiple_of(part * 512 + n * 256, 256)
        whole_mix[:, pl.ds(at, 256)] = dot(
            hidden_t[...], residual_ring[:, pl.ds(at, 256)]
        ).astype(BF16)

    def in_product(part, n):
        at = pl.multiple_of(part * 512 + n * 256, 256)
        here = pl.ds(pl.multiple_of(task.y * 1024 + at, 256), 256)
        value = dot(tokens[pl.ds(0, 512), here], d_pre_in[task.y], ((0,), (0,)))
        for dy in (1, 2, 3):
            value = value + dot(
                far_tokens[dy - 1, :, pl.ds(at, 256)],
                d_pre_in[plus(task.y, dy, 4)],
                ((0,), (0,)),
            )
        whole_in[pl.ds(pl.multiple_of(part * 528 + n * 256, 16), 256), :] = value.astype(BF16)

    def out_product(dy):
        tall_product(normed, d_pre_out, whole_out, 512, dy)

    def out_first():
        out_product(2)
        for_out.far()

    scatter = Scatter(place, wires, partial, twin_part_b, landing_b, scatter_slots)
    scatter.open(lambda half: wide_product(d_pre_out, w_out_v, partial, half, True), out_first)
    out_product(1)
    out_product(3)
    for_out.near()
    scatter.finish_far()
    scatter.finish_across()
    out_product(0)
    for_out.relay()
    scatter.finish_near()

    def store(half, value):
        d_normed[:, half_cols(half)] = value

    scatter.finish(store)
    gain_rows = jnp.zeros((8, 4096), F32)
    for m in range(2):
        r = pl.ds(m * 16, 16)
        v = residual[r, :]
        inverse = lax.rsqrt(jnp.mean(v * v, axis=1, keepdims=True) + NORM_EPS)
        d = d_normed[r, :]
        scaled = d * gain_all[...]
        inner = jnp.sum(scaled * v, axis=1, keepdims=True)
        step = inverse * scaled - v * (inverse * inverse * inverse * inner * (1.0 / 4096))
        arrived[pl.ds(pl.multiple_of(me * 32 + m * 16, 16), 16), :] = step.astype(BF16)
        d_normed[r, :] = d * v * inverse
    wires.drain(("tp",))
    gather = Gather(place, wires, row_view(arrived), gather_a)
    gather.open()
    ring_rows = lambda y: pl.ds(pl.multiple_of(me * 128 + y * 32, 32), 32)
    quarter = lambda y: pl.ds(pl.multiple_of(y * 1024, 1024), 1024)
    own32 = pl.ds(pl.multiple_of(me * 32, 32), 32)
    residual_ring[ring_rows(task.y), :] = arrived[own32, quarter(task.y)]
    for_residual = RingExchange(
        task,
        wires,
        lambda y: arrived.at[own32, quarter(y)],
        lambda dy: residual_ring.at[ring_rows(plus(task.y, dy, 4)), :],
    )
    for dy in (2, 1, 3):
        y = plus(task.y, dy, 4)
        wires.send(
            arrived.at[own32, quarter(y)],
            residual_ring.at[ring_rows(task.y), :],
            for_residual.first + 3 - dy,
            task.xh * 4 + y,
            "task",
        )
    for m in range(4):
        gain_rows = gain_rows + d_normed[pl.ds(m * 8, 8), :]
    for n in range(16):
        gain_parts[n] = gain_rows[:, n * 256 : n * 256 + 256]
    gains = AllPairs(wires, "tp", 16, gain_land, heads.first)
    for hop in range(1, 16):
        gains.post(hop, lambda peer: gain_parts.at[peer])

    def hidden_slab(dz):
        rows = pl.ds(pl.multiple_of(plus(place.z, dz, 4) * 128, 128), 128)
        d = dot(arrived[rows, :], w_mix_v[...], ((1,), (1,)))
        d_pre_in[task.y, rows, :] = (d * slope(pre_in[rows, :])).astype(BF16)

    slabs = (0, 1, 3, 2)
    for_slope = RingGather(
        task,
        wires,
        lambda y, piece: d_pre_in.at[
            y, pl.ds(pl.multiple_of(plus(place.z, slabs[piece], 4) * 128, 128), 128), :
        ],
        4,
    )
    for_out.fold()
    gather.middle()
    for_out.finish()
    gather.wait_twin(gather.OWN, gather.ACROSS)
    hidden_slab(0)
    for_slope.open(0)
    gather.late()
    for dy in (1, 3, 2):
        for_residual.wait(dy)
    ring = Gather(
        place,
        wires,
        lambda block, half: residual_ring.at[
            pl.ds(pl.multiple_of(block * 128, 128), 128), pl.ds(half * 512, 512)
        ],
        gather_b,
        True,
    )
    ring.open()
    gather.wait_twin(gather.FROM_UP, gather.UP_ACROSS)
    hidden_slab(1)
    for_slope.open(1)
    gather.last()
    gather.wait_twin(gather.FROM_DOWN, gather.DOWN_ACROSS)
    hidden_slab(3)
    for_slope.open(2)
    for_slope.relay(0)
    gather.wait_twin(gather.FAR, gather.FAR_ACROSS)
    hidden_slab(2)
    for_slope.open(3)
    small = dot(d_heads[...], hidden_out[...], ((0,), (0,)))
    bias = jnp.sum(d_heads[...].astype(F32), axis=0, keepdims=True)
    gain_total = jnp.sum(gain_parts[me], axis=0, keepdims=True)
    for hop in range(1, 16):
        gains.wait(hop)
        gain_total = gain_total + jnp.sum(gain_land[hop - 1], axis=0, keepdims=True)
    row = sublanes((128, 256))
    bias = jnp.concatenate([bias, jnp.zeros((1, 128), F32)], axis=1)
    small_own[...] = jnp.where(
        row == 80, bias, jnp.where(row == 88, gain_total, small)
    ).astype(BF16)
    small_rows = lambda y: small_own.at[pl.ds(pl.multiple_of(y * 32, 32), 32), :]
    for_small = RingExchange(task, wires, small_rows, lambda dy: small_land.at[dy - 1])
    for_small.open()
    for_slope.relay(1)
    for_slope.relay(2)
    for_slope.relay(3)
    ring.middle_near()
    for_out.spread()
    ring.middle_across()
    for dy in (1, 2, 3):
        wires.arrived(far_tokens.at[dy - 1, twin_rows, :], token_slot + dy - 1)
    extra = small_rows(task.y)[...].astype(F32)
    for dy in (1, 3, 2):
        for_small.wait(dy)
        extra = extra + small_land[dy - 1].astype(F32)
    for part in (0, 1):
        whole_in[pl.ds(part * 528 + 512, 16), :] = extra[part * 16 : part * 16 + 16, :].astype(BF16)
    for_slope.end()
    in_product(1 - task.xh, 0)
    ins[0].fold()
    in_product(1 - task.xh, 1)
    ins[1].fold()
    ring.middle_far()
    in_product(task.xh, 0)
    ring.late()
    in_product(task.xh, 1)
    ins[0].finish()
    ring.last()
    ins[1].finish()
    ring.wait_twin(*range(8))
    mix_product(1 - task.xh, 0)
    mixes[0].fold()
    mix_product(1 - task.xh, 1)
    mixes[1].fold()
    mix_product(task.xh, 0)
    mix_product(task.xh, 1)
    for_out.spread_far()
    ins[0].spread()
    ins[1].spread()
    mixes[0].finish()
    ins[0].spread_far()
    last_mix.finish()
    ins[1].spread_far()
    mixes[0].spread()
    last_mix.relay()
    last_mix.cross()
    for_out.end()
    keep_out = load(sum_out, sum_out_hbm, local_sems, 4)
    mixes[0].spread_far()
    last_mix.cross_far()
    ins[0].end()
    ins[1].end()
    keep_in = load(sum_in, sum_in_hbm, local_sems, 6)
    mixes[0].end()
    last_mix.end()
    keep_mix = load(sum_mix, sum_mix_hbm, local_sems, 5)
    wires.drain()
    for keep in (keep_out, keep_mix, keep_in):
        keep.wait()


def finish_kernel(
    sum_out, sum_mix, sum_in, new_head, stats,
    grad_in, grad_mix, grad_out, gain, head, bias, head_now, bias_now, mean, scale,
    out_b, mix_b, in_b, small_b, out_f, mix_f, in_f, sems,
):
    gets = []
    for n in range(8):
        r = pl.ds(n * 512, 512)
        gets.append(load(sum_in.at[pl.ds(n * 528, 512), :], in_b.at[r, :], sems, n))
    for n in range(8):
        gets.append(
            load(sum_in.at[pl.ds(n * 528 + 512, 16), :], small_b.at[pl.ds(n * 16, 16), :], sems, 8 + n)
        )
    for n in range(4):
        r = pl.ds(n * 64, 64)
        gets.append(load(sum_mix.at[r, :], mix_b.at[r, :], sems, 16 + n))
    for n in range(8):
        r = pl.ds(n * 512, 512)
        gets.append(load(sum_out.at[r, :], out_b.at[r, :], sems, 20 + n))
    puts = []
    for n in range(8):
        r = pl.ds(n * 512, 512)
        gets[n].wait()
        in_f[r, :] = in_b[r, :].astype(F32)
        puts.append(load(in_f.at[r, :], grad_in.at[r, :], sems, 28 + n))
    for n in range(4):
        r = pl.ds(n * 64, 64)
        gets[16 + n].wait()
        mix_f[r, :] = mix_b[r, :].astype(F32)
        puts.append(load(mix_f.at[r, :], grad_mix.at[r, :], sems, 36 + n))
    for n in range(8):
        r = pl.ds(n * 512, 512)
        gets[20 + n].wait()
        out_f[r, :] = out_b[r, :].astype(F32)
        puts.append(load(out_f.at[r, :], grad_out.at[r, :], sems, 40 + n))
    for n in range(8):
        gets[8 + n].wait()
    small = small_b[...].astype(F32)
    head[...] = small[0:75, :]
    bias[...] = small[80:81, 0:75]
    gain[...] = small[88:89, :]
    head_now[...] = new_head[0:75, :]
    values = pltpu.roll(stats[...], 128 - ACTIONS, 1)
    mean[...] = values[0:1, 0:TASKS]
    scale[...] = values[1:2, 0:TASKS]
    bias_now[...] = stats[2:3, 0:75]
    for put in puts:
        put.wait()


def hbm():
    return pl.BlockSpec(memory_space=pltpu.HBM)


def vmem():
    return pl.BlockSpec(memory_space=pltpu.VMEM)


def step_call(*arguments):
    v, h = vmem(), hbm()
    scratch = [
        ((528, 4096), BF16), ((4096, 256), BF16), ((256, 4096), BF16), ((4096, 256), BF16),
        ((512, 256), F32), ((512, 256), BF16), ((32, 4096), F32), ((1, 4096), F32),
        ((512, 4096), BF16),
        ((512, 256), F32), ((512, 256), BF16), ((512, 128), BF16), ((15, 32, 128), BF16),
        ((512, 128), BF16), ((8, 128), F32), ((7, 8, 128), F32),
        ((512, 256), BF16), ((4, 512, 256), BF16), ((256, 2048), BF16), ((32, 4096), F32),
        ((16, 4, 32, 256), BF16), ((3, 512, 1024), BF16), ((2048, 1024), BF16),
        ((128, 256), BF16), ((3, 32, 256), BF16),
        ((512, 4096), BF16), ((8, 32, 4096), BF16), ((7, 32, 4096), BF16),
        ((8, 32, 4096), BF16), ((7, 32, 4096), BF16), ((512, 4096), BF16),
        ((16, 8, 256), F32), ((15, 8, 256), F32),
        ((4096, 256), BF16), ((256, 1024), BF16), ((1056, 256), BF16),
        ((3, 2, 512, 256), BF16),
        ((512, 256), BF16), ((2, 256, 256), BF16), ((528, 256), BF16),
        ((4096, 256), BF16), ((256, 4096), BF16), ((4224, 256), BF16),
    ]
    return pl.pallas_call(
        step_kernel,
        out_shape=[
            jax.ShapeDtypeStruct((4096, 256), BF16),
            jax.ShapeDtypeStruct((256, 4096), BF16),
            jax.ShapeDtypeStruct((4224, 256), BF16),
            jax.ShapeDtypeStruct((128, 256), BF16),
            jax.ShapeDtypeStruct((8, 128), F32),
        ],
        in_specs=[h, v, h, h, h, v, v, v, v, v, v, v, v, v],
        out_specs=[h, h, h, v, v],
        scratch_shapes=[pltpu.VMEM(*s) for s in scratch]
        + [pltpu.SemaphoreType.DMA((SENDS,)), pltpu.SemaphoreType.DMA((RECEIVES,)), pltpu.SemaphoreType.DMA((7,))],
        compiler_params=pltpu.CompilerParams(
            collective_id=0, has_side_effects=True, vmem_limit_bytes=63 * 2**20
        ),
        name="step",
    )(*arguments)


def finish_call(*arguments):
    v, h = vmem(), hbm()
    return pl.pallas_call(
        finish_kernel,
        out_shape=[
            jax.ShapeDtypeStruct((4096, 256), F32),
            jax.ShapeDtypeStruct((256, 4096), F32),
            jax.ShapeDtypeStruct((4096, 256), F32),
            jax.ShapeDtypeStruct((1, 256), F32),
            jax.ShapeDtypeStruct((75, 256), F32),
            jax.ShapeDtypeStruct((1, 75), F32),
            jax.ShapeDtypeStruct((75, 256), BF16),
            jax.ShapeDtypeStruct((1, 75), F32),
            jax.ShapeDtypeStruct((1, TASKS), F32),
            jax.ShapeDtypeStruct((1, TASKS), F32),
        ],
        in_specs=[h, h, h, v, v],
        out_specs=[h, h, h, v, v, v, v, v, v, v],
        scratch_shapes=[
            pltpu.VMEM((4096, 256), BF16),
            pltpu.VMEM((256, 4096), BF16),
            pltpu.VMEM((4096, 256), BF16),
            pltpu.VMEM((128, 256), BF16),
            pltpu.VMEM((4096, 256), F32),
            pltpu.VMEM((256, 4096), F32),
            pltpu.VMEM((4096, 256), F32),
            pltpu.SemaphoreType.DMA((48,)),
        ],
        compiler_params=pltpu.CompilerParams(vmem_limit_bytes=63 * 2**20),
        name="finish",
    )(*arguments)


def on_device(
    observations, gain, w_in, w_mix, w_out, w_head, head_bias, pop_mean, pop_scale,
    task_indices, actions, rewards, episode_ends, behaviour_log_prob,
):
    sums = step_call(
        observations.reshape(512, 256),
        gain.reshape(1, 256),
        w_in,
        w_mix,
        w_out,
        w_head.T,
        head_bias.reshape(1, ACTIONS + TASKS),
        pop_mean.reshape(1, TASKS),
        pop_scale.reshape(1, TASKS),
        task_indices.reshape(1, 32),
        actions.T,
        rewards.T,
        episode_ends.T,
        behaviour_log_prob.T,
    )
    (
        grad_in, grad_mix, grad_out, grad_gain, grad_head, grad_bias,
        new_head, new_bias, mean, scale,
    ) = finish_call(*sums)
    return (
        grad_in,
        grad_mix,
        grad_out,
        grad_gain.reshape(256),
        grad_head.T,
        grad_bias.reshape(75),
        new_head.T,
        new_bias.reshape(75),
        mean.reshape(TASKS),
        scale.reshape(TASKS),
    )


def solution(mesh):
    in_specs = (
        P("task", None, "tp"),
        P("tp"),
        P(None, "tp"),
        P("tp", None),
        P(None, "tp"),
        P("tp", None),
        P(),
        P(),
        P(),
        P("task"),
        P("task", None),
        P("task", None),
        P("task", None),
        P("task", None),
    )
    out_specs = (
        P(None, "tp"),
        P("tp", None),
        P(None, "tp"),
        P("tp"),
        P("tp", None),
        P(),
        P("tp", None),
        P(),
        P(),
        P(),
    )
    return jax.shard_map(
        on_device, mesh=mesh, in_specs=in_specs, out_specs=out_specs, check_vma=False
    )
```
